32 devices in a mesh: gx: 2 (over core), gy: 4 (over y, x), lev: 4 (over z).
Axes of the slice: x: 2, y: 2, z: 4, core: 2. Of those that a mesh axis runs over, the one named last changes fastest.
Arguments:
- u_wind: float32 [256, 32, 512], P('lev', 'gx', 'gy'), may hold values from -6 to 6
- v_wind: float32 [256, 32, 512], P('lev', 'gx', 'gy'), may hold values from -6 to 6
- w_wind: float32 [256, 32, 512], P('lev', 'gx', 'gy'), may hold values from -4 to 4
- pressure: float32 [256, 32, 512], P('lev', 'gx', 'gy'), may hold values from -6 to 6
- buoyancy: float32 [256, 32, 512], P('lev', 'gx', 'gy'), may hold values from 0.5 to 2
- stiffness: float32 [256, 32, 512], P('lev', 'gx', 'gy'), may hold values from 0.5 to 2
Outputs:
- u_final: float32 [256, 32, 512], P('lev', 'gx', 'gy')
- v_final: float32 [256, 32, 512], P('lev', 'gx', 'gy')
- w_final: float32 [256, 32, 512], P('lev', 'gx', 'gy')
- p_final: float32 [256, 32, 512], P('lev', 'gx', 'gy')
The draws below stay inside these ranges and needn't reach their ends.
All inputs are finite; a program needn't handle non-finite values.
Results may differ from the reference program's by a relative error of at most 0.002.
Values sent between devices are 32-bit elements; how exact they have to be, the bound alone decides.
A program may use at most 128 MiB of HBM per device.

```python
import math
import jax
import jax.numpy as jnp
from jax import lax

SUBSTEPS = 3
NX = 32
NY = 512
NZ = 256


def draw_w_wind(key, part):
    walk_key, rough_key = jax.random.split(jax.random.fold_in(key, 11))
    grid_shape = (NZ, NX, NY)
    increments = jax.random.normal(walk_key, grid_shape, jnp.float32)
    random_walk = jnp.cumsum(increments, axis=0) / jnp.sqrt(jnp.float32(NZ))
    rough_part = 0.3 * jax.random.normal(rough_key, grid_shape, jnp.float32)
    return jnp.clip(random_walk + rough_part, -4.0, 4.0)


def levels(own_key, extent, cuts, least, largest):
    factor_of, own = 1.0, jax.random.fold_in(own_key, 6)
    for axis_at, blocks in cuts:
        draws = jnp.exp(jax.random.uniform(jax.random.fold_in(own, axis_at), (blocks,), jnp.float32, least / len(cuts), largest / len(cuts)))
        factor_of = factor_of * jnp.repeat(draws, extent[axis_at] // blocks).reshape([-1 if axis == axis_at else 1 for axis in range(len(extent))])
    return factor_of


def scatter_about(stream_key, dims, deviation, reach, cuts=(), kind=jnp.bfloat16):
    loudness = levels(stream_key, dims, cuts, -0.22, 0.18) if cuts else 1.0
    drawn = jax.random.normal(stream_key, dims, jnp.float32) * deviation * loudness
    return jnp.minimum(jnp.maximum(drawn, -reach), reach).astype(kind)


def setup_inputs(seed: int = 0) -> dict:
    streams_of = jax.random.split(jax.random.key(seed), 7)
    u_wind = scatter_about(streams_of[0], (NZ, NX, NY), 1.0, 6.0, ((0, 4), (1, 2), (2, 4)), jnp.float32)
    v_wind = scatter_about(streams_of[1], (NZ, NX, NY), 1.0, 6.0, ((0, 4), (1, 2), (2, 4)), jnp.float32)
    w_wind = draw_w_wind(jax.random.fold_in(streams_of[6], 71), 0)
    pressure = scatter_about(streams_of[3], (NZ, NX, NY), 1.0, 6.0, ((0, 4), (1, 2), (2, 4)), jnp.float32)
    buoyancy = jnp.clip(jnp.exp(math.log(2.0) - 1.3862944 * jax.random.uniform(streams_of[4], (NZ, NX, NY), jnp.float32) ** levels(streams_of[4], (NZ, NX, NY), ((0, 4), (1, 2), (2, 4)), -0.2, 0.2)), 0.5, 2.0)
    stiffness = jnp.clip(jnp.exp(math.log(2.0) - 1.3862944 * jax.random.uniform(streams_of[5], (NZ, NX, NY), jnp.float32) ** levels(streams_of[5], (NZ, NX, NY), ((0, 4), (1, 2), (2, 4)), -0.2, 0.2)), 0.5, 2.0)
    return dict(u_wind=u_wind, v_wind=v_wind, w_wind=w_wind, pressure=pressure, buoyancy=buoyancy, stiffness=stiffness)


courant_h = 0.3
vertical_gain = 4096.0

def neighbour(grid_field, offset, axis_number):
    return jnp.roll(grid_field, -offset, axis=axis_number)

def reference(u_wind, v_wind, w_wind, pressure, buoyancy, stiffness):
    zero_row = jnp.zeros((1,) + pressure.shape[1:], jnp.float32)
    stiff_up = jnp.concatenate([stiffness[1:], zero_row], 0)
    lower_band = -vertical_gain * buoyancy * stiffness
    lower_band = jnp.concatenate([zero_row, lower_band[1:]], 0)
    upper_band = -vertical_gain * buoyancy * stiff_up
    main_band = 1.0 + vertical_gain * buoyancy * (stiffness + stiff_up)
    lower_cols = jnp.moveaxis(lower_band, 0, -1)
    main_cols = jnp.moveaxis(main_band, 0, -1)
    upper_cols = jnp.moveaxis(upper_band, 0, -1)
    for substep in range(SUBSTEPS):
        u_new = u_wind - courant_h * buoyancy * (neighbour(pressure, 1, 1) - neighbour(pressure, -1, 1))
        v_new = v_wind - courant_h * buoyancy * (neighbour(pressure, 1, 2) - neighbour(pressure, -1, 2))
        divergence = neighbour(u_new, 1, 1) - neighbour(u_new, -1, 1) + (neighbour(v_new, 1, 2) - neighbour(v_new, -1, 2))
        p_star = pressure - courant_h * stiffness * divergence
        p_above = jnp.concatenate([p_star[1:], zero_row], 0)
        right_side = w_wind - vertical_gain * buoyancy * (p_above - p_star)
        solved = lax.linalg.tridiagonal_solve(lower_cols, main_cols, upper_cols, jnp.moveaxis(right_side, 0, -1)[..., None])
        w_new = jnp.moveaxis(solved[..., 0], -1, 0)
        w_below = jnp.concatenate([zero_row, w_new[:-1]], 0)
        pressure = p_star - stiffness * (w_new - w_below)
        u_wind, v_wind, w_wind = (u_new, v_new, w_new)
    return (u_wind, v_wind, w_wind, pressure)
```

```python
import functools
from types import SimpleNamespace

import jax
import jax.numpy as jnp
from jax import lax
from jax.experimental import pallas as pl
from jax.experimental.pallas import tpu as pltpu
from jax.sharding import PartitionSpec as P

SUBSTEPS = 3
CH = 0.3
GAIN = 4096.0
MESH = pl.DeviceIdType.MESH
GROUP = 16
F32 = jnp.float32


def scratch(K, J, nz):
    R, T, KJ, K2, KH = 16 * K, SUBSTEPS, 8 * (K // GROUP), 2 * K, 4 * (K // GROUP)
    V = lambda *s: pltpu.VMEM((*s, J), F32)
    D = lambda *s: pltpu.SemaphoreType.DMA(s)
    m = max(nz - 1, 1)
    s = {n: V(R) for n in ("us", "vs", "s", "bi", "bj", "E", "D", "H", "X", "Y", "ps", "h")}
    s |= {n: V(3 * K2 + 16) for n in ("i0_low", "i0_high", "i0_up", "i0_down")}
    s |= {n: V(2 * KH) for n in ("j0_right", "j0_left", "j0_fl", "j0_fr")}
    s |= {n: V(3 * K2) for n in ("is_low", "is_high", "is_up", "is_down")}
    s |= {n: V(3 * KH) for n in ("js_right", "js_left", "js_fl", "js_fr")}
    s |= {n: V(T, 2 * K2) for n in ("iw_low", "iw_high", "iw_up", "iw_down")}
    s |= {n: V(T, 2 * KH) for n in ("jw_right", "jw_left", "jw_fl", "jw_fr")}
    s |= {n: V(T, nz, 8) for n in ("ic_low", "ic_high", "ic_up", "ic_down", "jc", "jc_fl", "jc_fr")}
    s |= {n: V(T, K2 + 16) for n in ("p_up", "p_down", "p_low")}
    s |= {n: V(3 * KJ) for n in ("own0",)}
    s |= {n: V(KJ) for n in ("hv", "hbj", "C", "vbr")}
    s |= {n: V(3 * KJ) for n in ("Hc", "Oc")}
    s |= {n: V(T, 2 * KJ) for n in ("Hw", "Ow")}
    s |= {n: V(T, KJ) for n in ("Hp", "Op")}
    s |= {n: V(K2 + 16) for n in ("hu", "hbi")}
    s |= {"cmine": V(64), "cgath": V(nz, 64), "fmine": V(T, 2, 16), "fgath": V(T, nz, 16)}
    s |= {"ctab": V(nz * nz, 32), "mine": V(80)}
    s |= {"in_sem": D(6)}
    for n in ("h0", "hs"):
        s |= {n + "_s": D(4), n + "_r": D(4)}
    s |= {"hw_s": D(T, 4), "hw_r": D(T, 4), "hc_s": D(T, 4, nz), "hc_r": D(T, 4, nz)}
    s |= {"cs_s": D(m), "cs_r": D(m), "ls_s": D(T, m), "ls_r": D(T, m)}
    return s


def kernel(names, K, nx, ny, nz, u_in, v_in, w_in, p_in, b_in, s_in, uo, vo, w, p, *refs):
    q = SimpleNamespace(**dict(zip(names, refs)))
    gx, gy, me = lax.axis_index("gx"), lax.axis_index("gy"), lax.axis_index("lev")
    up, down = lax.rem(gx + 1, nx), lax.rem(gx + nx - 1, nx)
    right, left = lax.rem(gy + 1, ny), lax.rem(gy + ny - 1, ny)
    groups = K // GROUP
    K2, KJ, KH = 2 * K, 8 * (K // GROUP), 4 * (K // GROUP)
    sides = ({"gy": right}, {"gy": left}, {"gx": down}, {"gx": up})

    loads = []
    for n, (src, dst) in enumerate(
        ((p_in, p), (b_in, q.bi), (u_in, q.us), (v_in, q.vs), (s_in, q.s), (w_in, w))
    ):
        c = pltpu.make_async_copy(src, dst, q.in_sem.at[n])
        c.start()
        loads.append(c)

    barrier = pltpu.get_barrier_semaphore()
    for dev in sides:
        pl.semaphore_signal(barrier, inc=1, device_id=dev, device_id_type=MESH)
    for o in range(1, nz):
        pl.semaphore_signal(
            barrier, inc=1, device_id={"lev": lax.rem(me + o, nz)}, device_id_type=MESH
        )

    lane = lax.broadcasted_iota(jnp.int32, (8, 128), 1)
    sub = lax.broadcasted_iota(jnp.int32, (8, 128), 0)
    quad = lane % 4
    zero = jnp.zeros((8, 128), F32)
    one = jnp.ones((8, 128), F32)

    def roll(x, shift, axis):
        shift = shift % x.shape[axis]
        return x if shift == 0 else pltpu.roll(x, shift, axis)

    def at(ref, row, aligned=True):
        return ref[pl.ds(pl.multiple_of(row, 8) if aligned else row, 8), :]

    def put(ref, row, value):
        ref[pl.ds(pl.multiple_of(row, 8), 8), :] = value

    def each(body, carry=None, downward=False):
        def step(n, c):
            g = groups - 1 - n if downward else n
            return body(g, c)
        return lax.fori_loop(0, groups, step, carry)

    def pair(ref, g, j):
        return at(ref, g * 256 + 16 * j), at(ref, g * 256 + 16 * j + 8)

    def put_pair(ref, g, j, value):
        put(ref, g * 256 + 16 * j, value[0])
        put(ref, g * 256 + 16 * j + 8, value[1])

    def edge_rows(g, j, x, low, high, base):
        row = base + g * 32 + 2 * j
        low[pl.ds(row, 2), :] = x[0][0:2]
        if high is not None:
            high[pl.ds(row, 2), :] = x[1][6:8]

    def pack_columns(j, x, acc):
        for half in range(2):
            n = 2 * j + half
            acc = jnp.where(lane // 4 == n, roll(x[half], 4 * n + 2, 1), acc)
        return acc

    def remote(src, dst, ss, rs, dev):
        return pltpu.make_async_remote_copy(
            src_ref=src, dst_ref=dst, send_sem=ss, recv_sem=rs, device_id=dev, device_id_type=MESH
        )

    def dense(own, base, to_right, to_left, row):
        for n in range(groups // 2):
            a, b = (own[base + 16 * n + 8 * m:base + 16 * n + 8 * m + 8, :] for m in range(2))
            to_right[row + 8 * n:row + 8 * n + 8, :] = jnp.where(quad < 2, a, roll(b, 2, 1))
            to_left[row + 8 * n:row + 8 * n + 8, :] = jnp.where(quad < 2, roll(a, -2, 1), b)

    def open_up(fl, fr, row, dst, base):
        for n in range(groups // 2):
            a, b = fl[row + 8 * n:row + 8 * n + 8, :], fr[row + 8 * n:row + 8 * n + 8, :]
            for m in range(2):
                k = base + 16 * n + 8 * m
                dst[k:k + 8, :] = jnp.where(
                    quad < 2, roll(b, -2 * m, 1), roll(a, 2, 1) if m == 0 else a
                )

    for c in loads[:4]:
        c.wait()

    def first_pack(g, carry):
        accp = accb = accv = zero
        for j in range(GROUP):
            for n, ref in enumerate((p, q.bi, q.us)):
                x = pair(ref, g, j)
                edge_rows(g, j, x, q.i0_low, q.i0_high, 8 + n * K2)
                if n == 0:
                    accp = pack_columns(j, x, accp)
                if n == 1:
                    accb = pack_columns(j, x, accb)
            accv = pack_columns(j, pair(q.vs, g, j), accv)
        put(q.own0, g * 8, accp)
        put(q.own0, KJ + g * 8, accb)
        put(q.own0, 2 * KJ + g * 8, accv)
        return carry

    each(first_pack, 0)

    dense(q.own0, 0, q.j0_right, q.j0_left, 0)
    for n in range(groups // 2):
        rights, lefts = [], []
        for m in range(2):
            k = 16 * n + 8 * m
            ab = q.own0[KJ + k:KJ + k + 8, :]
            av = q.own0[2 * KJ + k:2 * KJ + k + 8, :]
            rights.append(jnp.where(quad == 0, roll(av, -1, 1), ab))
            lefts.append(jnp.where(quad == 0, roll(av, -2, 1), roll(ab, -1, 1)))
        k = KH + 8 * n
        for ref, (a, b) in ((q.j0_right, rights), (q.j0_left, lefts)):
            ref[k:k + 8, :] = jnp.where(quad < 2, a, roll(b, 2, 1))

    pl.semaphore_wait(barrier, 4 + nz - 1)

    def exchange(name, ss, rs, at_=lambda r: r):
        return [
            remote(at_(getattr(q, name + a)), at_(getattr(q, name + b)), ss(n), rs(n), dev)
            for n, (a, b, dev) in enumerate(zip(
                ("_right", "_left", "_low", "_high"), ("_fl", "_fr", "_up", "_down"), sides
            ))
        ]

    def four(i, j, ss, rs, at_=lambda r: r):
        pairs = (
            (j + "_right", j + "_fl"), (j + "_left", j + "_fr"),
            (i + "_low", i + "_up"), (i + "_high", i + "_down"),
        )
        return [
            remote(at_(getattr(q, a)), at_(getattr(q, b)), ss(n), rs(n), dev)
            for n, ((a, b), dev) in enumerate(zip(pairs, sides))
        ]

    rows0 = pl.ds(8, 3 * K2)
    halos = [
        remote(
            a if n < 2 else a.at[rows0], b if n < 2 else b.at[rows0],
            q.h0_s.at[n], q.h0_r.at[n], dev,
        )
        for n, (a, b, dev) in enumerate(zip(
            (q.j0_right, q.j0_left, q.i0_low, q.i0_high),
            (q.j0_fl, q.j0_fr, q.i0_up, q.i0_down), sides,
        ))
    ]
    for c in halos:
        c.start()

    loads[4].wait()

    def factor(g, carry):
        B, Z = carry
        for j in reversed(range(GROUP)):
            bb, ss = pair(q.bi, g, j), pair(q.s, g, j)
            newB, newZ = [], []
            for m in range(2):
                row = g * 256 + 16 * j + 8 * m
                gb = GAIN * bb[m]
                o = 1.0 + gb * B[m]
                d = 1.0 / (o + gb * ss[m])
                hh = gb * d
                e = hh * ss[m]
                put(q.D, row, d)
                put(q.H, row, hh)
                put(q.E, row, e)
                put(q.Y, row, hh * Z[m])
                newB.append(ss[m] * (o * d))
                newZ.append(e * Z[m])
            B, Z = tuple(newB), tuple(newZ)
        return B, Z

    B, Z = each(factor, ((zero, zero), (one, one)), downward=True)

    def responses(g, carry):
        x, y = carry
        accs = [zero] * 3
        for j in range(GROUP):
            ee, hz = pair(q.E, g, j), pair(q.Y, g, j)
            x = tuple(ee[m] * x[m] for m in range(2))
            y = tuple(ee[m] * y[m] - hz[m] for m in range(2))
            put_pair(q.X, g, j, x)
            put_pair(q.Y, g, j, y)
            for n, val in enumerate((pair(q.s, g, j), x, y)):
                edge_rows(g, j, val, q.is_low, q.is_high, n * K2)
                accs[n] = pack_columns(j, val, accs[n])
        for n in range(3):
            put(q.Oc, n * KJ + g * 8, accs[n])
        return x, y

    x, y = each(responses, ((one, one), (zero, zero)))
    for n, val in enumerate((x, y, Z, B)):
        for m in range(2):
            q.cmine[16 * n + 8 * m:16 * n + 8 * m + 8, :] = val[m]
            q.cgath[me, 16 * n + 8 * m:16 * n + 8 * m + 8, :] = val[m]
    consts = [
        remote(q.cmine, q.cgath.at[me], q.cs_s.at[o - 1], q.cs_r.at[o - 1], {"lev": lax.rem(me + o, nz)})
        for o in range(1, nz)
    ]
    for c in consts:
        c.start()
    for n in range(3):
        dense(q.Oc, n * KJ, q.js_right, q.js_left, n * KH)
    setups = four("is", "js", lambda n: q.hs_s.at[n], lambda n: q.hs_r.at[n])
    for c in setups:
        c.start()

    def crow(d, n):
        return q.cgath[d, 16 * n:16 * n + 16, :]

    for c in halos:
        c.wait()

    for n in range(groups // 2):
        fr = q.j0_fr[KH + 8 * n:KH + 8 * n + 8, :]
        fl = q.j0_fl[KH + 8 * n:KH + 8 * n + 8, :]
        for m in range(2):
            k = 16 * n + 8 * m
            q.vbr[k:k + 8, :] = roll(fr, -2 * m, 1)
            flg = roll(fl, -2 * m, 1)
            ab = q.own0[KJ + k:KJ + k + 8, :]
            av = q.own0[2 * KJ + k:2 * KJ + k + 8, :]
            q.hv[k:k + 8, :] = jnp.where(quad == 2, roll(flg, 2, 1), roll(av, 1, 1))
            q.hbj[k:k + 8, :] = CH * roll(jnp.where(quad == 1, flg, ab), 1, 1)
    open_up(q.j0_fl, q.j0_fr, 0, q.Hp.at[0], 0)

    def stagger(g, carry):
        packed = at(q.vbr, g * 8)
        for j in range(GROUP):
            xb, xu, xv = pair(q.bi, g, j), pair(q.us, g, j), pair(q.vs, g, j)
            for (val, dst, scale, f) in ((xu, q.us, 1.0, 2), (xb, q.bi, CH, 1)):
                r0, r1 = roll(val[0], 7, 0), roll(val[1], 7, 0)
                edge = q.i0_up[pl.ds(8 + f * K2 + g * 32 + 2 * j - 7, 8), :]
                put_pair(dst, g, j, (
                    scale * jnp.where(sub < 7, r0, r1), scale * jnp.where(sub < 7, r1, edge)
                ))
            for (val, dst, scale, first) in ((xv, q.vs, 1.0, 127), (xb, q.bj, CH, 126)):
                out = []
                for m in range(2):
                    n = 2 * j + m
                    out.append(scale * jnp.where(
                        lane == 127, roll(packed, first - 4 * n, 1), roll(val[m], 127, 1)
                    ))
                put_pair(dst, g, j, out)
        for r in range(4):
            row = g * 32 + 8 * r
            for (dst, f, scale) in ((q.hu, 2, 1.0), (q.hbi, 1, CH)):
                base = 8 + f * K2 + row
                below = q.i0_down[pl.ds(base + 1, 8), :]
                own = q.i0_low[pl.ds(base - 1, 8), :]
                put(dst, 8 + row, scale * jnp.where(sub % 2 == 0, below, own))
        return carry

    each(stagger, 0)

    loads[5].wait()

    def interface():
        beta = jnp.zeros((16, 128), F32)
        betas, rs, zbrs, lams = ([None] * nz for _ in range(4))
        for d in range(nz - 1, -1, -1):
            betas[d] = beta
            rs[d] = 1.0 / (1.0 - crow(d, 1) * beta)
            zbrs[d] = crow(d, 2) * beta * rs[d]
            lams[d] = crow(d, 2) + zbrs[d] * crow(d, 1)
            beta = crow(d, 3) + zbrs[d] * crow(d, 0)
            if d == 0:
                last = beta
        tops = [last] + betas[:-1]
        psi = jnp.zeros((16, 128), F32)
        psis, r2s, xrs, xrps = ([None] * nz for _ in range(4))
        for d in range(nz):
            xrs[d] = crow(d, 0) / (1.0 - psi * crow(d, 3))
            xrps[d] = xrs[d] * psi
            psis[d] = psi
            r2s[d] = 1.0 / (1.0 - psi * tops[d])
            psi = crow(d, 1) + xrps[d] * crow(d, 2)

        def pick(vals):
            out = vals[0]
            for d in range(1, nz):
                out = jnp.where(me == d, vals[d], out)
            return out

        br = [betas[d] * rs[d] for d in range(nz)]
        brx = [br[d] * crow(d, 0) for d in range(nz)]
        for n, vals in enumerate((xrps, zbrs, [r2s[d] * psis[d] for d in range(nz)], br, brx)):
            q.mine[16 * n:16 * n + 16, :] = pick(vals)
        for L in range(nz):
            part = r2s[L]
            for d in range(L - 1, -1, -1):
                q.ctab[L * nz + d, 0:16, :] = part
                q.ctab[L * nz + d, 16:32, :] = brx[L] * part
                part = part * xrs[d]
            part, gain = jnp.ones((16, 128), F32), 1.0 + br[L] * crow(L, 1)
            rpl = r2s[L] * psis[L] * lams[L]
            for d in range(L + 1, nz):
                cw = rpl * part
                q.ctab[L * nz + d, 0:16, :] = cw
                q.ctab[L * nz + d, 16:32, :] = part * gain + brx[L] * cw
                part = part * lams[d]

    def halves(x):
        return x[0:8], x[8:16]

    def pack_pair(wx, px):
        (w0, w1), (p0, p1) = halves(wx), halves(px)
        acc = roll(w0, 2, 1)
        for n, val in ((1, w1), (2, p0), (3, p1)):
            acc = jnp.where(lane // 4 == n, roll(val, 4 * n + 2, 1), acc)
        return acc

    def spread(t):
        z = jnp.where(lane < 16, t, 0.0)
        for n in (16, 32, 64):
            z = z + roll(z, n, 1)
        r = roll(z, 8, 1)
        return jnp.where(lane % 16 < 8, z, r), jnp.where(lane % 16 < 8, r, z)

    for t in range(SUBSTEPS):
        final = t == SUBSTEPS - 1
        i_up, i_down, i_low = (
            (q.i0_up, q.i0_down, q.i0_low) if t == 0
            else (q.p_up.at[t - 1], q.p_down.at[t - 1], q.p_low.at[t - 1])
        )
        own_p, own_base = (q.own0, 0) if t == 0 else (q.Op.at[t - 1], 0)
        halo_p = q.Hp.at[t]

        for k in range(0, KJ, 8):
            hp = halo_p[k:k + 8, :]
            hv_new = q.hv[k:k + 8, :] - q.hbj[k:k + 8, :] * (own_p[own_base + k:own_base + k + 8, :] - hp)
            q.hv[k:k + 8, :] = hv_new
            q.C[k:k + 8, :] = jnp.where(quad < 2, hp, hv_new)

        def explicit(g, A):
            for r in range(4):
                row = g * 32 + 8 * r
                put(q.hu, 8 + row, at(q.hu, 8 + row) - at(q.hbi, 8 + row) * (
                    at(i_low, 8 + row) - at(i_down, 8 + row)
                ))
            c = at(q.C, g * 8)
            acc = zero
            for j in reversed(range(GROUP)):
                pp, uu, vv, ww = pair(p, g, j), pair(q.us, g, j), pair(q.vs, g, j), pair(w, g, j)
                bbi, bbj, ss = pair(q.bi, g, j), pair(q.bj, g, j), pair(q.s, g, j)
                ee, dd, hh = pair(q.E, g, j), pair(q.D, g, j), pair(q.H, g, j)
                r0, r1 = roll(pp[0], 6, 0), roll(pp[1], 6, 0)
                edge = at(i_up, 8 + g * 32 + 2 * j - 6, False)
                pi = (jnp.where(sub < 6, r0, r1), jnp.where(sub < 6, r1, edge))
                un = tuple(uu[m] - bbi[m] * (pi[m] - pp[m]) for m in range(2))
                put_pair(q.us, g, j, un)
                r0, r1 = roll(un[0], 2, 0), roll(un[1], 2, 0)
                edge = at(q.hu, 8 + g * 32 + 2 * j, False)
                um = (jnp.where(sub < 2, edge, r0), jnp.where(sub < 2, r0, r1))
                newA, hs, pss, vn = [], [], [], []
                for m in range(2):
                    edge = roll(c, 126 - 4 * (2 * j + m), 1)
                    pj = jnp.where(lane >= 126, edge, roll(pp[m], 126, 1))
                    v_new = vv[m] - bbj[m] * (pj - pp[m])
                    vm = jnp.where(lane < 2, edge, roll(v_new, 2, 1))
                    star = pp[m] - (CH * ss[m]) * ((un[m] - um[m]) + (v_new - vm))
                    dw = dd[m] * ww[m]
                    hs.append(dw + hh[m] * (star - A[m]))
                    newA.append(ee[m] * A[m] + ((star - ee[m] * star) - ss[m] * dw))
                    pss.append(star)
                    vn.append(v_new)
                put_pair(q.vs, g, j, vn)
                put_pair(q.ps, g, j, pss)
                put_pair(q.h, g, j, hs)
                if not final:
                    edge_rows(g, j, pss, q.iw_low.at[t], q.iw_high.at[t], 0)
                    acc = pack_columns(j, pss, acc)
                A = tuple(newA)
            if not final:
                put(q.Ow.at[t], g * 8, acc)
            return A

        A = each(explicit, (zero, zero), downward=True)

        def forward(g, x):
            acc = zero
            for j in range(GROUP):
                ee, hh = pair(q.E, g, j), pair(q.h, g, j)
                x = tuple(ee[m] * x[m] + hh[m] for m in range(2))
                put_pair(w, g, j, x)
                if not final:
                    edge_rows(g, j, x, q.iw_low.at[t], q.iw_high.at[t], K2)
                    acc = pack_columns(j, x, acc)
            if not final:
                put(q.Ow.at[t], KJ + g * 8, acc)
            return x

        x = each(forward, (zero, zero))
        if t == 0:
            for c in consts:
                c.wait()
            interface()

        wa, aw, r2psi, br, brx = (q.mine[16 * n:16 * n + 16, :] for n in range(5))
        A0, W0 = (jnp.concatenate(n, 0) for n in (A, x))
        up_row, down_row = W0 + wa * A0, A0 + aw * W0
        q.fmine[t, 0], q.fmine[t, 1] = up_row, down_row
        sends, peers = [], {}
        for o in range(1, nz):
            peers[o] = remote(
                q.fmine.at[t, lax.div(me + o, nz)], q.fgath.at[t, me],
                q.ls_s.at[t, o - 1], q.ls_r.at[t, o - 1], {"lev": lax.rem(me + o, nz)},
            )
        wb_own = r2psi * down_row
        pa_own = br * W0 + brx * wb_own
        order = sorted(range(nz), key=lambda o: -min(o, nz - o))
        for o in order:
            if not final:
                L = lax.rem(me + o, nz)
                if o:
                    row = q.fmine[t, lax.div(me + o, nz)]
                    wc, pc = (q.ctab[L * nz + me, 16 * n:16 * n + 16, :] * row for n in range(2))
                else:
                    wc, pc = wb_own, pa_own
                q.jc[t, o] = pack_pair(wc, pc)
                q.ic_low[t, o] = jnp.where(sub < 2, wc[0:8], roll(pc[0:8], 2, 0))
                q.ic_high[t, o] = jnp.where(sub < 2, roll(wc[8:16], 2, 0), roll(pc[8:16], 4, 0))
                for n, (a, b) in enumerate((
                    (q.jc, q.jc_fl), (q.jc, q.jc_fr), (q.ic_low, q.ic_up), (q.ic_high, q.ic_down)
                )):
                    c = remote(
                        a.at[t, o], b.at[t, me], q.hc_s.at[t, n, o], q.hc_r.at[t, n, o],
                        {**sides[n], "lev": L},
                    )
                    c.start()
                    sends.append(c)
            if o:
                peers[o].start()
                sends.append(peers[o])
        if not final:
            for n in range(2):
                dense(q.Ow.at[t], n * KJ, q.jw_right.at[t], q.jw_left.at[t], n * KH)
            works = four("iw", "jw", lambda n: q.hw_s.at[t, n], lambda n: q.hw_r.at[t, n], lambda r: r.at[t])
            for c in works:
                c.start()
            if t == 0:
                for c in setups:
                    c.wait()
                for n in range(3):
                    open_up(q.js_fl, q.js_fr, n * KH, q.Hc, n * KJ)
            for c in works:
                c.wait()
            for n in range(2):
                open_up(q.jw_fl.at[t], q.jw_fr.at[t], n * KH, q.Hw.at[t], n * KJ)

        if final:
            def emit(g, carry):
                hvg = at(q.hv, pl.multiple_of(g * 8, 8))
                for j in range(GROUP):
                    uu, vv = pair(q.us, g, j), pair(q.vs, g, j)
                    r0, r1 = roll(uu[0], 1, 0), roll(uu[1], 1, 0)
                    edge = at(q.hu, 8 + g * 32 + 2 * j + 1, False)
                    put_pair(uo, g, j, (jnp.where(sub < 1, edge, r0), jnp.where(sub < 1, r0, r1)))
                    put_pair(vo, g, j, [
                        jnp.where(
                            lane == 0, roll(hvg, 125 - 4 * (2 * j + m), 1), roll(vv[m], 1, 1)
                        )
                        for m in range(2)
                    ])
                return carry

            each(emit, 0)
        for c in sends:
            c.wait()

        wb, pa = wb_own, pa_own
        for o in range(1, nz):
            d = lax.rem(me + o, nz)
            row = q.fgath[t, d]
            wb = wb + q.ctab[me * nz + d, 0:16, :] * row
            pa = pa + q.ctab[me * nz + d, 16:32, :] * row
        wb2, pa2 = halves(wb), halves(pa)

        if not final:
            fr, fl, iu, idn = (
                functools.reduce(lambda a, b: a + b, [ref[t, d] for d in range(nz)])
                for ref in (q.jc_fr, q.jc_fl, q.ic_up, q.ic_down)
            )
            halo_wp = spread(jnp.where(quad < 2, roll(fr, -2, 1), roll(fl, 2, 1)))
            own_wp = spread(pack_pair(wb, pa))
            for (ws, ps_), src, const, dst in (
                (halo_wp, q.Hw.at[t], q.Hc, q.Hp.at[t + 1]), (own_wp, q.Ow.at[t], q.Oc, q.Op.at[t])
            ):
                before = ws
                for k in range(0, KJ, 8):
                    star, w0 = src[k:k + 8, :], src[KJ + k:KJ + k + 8, :]
                    cs, cx, cy = (const[n * KJ + k:n * KJ + k + 8, :] for n in range(3))
                    now = roll(w0 + cx * ws + cy * ps_, 8, 1)
                    dst[k:k + 8, :] = star - cs * (
                        (w0 + cx * ws + cy * ps_) - jnp.where(lane < 8, before, now)
                    )
                    before = now

            def rows_of(v, src, const, dst):
                z = jnp.where(sub < 4, v, roll(v, 4, 0))
                r = roll(z, 2, 0)
                ws, ps_ = jnp.where(sub % 4 < 2, z, r), jnp.where(sub % 4 < 2, r, z)
                before = ws
                for k in range(0, K2, 8):
                    star, w0 = src[k:k + 8, :], src[K2 + k:K2 + k + 8, :]
                    cs, cx, cy = (const[n * K2 + k:n * K2 + k + 8, :] for n in range(3))
                    wn = w0 + cx * ws + cy * ps_
                    now = roll(wn, 2, 0)
                    dst[8 + k:16 + k, :] = star - cs * (wn - jnp.where(sub < 2, before, now))
                    before = now

            rows_of(iu, q.iw_up.at[t], q.is_up, q.p_up.at[t])
            rows_of(idn, q.iw_down.at[t], q.is_down, q.p_down.at[t])

        def implicit(g, wprev):
            for j in range(GROUP):
                w0, xx, yy = pair(w, g, j), pair(q.X, g, j), pair(q.Y, g, j)
                ss, star = pair(q.s, g, j), pair(q.ps, g, j)
                wn = tuple(w0[m] + xx[m] * wb2[m] + yy[m] * pa2[m] for m in range(2))
                pn = tuple(star[m] - ss[m] * (wn[m] - wprev[m]) for m in range(2))
                put_pair(w, g, j, wn)
                put_pair(p, g, j, pn)
                if not final:
                    edge_rows(g, j, pn, q.p_low.at[t], None, 8)
                wprev = wn
            return wprev

        each(implicit, wb2)


def store(u, v, w, p, u_out, v_out, w_out, p_out, sem):
    copies = [
        pltpu.make_async_copy(src, dst, sem.at[n])
        for n, (src, dst) in enumerate(((u, u_out), (v, v_out), (w, w_out), (p, p_out)))
    ]
    for c in copies:
        c.start()
    for c in copies:
        c.wait()


def solution(mesh):
    nx, ny, nz = (mesh.shape[a] for a in ("gx", "gy", "lev"))

    def shards(*fields):
        K, I, J = fields[0].shape
        assert I == 16 and J == 128 and K % (2 * GROUP) == 0
        R = K * I
        full = pltpu.VMEM((R, J), F32)
        held = scratch(K, J, nz)
        outs = pl.pallas_call(
            functools.partial(kernel, tuple(held), K, nx, ny, nz),
            out_shape=[full] * 4,
            in_specs=[pl.BlockSpec(memory_space=pl.ANY)] * 6,
            out_specs=[pl.BlockSpec(memory_space=pltpu.VMEM)] * 4,
            scratch_shapes=list(held.values()),
            compiler_params=pltpu.CompilerParams(collective_id=0, has_side_effects=True),
        )(*(f.reshape(R, J) for f in fields))
        outs = pl.pallas_call(
            store,
            out_shape=[jax.ShapeDtypeStruct((R, J), F32)] * 4,
            in_specs=[pl.BlockSpec(memory_space=pltpu.VMEM)] * 4,
            out_specs=[pl.BlockSpec(memory_space=pl.ANY)] * 4,
            scratch_shapes=[pltpu.SemaphoreType.DMA((4,))],
        )(*(pltpu.with_memory_space_constraint(o, pltpu.VMEM) for o in outs))
        return tuple(o.reshape(K, I, J) for o in outs)

    spec = P("lev", "gx", "gy")
    return jax.shard_map(
        shards, mesh=mesh, in_specs=(spec,) * 6, out_specs=(spec,) * 4, check_vma=False
    )
```

```python
import functools
from types import SimpleNamespace

import jax
import jax.numpy as jnp
from jax import lax
from jax.experimental import pallas as pl
from jax.experimental.pallas import tpu as pltpu
from jax.sharding import PartitionSpec as P

SUBSTEPS = 3
CH = 0.3
GAIN = 4096.0
MESH = pl.DeviceIdType.MESH
GROUP = 16
F32 = jnp.float32


def scratch(K, J, nz):
    R, T, KJ, K2, KH = 16 * K, SUBSTEPS, 8 * (K // GROUP), 2 * K, 4 * (K // GROUP)
    V = lambda *s: pltpu.VMEM((*s, J), F32)
    D = lambda *s: pltpu.SemaphoreType.DMA(s)
    m = max(nz - 1, 1)
    s = {n: V(R) for n in (
        "us", "vs", "s", "bi", "bj", "E", "D", "H", "X", "Y", "ps", "h",
        "dX", "dY", "P", "Q", "XG", "YG",
    )}
    s |= {n: V(3 * K2 + 16) for n in ("i0_low", "i0_high", "i0_up", "i0_down")}
    s |= {n: V(2 * KH) for n in ("j0_right", "j0_left", "j0_fl", "j0_fr")}
    s |= {n: V(3 * K2) for n in ("is_low", "is_high", "is_up", "is_down")}
    s |= {n: V(3 * KH) for n in ("js_right", "js_left", "js_fl", "js_fr")}
    s |= {n: V(T, 2 * K2) for n in ("iw_low", "iw_high", "iw_up", "iw_down")}
    s |= {n: V(T, 2 * KH) for n in ("jw_right", "jw_left", "jw_fl", "jw_fr")}
    s |= {n: V(T, nz, 8) for n in ("ic_low", "ic_high", "ic_up", "ic_down", "jc", "jc_fl", "jc_fr")}
    s |= {n: V(T, K2 + 16) for n in ("p_up", "p_down", "p_low")}
    s |= {n: V(T, K2) for n in ("b_up", "b_down", "b_low")}
    s |= {n: V(K2) for n in ("bih",)}
    s |= {n: V(2 * K2 + 16) for n in ("mi",)}
    s |= {n: V(2 * KJ) for n in ("cj", "wo")}
    s |= {"coef": V(19, 16)}
    s |= {n: V(3 * KJ) for n in ("own0",)}
    s |= {n: V(KJ) for n in ("hv", "hbj", "C", "vbr")}
    s |= {n: V(3 * KJ) for n in ("Hc", "Oc")}
    s |= {n: V(T, 2 * KJ) for n in ("Hw", "Ow")}
    s |= {n: V(T, KJ) for n in ("Hp", "Op", "Hb", "Ob")}
    s |= {n: V(K2 + 16) for n in ("hu", "hbi")}
    s |= {"cmine": V(64), "cgath": V(nz, 64), "fmine": V(T, 2, 16), "fgath": V(T, nz, 16)}
    s |= {"ctab": V(nz * nz, 32), "mine": V(80)}
    s |= {"in_sem": D(6)}
    for n in ("h0", "hs"):
        s |= {n + "_s": D(4), n + "_r": D(4)}
    s |= {"hw_s": D(T, 4), "hw_r": D(T, 4), "hc_s": D(T, 4, nz), "hc_r": D(T, 4, nz)}
    s |= {"cs_s": D(m), "cs_r": D(m), "ls_s": D(T, m), "ls_r": D(T, m)}
    return s


def kernel(names, K, nx, ny, nz, u_in, v_in, w_in, p_in, b_in, s_in, uo, vo, w, p, *refs):
    q = SimpleNamespace(**dict(zip(names, refs)))
    gx, gy, me = lax.axis_index("gx"), lax.axis_index("gy"), lax.axis_index("lev")
    up, down = lax.rem(gx + 1, nx), lax.rem(gx + nx - 1, nx)
    right, left = lax.rem(gy + 1, ny), lax.rem(gy + ny - 1, ny)
    groups = K // GROUP
    K2, KJ, KH = 2 * K, 8 * (K // GROUP), 4 * (K // GROUP)
    sides = ({"gy": right}, {"gy": left}, {"gx": down}, {"gx": up})

    loads = []
    for n, (src, dst) in enumerate(
        ((p_in, p), (b_in, q.bi), (u_in, q.us), (v_in, q.vs), (s_in, q.s), (w_in, w))
    ):
        c = pltpu.make_async_copy(src, dst, q.in_sem.at[n])
        c.start()
        loads.append(c)

    barrier = pltpu.get_barrier_semaphore()
    for dev in sides:
        pl.semaphore_signal(barrier, inc=1, device_id=dev, device_id_type=MESH)
    for o in range(1, nz):
        pl.semaphore_signal(
            barrier, inc=1, device_id={"lev": lax.rem(me + o, nz)}, device_id_type=MESH
        )

    lane = lax.broadcasted_iota(jnp.int32, (8, 128), 1)
    sub = lax.broadcasted_iota(jnp.int32, (8, 128), 0)
    quad = lane % 4
    zero = jnp.zeros((8, 128), F32)
    one = jnp.ones((8, 128), F32)

    def roll(x, shift, axis):
        shift = shift % x.shape[axis]
        return x if shift == 0 else pltpu.roll(x, shift, axis)

    def at(ref, row, aligned=True):
        return ref[pl.ds(pl.multiple_of(row, 8) if aligned else row, 8), :]

    def put(ref, row, value):
        ref[pl.ds(pl.multiple_of(row, 8), 8), :] = value

    def each(body, carry=None, downward=False):
        def step(n, c):
            g = groups - 1 - n if downward else n
            return body(g, c)
        return lax.fori_loop(0, groups, step, carry)

    def pair(ref, g, j):
        return at(ref, g * 256 + 16 * j), at(ref, g * 256 + 16 * j + 8)

    def put_pair(ref, g, j, value):
        put(ref, g * 256 + 16 * j, value[0])
        put(ref, g * 256 + 16 * j + 8, value[1])

    def edge_rows(g, j, x, low, high, base):
        row = base + g * 32 + 2 * j
        low[pl.ds(row, 2), :] = x[0][0:2]
        if high is not None:
            high[pl.ds(row, 2), :] = x[1][6:8]

    def pack_columns(j, x, acc):
        for half in range(2):
            n = 2 * j + half
            acc = jnp.where(lane // 4 == n, roll(x[half], 4 * n + 2, 1), acc)
        return acc

    def remote(src, dst, ss, rs, dev):
        return pltpu.make_async_remote_copy(
            src_ref=src, dst_ref=dst, send_sem=ss, recv_sem=rs, device_id=dev, device_id_type=MESH
        )

    def dense(own, base, to_right, to_left, row):
        for n in range(groups // 2):
            a, b = (own[base + 16 * n + 8 * m:base + 16 * n + 8 * m + 8, :] for m in range(2))
            to_right[row + 8 * n:row + 8 * n + 8, :] = jnp.where(quad < 2, a, roll(b, 2, 1))
            to_left[row + 8 * n:row + 8 * n + 8, :] = jnp.where(quad < 2, roll(a, -2, 1), b)

    def open_up(fl, fr, row, dst, base):
        for n in range(groups // 2):
            a, b = fl[row + 8 * n:row + 8 * n + 8, :], fr[row + 8 * n:row + 8 * n + 8, :]
            for m in range(2):
                k = base + 16 * n + 8 * m
                dst[k:k + 8, :] = jnp.where(
                    quad < 2, roll(b, -2 * m, 1), roll(a, 2, 1) if m == 0 else a
                )

    for c in loads[:4]:
        c.wait()

    def first_pack(g, carry):
        accp = accb = accv = zero
        for j in range(GROUP):
            for n, ref in enumerate((p, q.bi, q.us)):
                x = pair(ref, g, j)
                edge_rows(g, j, x, q.i0_low, q.i0_high, 8 + n * K2)
                if n == 0:
                    accp = pack_columns(j, x, accp)
                if n == 1:
                    accb = pack_columns(j, x, accb)
            accv = pack_columns(j, pair(q.vs, g, j), accv)
        put(q.own0, g * 8, accp)
        put(q.own0, KJ + g * 8, accb)
        put(q.own0, 2 * KJ + g * 8, accv)
        return carry

    each(first_pack, 0)

    dense(q.own0, 0, q.j0_right, q.j0_left, 0)
    for n in range(groups // 2):
        rights, lefts = [], []
        for m in range(2):
            k = 16 * n + 8 * m
            ab = q.own0[KJ + k:KJ + k + 8, :]
            av = q.own0[2 * KJ + k:2 * KJ + k + 8, :]
            rights.append(jnp.where(quad == 0, roll(av, -1, 1), ab))
            lefts.append(jnp.where(quad == 0, roll(av, -2, 1), roll(ab, -1, 1)))
        k = KH + 8 * n
        for ref, (a, b) in ((q.j0_right, rights), (q.j0_left, lefts)):
            ref[k:k + 8, :] = jnp.where(quad < 2, a, roll(b, 2, 1))

    pl.semaphore_wait(barrier, 4 + nz - 1)

    def exchange(name, ss, rs, at_=lambda r: r):
        return [
            remote(at_(getattr(q, name + a)), at_(getattr(q, name + b)), ss(n), rs(n), dev)
            for n, (a, b, dev) in enumerate(zip(
                ("_right", "_left", "_low", "_high"), ("_fl", "_fr", "_up", "_down"), sides
            ))
        ]

    def four(i, j, ss, rs, at_=lambda r: r):
        pairs = (
            (j + "_right", j + "_fl"), (j + "_left", j + "_fr"),
            (i + "_low", i + "_up"), (i + "_high", i + "_down"),
        )
        return [
            remote(at_(getattr(q, a)), at_(getattr(q, b)), ss(n), rs(n), dev)
            for n, ((a, b), dev) in enumerate(zip(pairs, sides))
        ]

    rows0 = pl.ds(8, 3 * K2)
    halos = [
        remote(
            a if n < 2 else a.at[rows0], b if n < 2 else b.at[rows0],
            q.h0_s.at[n], q.h0_r.at[n], dev,
        )
        for n, (a, b, dev) in enumerate(zip(
            (q.j0_right, q.j0_left, q.i0_low, q.i0_high),
            (q.j0_fl, q.j0_fr, q.i0_up, q.i0_down), sides,
        ))
    ]
    for c in halos:
        c.start()

    loads[4].wait()

    def factor(g, carry):
        B, Z = carry
        for j in reversed(range(GROUP)):
            bb, ss = pair(q.bi, g, j), pair(q.s, g, j)
            newB, newZ = [], []
            for m in range(2):
                row = g * 256 + 16 * j + 8 * m
                gb = GAIN * bb[m]
                o = 1.0 + gb * B[m]
                d = 1.0 / (o + gb * ss[m])
                hh = gb * d
                e = hh * ss[m]
                put(q.D, row, d)
                put(q.H, row, hh)
                od = o * d
                put(q.E, row, e)
                put(q.Y, row, d * Z[m])
                put(q.dX, row, od)
                newB.append(ss[m] * od)
                newZ.append(e * Z[m])
            B, Z = tuple(newB), tuple(newZ)
        return B, Z

    B, Z = each(factor, ((zero, zero), (one, one)), downward=True)

    def responses(g, carry):
        x, y = carry
        accs = [zero] * 3
        for j in range(GROUP):
            bb, ss, dd = pair(q.bi, g, j), pair(q.s, g, j), pair(q.D, g, j)
            od, dz = pair(q.dX, g, j), pair(q.Y, g, j)
            vals = []
            for m in range(2):
                sd, gb = ss[m] * dd[m], GAIN * bb[m]
                xg, yg = sd * x[m], sd * y[m] - dz[m]
                dx, dy = -(od[m] * x[m]), -(od[m] * y[m] + gb * dz[m])
                vals.append((gb * xg, gb * yg, xg, yg, dx, dy, ss[m] * dx, ss[m] * dy))
            vals = list(zip(*vals))
            x, y = vals[:2]
            for ref, val in zip((q.X, q.Y, q.XG, q.YG, q.dX, q.dY, q.P, q.Q), vals):
                put_pair(ref, g, j, val)
            for n, val in enumerate((ss, vals[6], vals[7])):
                edge_rows(g, j, val, q.is_low, q.is_high, n * K2)
                accs[n] = pack_columns(j, val, accs[n])
        for n in range(3):
            put(q.Oc, n * KJ + g * 8, accs[n])
        return x, y

    x, y = each(responses, ((one, one), (zero, zero)))
    for n, val in enumerate((x, y, Z, B)):
        for m in range(2):
            q.cmine[16 * n + 8 * m:16 * n + 8 * m + 8, :] = val[m]
            q.cgath[me, 16 * n + 8 * m:16 * n + 8 * m + 8, :] = val[m]
    consts = [
        remote(q.cmine, q.cgath.at[me], q.cs_s.at[o - 1], q.cs_r.at[o - 1], {"lev": lax.rem(me + o, nz)})
        for o in range(1, nz)
    ]
    for c in consts:
        c.start()
    for n in range(3):
        dense(q.Oc, n * KJ, q.js_right, q.js_left, n * KH)
    setups = four("is", "js", lambda n: q.hs_s.at[n], lambda n: q.hs_r.at[n])
    for c in setups:
        c.start()

    def crow(d, n):
        return q.cgath[d, 16 * n:16 * n + 16, :]

    for c in halos:
        c.wait()

    for n in range(groups // 2):
        fr = q.j0_fr[KH + 8 * n:KH + 8 * n + 8, :]
        fl = q.j0_fl[KH + 8 * n:KH + 8 * n + 8, :]
        for m in range(2):
            k = 16 * n + 8 * m
            q.vbr[k:k + 8, :] = roll(fr, -2 * m, 1)
            flg = roll(fl, -2 * m, 1)
            ab = q.own0[KJ + k:KJ + k + 8, :]
            av = q.own0[2 * KJ + k:2 * KJ + k + 8, :]
            q.hv[k:k + 8, :] = jnp.where(quad == 2, roll(flg, 2, 1), roll(av, 1, 1))
            q.hbj[k:k + 8, :] = CH * roll(jnp.where(quad == 1, flg, ab), 1, 1)
    open_up(q.j0_fl, q.j0_fr, 0, q.Hp.at[0], 0)

    def stagger(g, carry):
        packed = at(q.vbr, g * 8)
        for j in range(GROUP):
            xb, xu, xv = pair(q.bi, g, j), pair(q.us, g, j), pair(q.vs, g, j)
            for (val, dst, scale, f) in ((xu, q.us, 1.0, 2), (xb, q.bi, CH, 1)):
                r0, r1 = roll(val[0], 7, 0), roll(val[1], 7, 0)
                edge = q.i0_up[pl.ds(8 + f * K2 + g * 32 + 2 * j - 7, 8), :]
                put_pair(dst, g, j, (
                    scale * jnp.where(sub < 7, r0, r1), scale * jnp.where(sub < 7, r1, edge)
                ))
            for (val, dst, scale, first) in ((xv, q.vs, 1.0, 127), (xb, q.bj, CH, 126)):
                out = []
                for m in range(2):
                    n = 2 * j + m
                    out.append(scale * jnp.where(
                        lane == 127, roll(packed, first - 4 * n, 1), roll(val[m], 127, 1)
                    ))
                put_pair(dst, g, j, out)
        for r in range(4):
            row = g * 32 + 8 * r
            for (dst, f, scale) in ((q.hu, 2, 1.0), (q.hbi, 1, CH)):
                base = 8 + f * K2 + row
                below = q.i0_down[pl.ds(base + 1, 8), :]
                own = q.i0_low[pl.ds(base - 1, 8), :]
                put(dst, 8 + row, scale * jnp.where(sub % 2 == 0, below, own))
        return carry

    each(stagger, 0)

    loads[5].wait()

    def interface():
        beta = jnp.zeros((16, 128), F32)
        betas, rs, zbrs, lams = ([None] * nz for _ in range(4))
        for d in range(nz - 1, -1, -1):
            betas[d] = beta
            rs[d] = 1.0 / (1.0 - crow(d, 1) * beta)
            zbrs[d] = crow(d, 2) * beta * rs[d]
            lams[d] = crow(d, 2) + zbrs[d] * crow(d, 1)
            beta = crow(d, 3) + zbrs[d] * crow(d, 0)
            if d == 0:
                last = beta
        tops = [last] + betas[:-1]
        psi = jnp.zeros((16, 128), F32)
        psis, r2s, xrs, xrps = ([None] * nz for _ in range(4))
        for d in range(nz):
            xrs[d] = crow(d, 0) / (1.0 - psi * crow(d, 3))
            xrps[d] = xrs[d] * psi
            psis[d] = psi
            r2s[d] = 1.0 / (1.0 - psi * tops[d])
            psi = crow(d, 1) + xrps[d] * crow(d, 2)

        def pick(vals):
            out = vals[0]
            for d in range(1, nz):
                out = jnp.where(me == d, vals[d], out)
            return out

        br = [betas[d] * rs[d] for d in range(nz)]
        brx = [br[d] * crow(d, 0) for d in range(nz)]
        for n, vals in enumerate((xrps, zbrs, [r2s[d] * psis[d] for d in range(nz)], br, brx)):
            q.mine[16 * n:16 * n + 16, :] = pick(vals)
        for L in range(nz):
            part = r2s[L]
            for d in range(L - 1, -1, -1):
                q.ctab[L * nz + d, 0:16, :] = part
                q.ctab[L * nz + d, 16:32, :] = brx[L] * part
                part = part * xrs[d]
            part, gain = jnp.ones((16, 128), F32), 1.0 + br[L] * crow(L, 1)
            rpl = r2s[L] * psis[L] * lams[L]
            for d in range(L + 1, nz):
                cw = rpl * part
                q.ctab[L * nz + d, 0:16, :] = cw
                q.ctab[L * nz + d, 16:32, :] = part * gain + brx[L] * cw
                part = part * lams[d]

    def halves(x):
        return x[0:8], x[8:16]

    def pack_pair(wx, px):
        (w0, w1), (p0, p1) = halves(wx), halves(px)
        acc = roll(w0, 2, 1)
        for n, val in ((1, w1), (2, p0), (3, p1)):
            acc = jnp.where(lane // 4 == n, roll(val, 4 * n + 2, 1), acc)
        return acc

    def spread(t):
        z = jnp.where(lane < 16, t, 0.0)
        for n in (16, 32, 64):
            z = z + roll(z, n, 1)
        r = roll(z, 8, 1)
        return jnp.where(lane % 16 < 8, z, r), jnp.where(lane % 16 < 8, r, z)

    def insert(v, base):
        return roll(v, 126 - base, 1)

    def level_sums():
        for k in range(0, K2, 8):
            own, above = q.i0_high[pl.ds(9 + K2 + k, 8), :], q.i0_up[pl.ds(7 + K2 + k, 8), :]
            q.bih[k:k + 8, :] = CH * jnp.where(sub % 2 == 0, own, above)
            for n in range(2):
                q.mi[n * K2 + k:n * K2 + k + 8, :] = (
                    q.hbi[8 + k:16 + k, :] * q.is_down[(n + 1) * K2 + k:(n + 1) * K2 + k + 8, :]
                )
        for k in range(0, KJ, 8):
            bjo = CH * jnp.where(quad == 0, roll(q.own0[KJ + k:KJ + k + 8, :], -1, 1), q.vbr[k:k + 8, :])
            for n in range(2):
                h, o = (r[(n + 1) * KJ + k:(n + 1) * KJ + k + 8, :] for r in (q.Hc, q.Oc))
                q.cj[n * KJ + k:n * KJ + k + 8, :] = jnp.where(quad < 2, h, q.hbj[k:k + 8, :] * h)
                q.wo[n * KJ + k:n * KJ + k + 8, :] = CH * jnp.where(quad < 2, o * bjo, o)

        def add(acc, n, m, value):
            acc[n][m] = acc[n][m] + value

        def along_i(g, carry):
            acc = [list(c) for c in carry]
            for j in range(GROUP):
                pq = (pair(q.P, g, j), pair(q.Q, g, j))
                bb = pair(q.bi, g, j)
                ahead, behind = [], []
                for n, (g0, g1) in enumerate(pq):
                    r0, r1 = roll(g0, 6, 0), roll(g1, 6, 0)
                    edge = q.is_up[pl.ds((n + 1) * K2 + g * 32 + 2 * j - 6, 8), :]
                    ahead.append((
                        bb[0] * jnp.where(sub < 6, r0, r1), bb[1] * jnp.where(sub < 6, r1, edge)
                    ))
                    r0, r1 = roll(bb[0] * g0, 2, 0), roll(bb[1] * g1, 2, 0)
                    edge = q.mi[pl.ds(n * K2 + g * 32 + 2 * j, 8), :]
                    behind.append((jnp.where(sub < 2, edge, r0), jnp.where(sub < 2, r0, r1)))
                for f in range(2):
                    for m in range(2):
                        cf = CH * pq[f][m]
                        for n in range(2):
                            add(acc, 2 * f + n, m, cf * ahead[n][m])
                            add(acc, 4 + 2 * f + n, m, cf * behind[n][m])
            return tuple(tuple(c) for c in acc)

        def along_j(g, carry):
            acc = [list(c) for c in carry]
            cs = [at(q.cj, n * KJ + g * 8) for n in range(2)]
            for j in range(GROUP):
                pq = (pair(q.P, g, j), pair(q.Q, g, j))
                bb = pair(q.bj, g, j)
                for m in range(2):
                    ahead, behind = [], []
                    for n in range(2):
                        edge = insert(cs[n], 4 * (2 * j + m))
                        ahead.append(bb[m] * jnp.where(lane >= 126, edge, roll(pq[n][m], 126, 1)))
                        behind.append(jnp.where(lane < 2, edge, roll(bb[m] * pq[n][m], 2, 1)))
                    for f in range(2):
                        cf = CH * pq[f][m]
                        for n in range(2):
                            add(acc, 2 * f + n, m, cf * ahead[n])
                            add(acc, 4 + 2 * f + n, m, cf * behind[n])
            return tuple(tuple(c) for c in acc)

        def centre(g, carry):
            acc = [list(c) for c in carry]
            hb = at(q.hbj, g * 8)
            for j in range(GROUP):
                bbi, bbj = pair(q.bi, g, j), pair(q.bj, g, j)
                pp, qq, dx, dy = (pair(r, g, j) for r in (q.P, q.Q, q.dX, q.dY))
                xx, yy, xg, yg = (pair(r, g, j) for r in (q.X, q.Y, q.XG, q.YG))
                r0, r1 = roll(bbi[0], 2, 0), roll(bbi[1], 2, 0)
                edge = at(q.hbi, 8 + g * 32 + 2 * j, False)
                bim = (jnp.where(sub < 2, edge, r0), jnp.where(sub < 2, r0, r1))
                for m in range(2):
                    bjm = jnp.where(lane < 2, insert(hb, 4 * (2 * j + m)), roll(bbj[m], 2, 1))
                    sb = CH * ((bbi[m] + bim[m]) + (bbj[m] + bjm))
                    fx, fy = dx[m] - sb * pp[m], dy[m] - sb * qq[m]
                    add(acc, 0, m, pp[m] * fx - xg[m] * xx[m])
                    add(acc, 1, m, qq[m] * fx - xg[m] * yy[m])
                    add(acc, 2, m, qq[m] * fy - yg[m] * yy[m])
            return tuple(tuple(c) for c in acc)

        first = 0
        for body, count in ((centre, 3), (along_i, 8), (along_j, 8)):
            for n, val in enumerate(each(body, ((zero, zero),) * count)):
                q.coef[first + n, 0:8, :], q.coef[first + n, 8:16, :] = val
            first += count

    def base_rows(t):
        def body(g, carry):
            A, W, before = carry
            for j in range(GROUP):
                star, w0, ss, uu, vv, bbi, bbj, dx, dy, pp, qq, xg, yg = (
                    pair(r, g, j) for r in (
                        q.ps, w, q.s, q.us, q.vs, q.bi, q.bj, q.dX, q.dY, q.P, q.Q, q.XG, q.YG
                    )
                )
                pt = tuple(star[m] - ss[m] * (w0[m] - before[m]) for m in range(2))
                r0, r1 = roll(pt[0], 6, 0), roll(pt[1], 6, 0)
                pi = (jnp.where(sub < 6, r0, r1), jnp.where(sub < 6, r1, 0.0))
                un = tuple(uu[m] - bbi[m] * (pi[m] - pt[m]) for m in range(2))
                r0, r1 = roll(un[0], 2, 0), roll(un[1], 2, 0)
                um = (jnp.where(sub < 2, 0.0, r0), jnp.where(sub < 2, r0, r1))
                newA, newW = [], []
                for m in range(2):
                    pj = jnp.where(lane >= 126, 0.0, roll(pt[m], 126, 1))
                    vn = vv[m] - bbj[m] * (pj - pt[m])
                    vm = jnp.where(lane < 2, 0.0, roll(vn, 2, 1))
                    div = CH * ((un[m] - um[m]) + (vn - vm))
                    newA.append(A[m] + (pp[m] * div - (dx[m] * pt[m] + xg[m] * w0[m])))
                    newW.append(W[m] + (qq[m] * div - (dy[m] * pt[m] + yg[m] * w0[m])))
                A, W, before = tuple(newA), tuple(newW), w0
            return A, W, before

        A, W, _ = each(body, ((zero, zero),) * 3)
        return list(A), list(W)

    def rows_without(src, const, dst):
        before = zero
        for k in range(0, K2, 8):
            star, w0, cs = src[k:k + 8, :], src[K2 + k:K2 + k + 8, :], const[k:k + 8, :]
            now = roll(w0, 2, 0)
            dst[k:k + 8, :] = star - cs * (w0 - jnp.where(sub < 2, before, now))
            before = now

    def columns_without(src, const, dst):
        before = zero
        for k in range(0, KJ, 8):
            star, w0, cs = src[k:k + 8, :], src[KJ + k:KJ + k + 8, :], const[k:k + 8, :]
            now = roll(w0, 8, 1)
            dst[k:k + 8, :] = star - cs * (w0 - jnp.where(lane < 8, before, now))
            before = now

    def halo_rows(t, A, W):
        lows, highs, cols = [zero, zero], [zero, zero], [zero, zero]
        for k in range(0, K2, 8):
            hu_new = q.hu[8 + k:16 + k, :] - q.hbi[8 + k:16 + k, :] * (
                q.b_low[t, k:k + 8, :] - q.b_down[t, k:k + 8, :]
            )
            high = q.bih[k:k + 8, :] * q.b_up[t, k:k + 8, :]
            for n in range(2):
                r = (n + 1) * K2 + k
                lows[n] = lows[n] + q.is_low[r:r + 8, :] * hu_new
                highs[n] = highs[n] + q.is_high[r:r + 8, :] * high
        for k in range(0, KJ, 8):
            hp = q.Hb[t, k:k + 8, :]
            c = jnp.where(
                quad < 2, hp, q.hv[k:k + 8, :] - q.hbj[k:k + 8, :] * (q.Ob[t, k:k + 8, :] - hp)
            )
            for n in range(2):
                cols[n] = cols[n] + q.wo[n * KJ + k:n * KJ + k + 8, :] * c
        for n, rows in enumerate((A, W)):
            low, high, col = lows[n], highs[n], cols[n]
            for r in (4, 2):
                low, high = low + roll(low, r, 0), high + roll(high, r, 0)
            for r in (64, 32, 16, 8):
                col = col + roll(col, r, 1)
            rows[0] = rows[0] - jnp.where(sub < 2, CH * low, 0.0)
            rows[1] = rows[1] - jnp.where(sub >= 6, CH * high, 0.0)
            for m in range(2):
                rows[m] = rows[m] - jnp.where((lane >= 126) | (lane < 2), insert(col, 4 * m), 0.0)

    def send_round(t, W0, A0):
        final = t == SUBSTEPS - 1
        wa, aw, r2psi, br, brx = (q.mine[16 * n:16 * n + 16, :] for n in range(5))
        up_row, down_row = W0 + wa * A0, A0 + aw * W0
        q.fmine[t, 0], q.fmine[t, 1] = up_row, down_row
        sends = []
        wb_own = r2psi * down_row
        pa_own = br * W0 + brx * wb_own
        for o in sorted(range(nz), key=lambda o: -min(o, nz - o)):
            L = lax.rem(me + o, nz)
            if not final:
                if o:
                    row = jnp.where(L > me, up_row, down_row)
                    wc, pc = (q.ctab[L * nz + me, 16 * n:16 * n + 16, :] * row for n in range(2))
                else:
                    wc, pc = wb_own, pa_own
                q.jc[t, o] = pack_pair(wc, pc)
                q.ic_low[t, o] = jnp.where(sub < 2, wc[0:8], roll(pc[0:8], 2, 0))
                q.ic_high[t, o] = jnp.where(sub < 2, roll(wc[8:16], 2, 0), roll(pc[8:16], 4, 0))
                for n, (a, b) in enumerate((
                    (q.jc, q.jc_fl), (q.jc, q.jc_fr), (q.ic_low, q.ic_up), (q.ic_high, q.ic_down)
                )):
                    c = remote(
                        a.at[t, o], b.at[t, me], q.hc_s.at[t, n, o], q.hc_r.at[t, n, o],
                        {**sides[n], "lev": L},
                    )
                    c.start()
                    sends.append(c)
            if o:
                c = remote(
                    q.fmine.at[t, lax.div(me + o, nz)], q.fgath.at[t, me],
                    q.ls_s.at[t, o - 1], q.ls_r.at[t, o - 1], {"lev": L},
                )
                c.start()
                sends.append(c)
        return sends, wb_own, pa_own

    for t in range(SUBSTEPS):
        final = t == SUBSTEPS - 1
        if t:
            each(implicit, wb2)

            def add_columns(src, const, wp, dst):
                for k in range(0, KJ, 8):
                    dst[k:k + 8, :] = src[k:k + 8, :] - (
                        const[KJ + k:KJ + k + 8, :] * wp[0] + const[2 * KJ + k:2 * KJ + k + 8, :] * wp[1]
                    )

            def add_rows(src, const, v, dst):
                z = jnp.where(sub < 4, v, roll(v, 4, 0))
                r = roll(z, 2, 0)
                ws, ps_ = jnp.where(sub % 4 < 2, z, r), jnp.where(sub % 4 < 2, r, z)
                for k in range(0, K2, 8):
                    dst[8 + k:16 + k, :] = src[k:k + 8, :] - (
                        const[K2 + k:K2 + k + 8, :] * ws + const[2 * K2 + k:2 * K2 + k + 8, :] * ps_
                    )

            add_columns(q.Hb.at[t - 1], q.Hc, spread(halo_j), q.Hp.at[t])
            add_columns(q.Ob.at[t - 1], q.Oc, spread(pack_pair(wb, pa)), q.Op.at[t])
            low = jnp.where(sub < 2, wb[0:8], roll(pa[0:8], 2, 0))
            add_rows(q.b_up.at[t - 1], q.is_up, halo_up, q.p_up.at[t])
            add_rows(q.b_down.at[t - 1], q.is_down, halo_down, q.p_down.at[t])
            add_rows(q.b_low.at[t - 1], q.is_low, low, q.p_low.at[t])
        i_up, i_down, i_low = (
            (q.i0_up, q.i0_down, q.i0_low) if t == 0
            else (q.p_up.at[t], q.p_down.at[t], q.p_low.at[t])
        )
        own_p = q.own0 if t == 0 else q.Op.at[t]
        halo_p = q.Hp.at[t]

        for k in range(0, KJ, 8):
            hp = halo_p[k:k + 8, :]
            hv_new = q.hv[k:k + 8, :] - q.hbj[k:k + 8, :] * (own_p[k:k + 8, :] - hp)
            q.hv[k:k + 8, :] = hv_new
            q.C[k:k + 8, :] = jnp.where(quad < 2, hp, hv_new)

        def explicit(g, A):
            for r in range(4):
                row = g * 32 + 8 * r
                put(q.hu, 8 + row, at(q.hu, 8 + row) - at(q.hbi, 8 + row) * (
                    at(i_low, 8 + row) - at(i_down, 8 + row)
                ))
            c = at(q.C, g * 8)
            acc = zero
            for j in reversed(range(GROUP)):
                pp, uu, vv, ww = pair(p, g, j), pair(q.us, g, j), pair(q.vs, g, j), pair(w, g, j)
                bbi, bbj, ss = pair(q.bi, g, j), pair(q.bj, g, j), pair(q.s, g, j)
                ee, dd, hh = pair(q.E, g, j), pair(q.D, g, j), pair(q.H, g, j)
                r0, r1 = roll(pp[0], 6, 0), roll(pp[1], 6, 0)
                edge = at(i_up, 8 + g * 32 + 2 * j - 6, False)
                pi = (jnp.where(sub < 6, r0, r1), jnp.where(sub < 6, r1, edge))
                un = tuple(uu[m] - bbi[m] * (pi[m] - pp[m]) for m in range(2))
                put_pair(q.us, g, j, un)
                r0, r1 = roll(un[0], 2, 0), roll(un[1], 2, 0)
                edge = at(q.hu, 8 + g * 32 + 2 * j, False)
                um = (jnp.where(sub < 2, edge, r0), jnp.where(sub < 2, r0, r1))
                newA, hs, pss, vn = [], [], [], []
                for m in range(2):
                    edge = roll(c, 126 - 4 * (2 * j + m), 1)
                    pj = jnp.where(lane >= 126, edge, roll(pp[m], 126, 1))
                    v_new = vv[m] - bbj[m] * (pj - pp[m])
                    vm = jnp.where(lane < 2, edge, roll(v_new, 2, 1))
                    star = pp[m] - (CH * ss[m]) * ((un[m] - um[m]) + (v_new - vm))
                    dw = dd[m] * ww[m]
                    hs.append(dw + hh[m] * (star - A[m]))
                    newA.append(ee[m] * A[m] + ((star - ee[m] * star) - ss[m] * dw))
                    pss.append(star)
                    vn.append(v_new)
                put_pair(q.vs, g, j, vn)
                put_pair(q.ps, g, j, pss)
                put_pair(q.h, g, j, hs)
                if not final:
                    edge_rows(g, j, pss, q.iw_low.at[t], q.iw_high.at[t], 0)
                    acc = pack_columns(j, pss, acc)
                A = tuple(newA)
            if not final:
                put(q.Ow.at[t], g * 8, acc)
            return A

        A = each(explicit, (zero, zero), downward=True)

        def forward(g, x):
            acc = zero
            for j in range(GROUP):
                ee, hh = pair(q.E, g, j), pair(q.h, g, j)
                x = tuple(ee[m] * x[m] + hh[m] for m in range(2))
                put_pair(w, g, j, x)
                if not final:
                    edge_rows(g, j, x, q.iw_low.at[t], q.iw_high.at[t], K2)
                    acc = pack_columns(j, x, acc)
            if not final:
                put(q.Ow.at[t], KJ + g * 8, acc)
            return x

        x = each(forward, (zero, zero))
        if t == 0:
            for c in consts:
                c.wait()
            interface()
            A0, W0 = (jnp.concatenate(n, 0) for n in (A, x))
            sends, wb_own, pa_own = send_round(0, W0, A0)
        if not final:
            for n in range(2):
                dense(q.Ow.at[t], n * KJ, q.jw_right.at[t], q.jw_left.at[t], n * KH)
            works = four("iw", "jw", lambda n: q.hw_s.at[t, n], lambda n: q.hw_r.at[t, n], lambda r: r.at[t])
            for c in works:
                c.start()
            A1, W1 = base_rows(t)
            if t == 0:
                for c in setups:
                    c.wait()
                for n in range(3):
                    open_up(q.js_fl, q.js_fr, n * KH, q.Hc, n * KJ)
                level_sums()
            columns_without(q.Ow.at[t], q.Oc, q.Ob.at[t])
            rows_without(q.iw_low.at[t], q.is_low, q.b_low.at[t])
            for c in works:
                c.wait()
            for n in range(2):
                open_up(q.jw_fl.at[t], q.jw_fr.at[t], n * KH, q.Hw.at[t], n * KJ)
            columns_without(q.Hw.at[t], q.Hc, q.Hb.at[t])
            rows_without(q.iw_up.at[t], q.is_up, q.b_up.at[t])
            rows_without(q.iw_down.at[t], q.is_down, q.b_down.at[t])
            halo_rows(t, A1, W1)

        if final:
            def emit(g, carry):
                hvg = at(q.hv, pl.multiple_of(g * 8, 8))
                for j in range(GROUP):
                    uu, vv = pair(q.us, g, j), pair(q.vs, g, j)
                    r0, r1 = roll(uu[0], 1, 0), roll(uu[1], 1, 0)
                    edge = at(q.hu, 8 + g * 32 + 2 * j + 1, False)
                    put_pair(uo, g, j, (jnp.where(sub < 1, edge, r0), jnp.where(sub < 1, r0, r1)))
                    put_pair(vo, g, j, [
                        jnp.where(
                            lane == 0, roll(hvg, 125 - 4 * (2 * j + m), 1), roll(vv[m], 1, 1)
                        )
                        for m in range(2)
                    ])
                return carry

            each(emit, 0)
        for c in sends:
            c.wait()

        wb, pa = wb_own, pa_own
        for o in range(1, nz):
            d = lax.rem(me + o, nz)
            row = q.fgath[t, d]
            wb = wb + q.ctab[me * nz + d, 0:16, :] * row
            pa = pa + q.ctab[me * nz + d, 16:32, :] * row
        wb2, pa2 = halves(wb), halves(pa)

        if not final:
            fr, fl, halo_up, halo_down = (
                functools.reduce(lambda a, b: a + b, [ref[t, d] for d in range(nz)])
                for ref in (q.jc_fr, q.jc_fl, q.ic_up, q.ic_down)
            )
            halo_j = jnp.where(quad < 2, roll(fr, -2, 1), roll(fl, 2, 1))
            stencil = []
            for n, v in enumerate((wb2, pa2)):
                a0, a1, b0, b1 = (roll(v[m], k, 0) for k in (6, 2) for m in range(2))
                above, below = roll(halo_up, 6 - 2 * n, 0), roll(halo_down, -2 * n, 0)
                edges = [insert(halo_j, 8 * n + 4 * m) for m in range(2)]
                stencil.append((
                    v,
                    (jnp.where(sub < 6, a0, a1), jnp.where(sub < 6, a1, above)),
                    (jnp.where(sub < 2, below, b0), jnp.where(sub < 2, b0, b1)),
                    tuple(jnp.where(lane >= 126, edges[m], roll(v[m], 126, 1)) for m in range(2)),
                    tuple(jnp.where(lane < 2, edges[m], roll(v[m], 2, 1)) for m in range(2)),
                ))
            rows = []
            for f, base in enumerate((A1, W1)):
                halves_ = []
                for m in range(2):
                    terms = [base[m]]
                    for n in range(2):
                        for k in range(5):
                            c = f + n if k == 0 else 3 + 4 * (k - 1) + 2 * f + n
                            terms.append(q.coef[c, 8 * m:8 * m + 8, :] * stencil[n][k][m])
                    while len(terms) > 1:
                        terms = [
                            sum(terms[k + 1:k + 2], terms[k]) for k in range(0, len(terms), 2)
                        ]
                    halves_.append(terms[0])
                rows.append(jnp.concatenate(halves_, 0))
            sends, wb_own, pa_own = send_round(t + 1, rows[1], rows[0])

        def implicit(g, wprev, wb2=wb2, pa2=pa2):
            for j in range(GROUP):
                w0, xx, yy = pair(w, g, j), pair(q.X, g, j), pair(q.Y, g, j)
                ss, star = pair(q.s, g, j), pair(q.ps, g, j)
                wn = tuple(w0[m] + xx[m] * wb2[m] + yy[m] * pa2[m] for m in range(2))
                pn = tuple(star[m] - ss[m] * (wn[m] - wprev[m]) for m in range(2))
                put_pair(w, g, j, wn)
                put_pair(p, g, j, pn)
                wprev = wn
            return wprev

    each(implicit, wb2)


def store(u, v, w, p, u_out, v_out, w_out, p_out, sem):
    copies = [
        pltpu.make_async_copy(src, dst, sem.at[n])
        for n, (src, dst) in enumerate(((u, u_out), (v, v_out), (w, w_out), (p, p_out)))
    ]
    for c in copies:
        c.start()
    for c in copies:
        c.wait()


def solution(mesh):
    nx, ny, nz = (mesh.shape[a] for a in ("gx", "gy", "lev"))

    def shards(*fields):
        K, I, J = fields[0].shape
        assert I == 16 and J == 128 and K % (2 * GROUP) == 0
        R = K * I
        full = pltpu.VMEM((R, J), F32)
        held = scratch(K, J, nz)
        outs = pl.pallas_call(
            functools.partial(kernel, tuple(held), K, nx, ny, nz),
            out_shape=[full] * 4,
            in_specs=[pl.BlockSpec(memory_space=pl.ANY)] * 6,
            out_specs=[pl.BlockSpec(memory_space=pltpu.VMEM)] * 4,
            scratch_shapes=list(held.values()),
            compiler_params=pltpu.CompilerParams(collective_id=0, has_side_effects=True),
        )(*(f.reshape(R, J) for f in fields))
        outs = pl.pallas_call(
            store,
            out_shape=[jax.ShapeDtypeStruct((R, J), F32)] * 4,
            in_specs=[pl.BlockSpec(memory_space=pltpu.VMEM)] * 4,
            out_specs=[pl.BlockSpec(memory_space=pl.ANY)] * 4,
            scratch_shapes=[pltpu.SemaphoreType.DMA((4,))],
        )(*(pltpu.with_memory_space_constraint(o, pltpu.VMEM) for o in outs))
        return tuple(o.reshape(K, I, J) for o in outs)

    spec = P("lev", "gx", "gy")
    return jax.shard_map(
        shards, mesh=mesh, in_specs=(spec,) * 6, out_specs=(spec,) * 4, check_vma=False
    )
```

```python
import functools
from types import SimpleNamespace

import jax
import jax.numpy as jnp
from jax import lax
from jax.experimental import pallas as pl
from jax.experimental.pallas import tpu as pltpu
from jax.sharding import PartitionSpec as P

SUBSTEPS = 3
CH = 0.3
GAIN = 4096.0
MESH = pl.DeviceIdType.MESH
GROUP = 16
F32 = jnp.float32


def scratch(K, J, nz):
    R, T, KJ, K2, KH = 16 * K, SUBSTEPS, 8 * (K // GROUP), 2 * K, 4 * (K // GROUP)
    V = lambda *s: pltpu.VMEM((*s, J), F32)
    D = lambda *s: pltpu.SemaphoreType.DMA(s)
    m = max(nz - 1, 1)
    s = {n: V(R) for n in (
        "us", "vs", "s", "bi", "bj", "E", "D", "H", "X", "Y", "ps", "h",
        "dX", "dY", "P", "Q", "XG", "YG",
    )}
    s |= {n: V(3 * K2 + 16) for n in ("i0_low", "i0_high", "i0_up", "i0_down")}
    s |= {n: V(2 * KH) for n in ("j0_right", "j0_left", "j0_fl", "j0_fr")}
    s |= {n: V(3 * K2) for n in ("is_low", "is_high", "is_up", "is_down")}
    s |= {n: V(3 * KH) for n in ("js_right", "js_left", "js_fl", "js_fr")}
    s |= {n: V(T, 2 * K2) for n in ("iw_low", "iw_high", "iw_up", "iw_down")}
    s |= {n: V(T, 2 * KH) for n in ("jw_right", "jw_left", "jw_fl", "jw_fr")}
    s |= {n: V(T, nz, 8) for n in ("ic_low", "ic_high", "ic_up", "ic_down", "jc", "jc_fl", "jc_fr")}
    s |= {n: V(T, K2 + 16) for n in ("p_up", "p_down", "p_low")}
    s |= {n: V(T, K2) for n in ("b_up", "b_down", "b_low")}
    s |= {n: V(K2) for n in ("bih",)}
    s |= {n: V(2 * K2 + 16) for n in ("mi",)}
    s |= {n: V(2 * KJ) for n in ("cj", "wo")}
    s |= {"coef": V(19, 16)}
    s |= {n: V(3 * KJ) for n in ("own0",)}
    s |= {n: V(KJ) for n in ("hv", "hbj")}
    s |= {n: V(3 * KJ) for n in ("Hc", "Oc")}
    s |= {n: V(T, 2 * KJ) for n in ("Hw", "Ow")}
    s |= {n: V(T, KJ) for n in ("Hp", "Op", "Hb", "Ob")}
    s |= {n: V(K2 + 16) for n in ("hu", "hbi")}
    s |= {"cmine": V(48), "cgath": V(nz, 48), "fmine": V(T, 2, 16), "fgath": V(T, nz, 16)}
    s |= {"ctab": V(nz * nz, 32), "mine": V(80)}
    s |= {"in_sem": D(6)}
    for n in ("h0", "hs"):
        s |= {n + "_s": D(4), n + "_r": D(4)}
    s |= {"hw_s": D(T, 4), "hw_r": D(T, 4), "hc_s": D(T, 4, nz), "hc_r": D(T, 4, nz)}
    s |= {"cs_s": D(m), "cs_r": D(m), "ls_s": D(T, m), "ls_r": D(T, m)}
    return s


def kernel(names, K, nx, ny, nz, u_in, v_in, w_in, p_in, b_in, s_in, uo, vo, w, p, *refs):
    q = SimpleNamespace(**dict(zip(names, refs)))
    gx, gy, me = lax.axis_index("gx"), lax.axis_index("gy"), lax.axis_index("lev")
    up, down = lax.rem(gx + 1, nx), lax.rem(gx + nx - 1, nx)
    right, left = lax.rem(gy + 1, ny), lax.rem(gy + ny - 1, ny)
    groups = K // GROUP
    K2, KJ, KH = 2 * K, 8 * (K // GROUP), 4 * (K // GROUP)
    sides = ({"gy": right}, {"gy": left}, {"gx": down}, {"gx": up})

    loads = []
    for n, (src, dst) in enumerate(
        ((p_in, p), (b_in, q.bi), (v_in, q.vs), (s_in, q.s), (u_in, q.us), (w_in, w))
    ):
        c = pltpu.make_async_copy(src, dst, q.in_sem.at[n])
        c.start()
        loads.append(c)

    barrier = pltpu.get_barrier_semaphore()
    for dev in sides:
        pl.semaphore_signal(barrier, inc=1, device_id=dev, device_id_type=MESH)
    for o in range(1, nz):
        pl.semaphore_signal(
            barrier, inc=1, device_id={"lev": lax.rem(me + o, nz)}, device_id_type=MESH
        )

    lane = lax.broadcasted_iota(jnp.int32, (8, 128), 1)
    sub = lax.broadcasted_iota(jnp.int32, (8, 128), 0)
    quad = lane % 4
    zero = jnp.zeros((8, 128), F32)
    one = jnp.ones((8, 128), F32)

    def roll(x, shift, axis):
        shift = shift % x.shape[axis]
        return x if shift == 0 else pltpu.roll(x, shift, axis)

    def at(ref, row, aligned=True):
        return ref[pl.ds(pl.multiple_of(row, 8) if aligned else row, 8), :]

    def put(ref, row, value):
        ref[pl.ds(pl.multiple_of(row, 8), 8), :] = value

    def each(body, carry=None, downward=False):
        def step(n, c):
            g = groups - 1 - n if downward else n
            return body(g, c)
        return lax.fori_loop(0, groups, step, carry)

    def pair(ref, g, j):
        return at(ref, g * 256 + 16 * j), at(ref, g * 256 + 16 * j + 8)

    def put_pair(ref, g, j, value):
        put(ref, g * 256 + 16 * j, value[0])
        put(ref, g * 256 + 16 * j + 8, value[1])

    def edge_rows(g, j, x, low, high, base):
        row = base + g * 32 + 2 * j
        low[pl.ds(row, 2), :] = x[0][0:2]
        if high is not None:
            high[pl.ds(row, 2), :] = x[1][6:8]

    def pack_columns(j, x, acc):
        for half in range(2):
            n = 2 * j + half
            acc = jnp.where(lane // 4 == n, roll(x[half], 4 * n + 2, 1), acc)
        return acc

    def remote(src, dst, ss, rs, dev):
        return pltpu.make_async_remote_copy(
            src_ref=src, dst_ref=dst, send_sem=ss, recv_sem=rs, device_id=dev, device_id_type=MESH
        )

    def dense(own, base, to_right, to_left, row):
        for n in range(groups // 2):
            a, b = (own[base + 16 * n + 8 * m:base + 16 * n + 8 * m + 8, :] for m in range(2))
            to_right[row + 8 * n:row + 8 * n + 8, :] = jnp.where(quad < 2, a, roll(b, 2, 1))
            to_left[row + 8 * n:row + 8 * n + 8, :] = jnp.where(quad < 2, roll(a, -2, 1), b)

    def open_up(fl, fr, row, dst, base):
        for n in range(groups // 2):
            a, b = fl[row + 8 * n:row + 8 * n + 8, :], fr[row + 8 * n:row + 8 * n + 8, :]
            for m in range(2):
                k = base + 16 * n + 8 * m
                dst[k:k + 8, :] = jnp.where(
                    quad < 2, roll(b, -2 * m, 1), roll(a, 2, 1) if m == 0 else a
                )

    for c in loads[:3]:
        c.wait()

    def first_pack(g, carry):
        accp = accb = accv = zero
        for j in range(GROUP):
            accp = pack_columns(j, pair(p, g, j), accp)
            accb = pack_columns(j, pair(q.bi, g, j), accb)
            accv = pack_columns(j, pair(q.vs, g, j), accv)
        put(q.own0, g * 8, accp)
        put(q.own0, KJ + g * 8, accb)
        put(q.own0, 2 * KJ + g * 8, accv)
        return carry

    each(first_pack, 0)

    dense(q.own0, 0, q.j0_right, q.j0_left, 0)
    for n in range(groups // 2):
        rights, lefts = [], []
        for m in range(2):
            k = 16 * n + 8 * m
            ab = q.own0[KJ + k:KJ + k + 8, :]
            av = q.own0[2 * KJ + k:2 * KJ + k + 8, :]
            rights.append(jnp.where(quad == 0, roll(av, -1, 1), ab))
            lefts.append(jnp.where(quad == 0, roll(av, -2, 1), roll(ab, -1, 1)))
        k = KH + 8 * n
        for ref, (a, b) in ((q.j0_right, rights), (q.j0_left, lefts)):
            ref[k:k + 8, :] = jnp.where(quad < 2, a, roll(b, 2, 1))

    pl.semaphore_wait(barrier, 4 + nz - 1)

    def four(i, j, ss, rs, at_=lambda r: r):
        pairs = (
            (j + "_right", j + "_fl"), (j + "_left", j + "_fr"),
            (i + "_low", i + "_up"), (i + "_high", i + "_down"),
        )
        return [
            remote(at_(getattr(q, a)), at_(getattr(q, b)), ss(n), rs(n), dev)
            for n, ((a, b), dev) in enumerate(zip(pairs, sides))
        ]

    rows0 = pl.ds(8, 3 * K2)
    halos = [
        remote(
            a if n < 2 else a.at[rows0], b if n < 2 else b.at[rows0],
            q.h0_s.at[n], q.h0_r.at[n], dev,
        )
        for n, (a, b, dev) in enumerate(zip(
            (q.j0_right, q.j0_left, q.i0_low, q.i0_high),
            (q.j0_fl, q.j0_fr, q.i0_up, q.i0_down), sides,
        ))
    ]
    for c in halos[:2]:
        c.start()

    loads[4].wait()

    def first_rows(g, carry):
        for j in range(GROUP):
            for n, ref in enumerate((p, q.bi, q.us)):
                edge_rows(g, j, pair(ref, g, j), q.i0_low, q.i0_high, 8 + n * K2)
        return carry

    each(first_rows, 0)
    for c in halos[2:]:
        c.start()

    loads[3].wait()

    def factor(g, carry):
        B, Z, yend = carry
        for j in reversed(range(GROUP)):
            bb, ss = pair(q.bi, g, j), pair(q.s, g, j)
            newB, newZ, newy = [], [], []
            for m in range(2):
                row = g * 256 + 16 * j + 8 * m
                gb = GAIN * bb[m]
                o = 1.0 + gb * B[m]
                d = 1.0 / (o + gb * ss[m])
                hh = gb * d
                e = hh * ss[m]
                put(q.D, row, d)
                put(q.H, row, hh)
                od = o * d
                put(q.E, row, e)
                dz = d * Z[m]
                put(q.Y, row, dz)
                put(q.dX, row, od)
                newB.append(ss[m] * od)
                newZ.append(e * Z[m])
                newy.append(yend[m] - (gb * dz) * Z[m])
            B, Z, yend = tuple(newB), tuple(newZ), tuple(newy)
        return B, Z, yend

    B, Z, yend = each(factor, ((zero, zero), (one, one), (zero, zero)), downward=True)
    for n, val in enumerate((Z, yend, B)):
        for m in range(2):
            q.cmine[16 * n + 8 * m:16 * n + 8 * m + 8, :] = val[m]
            q.cgath[me, 16 * n + 8 * m:16 * n + 8 * m + 8, :] = val[m]
    consts = [
        remote(q.cmine, q.cgath.at[me], q.cs_s.at[o - 1], q.cs_r.at[o - 1], {"lev": lax.rem(me + o, nz)})
        for o in range(1, nz)
    ]
    for c in consts:
        c.start()

    def responses(g, carry):
        x, y = carry
        accs = [zero] * 3
        for j in range(GROUP):
            bb, ss, dd = pair(q.bi, g, j), pair(q.s, g, j), pair(q.D, g, j)
            od, dz = pair(q.dX, g, j), pair(q.Y, g, j)
            vals = []
            for m in range(2):
                sd, gb = ss[m] * dd[m], GAIN * bb[m]
                xg, yg = sd * x[m], sd * y[m] - dz[m]
                dx, dy = -(od[m] * x[m]), -(od[m] * y[m] + gb * dz[m])
                vals.append((gb * xg, gb * yg, xg, yg, dx, dy, ss[m] * dx, ss[m] * dy))
            vals = list(zip(*vals))
            x, y = vals[:2]
            for ref, val in zip((q.X, q.Y, q.XG, q.YG, q.dX, q.dY, q.P, q.Q), vals):
                put_pair(ref, g, j, val)
            for n, val in enumerate((ss, vals[6], vals[7])):
                edge_rows(g, j, val, q.is_low, q.is_high, n * K2)
                accs[n] = pack_columns(j, val, accs[n])
        for n in range(3):
            put(q.Oc, n * KJ + g * 8, accs[n])
        return x, y

    each(responses, ((one, one), (zero, zero)))
    for n in range(3):
        dense(q.Oc, n * KJ, q.js_right, q.js_left, n * KH)
    setups = four("is", "js", lambda n: q.hs_s.at[n], lambda n: q.hs_r.at[n])
    for c in setups:
        c.start()

    def crow(d, n):
        n = (0, 1, 0, 2)[n]
        return q.cgath[d, 16 * n:16 * n + 16, :]

    def stagger(g, carry):
        for j in range(GROUP):
            xb, xu, xv = pair(q.bi, g, j), pair(q.us, g, j), pair(q.vs, g, j)
            xb = tuple(CH * v for v in xb)
            for val, dst in ((xu, q.us), (xb, q.bi)):
                r0, r1 = roll(val[0], 7, 0), roll(val[1], 7, 0)
                put_pair(dst, g, j, (jnp.where(sub < 7, r0, r1), r1))
            for val, dst in ((xv, q.vs), (xb, q.bj)):
                put_pair(dst, g, j, [roll(v, 127, 1) for v in val])
        return carry

    each(stagger, 0)

    loads[5].wait()
    for c in halos:
        c.wait()

    for n in range(groups // 2):
        fr = q.j0_fr[KH + 8 * n:KH + 8 * n + 8, :]
        fl = q.j0_fl[KH + 8 * n:KH + 8 * n + 8, :]
        for m in range(2):
            k = 16 * n + 8 * m
            frg, flg = roll(fr, -2 * m, 1), roll(fl, -2 * m, 1)
            ab = q.own0[KJ + k:KJ + k + 8, :]
            av = q.own0[2 * KJ + k:2 * KJ + k + 8, :]
            vright = jnp.where(quad == 0, roll(av, -1, 1), roll(frg, 1, 1))
            bright = jnp.where(quad == 0, roll(ab, -1, 1), frg)
            vleft = jnp.where(quad == 2, roll(flg, 2, 1), roll(av, 1, 1))
            bleft = roll(jnp.where(quad == 1, flg, ab), 1, 1)
            q.hv[k:k + 8, :] = jnp.where(quad < 2, vright, vleft)
            q.hbj[k:k + 8, :] = CH * jnp.where(quad < 2, -bright, bleft)
    open_up(q.j0_fl, q.j0_fr, 0, q.Hp.at[0], 0)

    def patch(g, carry):
        for j in range(GROUP):
            row = g * 256 + 16 * j + 15
            q.us[pl.ds(row, 1), :] = q.i0_up[pl.ds(8 + 2 * K2 + g * 32 + 2 * j, 1), :]
            q.bi[pl.ds(row, 1), :] = CH * q.i0_up[pl.ds(8 + K2 + g * 32 + 2 * j, 1), :]
        for r in range(4):
            row = g * 32 + 8 * r
            for (dst, f, scale) in ((q.hu, 2, 1.0), (q.hbi, 1, CH)):
                base = 8 + f * K2 + row
                below = q.i0_down[pl.ds(base + 1, 8), :]
                own = q.i0_low[pl.ds(base - 1, 8), :]
                put(dst, 8 + row, scale * jnp.where(sub % 2 == 0, below, own))
        return carry

    each(patch, 0)

    def interface():
        beta = jnp.zeros((16, 128), F32)
        betas, rs, zbrs, lams = ([None] * nz for _ in range(4))
        for d in range(nz - 1, -1, -1):
            betas[d] = beta
            rs[d] = 1.0 / (1.0 - crow(d, 1) * beta)
            zbrs[d] = crow(d, 2) * beta * rs[d]
            lams[d] = crow(d, 2) + zbrs[d] * crow(d, 1)
            beta = crow(d, 3) + zbrs[d] * crow(d, 0)
            if d == 0:
                last = beta
        tops = [last] + betas[:-1]
        psi = jnp.zeros((16, 128), F32)
        psis, r2s, xrs, xrps = ([None] * nz for _ in range(4))
        for d in range(nz):
            xrs[d] = crow(d, 0) / (1.0 - psi * crow(d, 3))
            xrps[d] = xrs[d] * psi
            psis[d] = psi
            r2s[d] = 1.0 / (1.0 - psi * tops[d])
            psi = crow(d, 1) + xrps[d] * crow(d, 2)

        def pick(vals):
            out = vals[0]
            for d in range(1, nz):
                out = jnp.where(me == d, vals[d], out)
            return out

        br = [betas[d] * rs[d] for d in range(nz)]
        brx = [br[d] * crow(d, 0) for d in range(nz)]
        for n, vals in enumerate((xrps, zbrs, [r2s[d] * psis[d] for d in range(nz)], br, brx)):
            q.mine[16 * n:16 * n + 16, :] = pick(vals)
        for L in range(nz):
            part = r2s[L]
            for d in range(L - 1, -1, -1):
                q.ctab[L * nz + d, 0:16, :] = part
                q.ctab[L * nz + d, 16:32, :] = brx[L] * part
                part = part * xrs[d]
            part, gain = jnp.ones((16, 128), F32), 1.0 + br[L] * crow(L, 1)
            rpl = r2s[L] * psis[L] * lams[L]
            for d in range(L + 1, nz):
                cw = rpl * part
                q.ctab[L * nz + d, 0:16, :] = cw
                q.ctab[L * nz + d, 16:32, :] = part * gain + brx[L] * cw
                part = part * lams[d]

    def halves(x):
        return x[0:8], x[8:16]

    def pack_pair(wx, px):
        (w0, w1), (p0, p1) = halves(wx), halves(px)
        acc = roll(w0, 2, 1)
        for n, val in ((1, w1), (2, p0), (3, p1)):
            acc = jnp.where(lane // 4 == n, roll(val, 4 * n + 2, 1), acc)
        return acc

    def spread(t):
        z = jnp.where(lane < 16, t, 0.0)
        for n in (16, 32, 64):
            z = z + roll(z, n, 1)
        r = roll(z, 8, 1)
        return jnp.where(lane % 16 < 8, z, r), jnp.where(lane % 16 < 8, r, z)

    def insert(v, base):
        return roll(v, 126 - base, 1)

    def level_sums():
        for k in range(0, K2, 8):
            own, above = q.i0_high[pl.ds(9 + K2 + k, 8), :], q.i0_up[pl.ds(7 + K2 + k, 8), :]
            q.bih[k:k + 8, :] = CH * jnp.where(sub % 2 == 0, own, above)
            for n in range(2):
                q.mi[n * K2 + k:n * K2 + k + 8, :] = (
                    q.hbi[8 + k:16 + k, :] * q.is_down[(n + 1) * K2 + k:(n + 1) * K2 + k + 8, :]
                )
        for k in range(0, KJ, 8):
            hb = q.hbj[k:k + 8, :]
            for n in range(2):
                h, o = (r[(n + 1) * KJ + k:(n + 1) * KJ + k + 8, :] for r in (q.Hc, q.Oc))
                q.cj[n * KJ + k:n * KJ + k + 8, :] = jnp.where(quad < 2, -hb, hb) * h
                q.wo[n * KJ + k:n * KJ + k + 8, :] = CH * jnp.where(quad < 2, -o, o)

        def add(acc, n, m, value):
            acc[n][m] = acc[n][m] + value

        def along_i(g, carry):
            acc = [list(c) for c in carry]
            for j in range(GROUP):
                pq = (pair(q.P, g, j), pair(q.Q, g, j))
                bb = pair(q.bi, g, j)
                ahead, behind = [], []
                for n, (g0, g1) in enumerate(pq):
                    r0, r1 = roll(g0, 6, 0), roll(g1, 6, 0)
                    edge = q.is_up[pl.ds((n + 1) * K2 + g * 32 + 2 * j - 6, 8), :]
                    ahead.append((
                        bb[0] * jnp.where(sub < 6, r0, r1), bb[1] * jnp.where(sub < 6, r1, edge)
                    ))
                    r0, r1 = roll(bb[0] * g0, 2, 0), roll(bb[1] * g1, 2, 0)
                    edge = q.mi[pl.ds(n * K2 + g * 32 + 2 * j, 8), :]
                    behind.append((jnp.where(sub < 2, edge, r0), jnp.where(sub < 2, r0, r1)))
                for f in range(2):
                    for m in range(2):
                        cf = CH * pq[f][m]
                        for n in range(2):
                            add(acc, 2 * f + n, m, cf * ahead[n][m])
                            add(acc, 4 + 2 * f + n, m, cf * behind[n][m])
            return tuple(tuple(c) for c in acc)

        def along_j(g, carry):
            acc = [list(c) for c in carry]
            cs = [at(q.cj, n * KJ + g * 8) for n in range(2)]
            for j in range(GROUP):
                pq = (pair(q.P, g, j), pair(q.Q, g, j))
                bb = pair(q.bj, g, j)
                for m in range(2):
                    ahead, behind = [], []
                    for n in range(2):
                        edge = insert(cs[n], 4 * (2 * j + m))
                        ahead.append(jnp.where(lane >= 126, edge, bb[m] * roll(pq[n][m], 126, 1)))
                        behind.append(jnp.where(lane < 2, edge, roll(bb[m] * pq[n][m], 2, 1)))
                    for f in range(2):
                        cf = CH * pq[f][m]
                        for n in range(2):
                            add(acc, 2 * f + n, m, cf * ahead[n])
                            add(acc, 4 + 2 * f + n, m, cf * behind[n])
            return tuple(tuple(c) for c in acc)

        def centre(g, carry):
            acc = [list(c) for c in carry]
            hb = at(q.hbj, g * 8)
            hb = jnp.where(quad < 2, -hb, hb)
            for j in range(GROUP):
                bbi, bbj = pair(q.bi, g, j), pair(q.bj, g, j)
                pp, qq, dx, dy = (pair(r, g, j) for r in (q.P, q.Q, q.dX, q.dY))
                xx, yy, xg, yg = (pair(r, g, j) for r in (q.X, q.Y, q.XG, q.YG))
                r0, r1 = roll(bbi[0], 2, 0), roll(bbi[1], 2, 0)
                edge = at(q.hbi, 8 + g * 32 + 2 * j, False)
                bim = (jnp.where(sub < 2, edge, r0), jnp.where(sub < 2, r0, r1))
                for m in range(2):
                    edge = insert(hb, 4 * (2 * j + m))
                    bjm = jnp.where(lane < 2, edge, roll(bbj[m], 2, 1))
                    sb = CH * ((bbi[m] + bim[m]) + (jnp.where(lane >= 126, edge, bbj[m]) + bjm))
                    fx, fy = dx[m] - sb * pp[m], dy[m] - sb * qq[m]
                    add(acc, 0, m, pp[m] * fx - xg[m] * xx[m])
                    add(acc, 1, m, qq[m] * fx - xg[m] * yy[m])
                    add(acc, 2, m, qq[m] * fy - yg[m] * yy[m])
            return tuple(tuple(c) for c in acc)

        first = 0
        for body, count in ((centre, 3), (along_i, 8), (along_j, 8)):
            for n, val in enumerate(each(body, ((zero, zero),) * count)):
                q.coef[first + n, 0:8, :], q.coef[first + n, 8:16, :] = val
            first += count

    def base_rows(t):
        def body(g, carry):
            A, W, before = carry
            for j in range(GROUP):
                star, w0, ss, uu, vv, bbi, bbj, dx, dy, pp, qq, xg, yg = (
                    pair(r, g, j) for r in (
                        q.ps, w, q.s, q.us, q.vs, q.bi, q.bj, q.dX, q.dY, q.P, q.Q, q.XG, q.YG
                    )
                )
                pt = tuple(star[m] - ss[m] * (w0[m] - before[m]) for m in range(2))
                r0, r1 = roll(pt[0], 6, 0), roll(pt[1], 6, 0)
                pi = (jnp.where(sub < 6, r0, r1), jnp.where(sub < 6, r1, 0.0))
                un = tuple(uu[m] - bbi[m] * (pi[m] - pt[m]) for m in range(2))
                r0, r1 = roll(un[0], 2, 0), roll(un[1], 2, 0)
                um = (jnp.where(sub < 2, 0.0, r0), jnp.where(sub < 2, r0, r1))
                newA, newW = [], []
                for m in range(2):
                    vn = vv[m] - bbj[m] * (roll(pt[m], 126, 1) - pt[m])
                    vn = jnp.where(lane >= 126, 0.0, vn)
                    vm = jnp.where(lane < 2, 0.0, roll(vn, 2, 1))
                    div = CH * ((un[m] - um[m]) + (vn - vm))
                    newA.append(A[m] + (pp[m] * div - (dx[m] * pt[m] + xg[m] * w0[m])))
                    newW.append(W[m] + (qq[m] * div - (dy[m] * pt[m] + yg[m] * w0[m])))
                A, W, before = tuple(newA), tuple(newW), w0
            return A, W, before

        A, W, _ = each(body, ((zero, zero),) * 3)
        return list(A), list(W)

    def rows_without(src, const, dst):
        before = zero
        for k in range(0, K2, 8):
            star, w0, cs = src[k:k + 8, :], src[K2 + k:K2 + k + 8, :], const[k:k + 8, :]
            now = roll(w0, 2, 0)
            dst[k:k + 8, :] = star - cs * (w0 - jnp.where(sub < 2, before, now))
            before = now

    def columns_without(src, const, dst):
        before = zero
        for k in range(0, KJ, 8):
            star, w0, cs = src[k:k + 8, :], src[KJ + k:KJ + k + 8, :], const[k:k + 8, :]
            now = roll(w0, 8, 1)
            dst[k:k + 8, :] = star - cs * (w0 - jnp.where(lane < 8, before, now))
            before = now

    def halo_rows(t, A, W):
        lows, highs, cols = [zero, zero], [zero, zero], [zero, zero]
        for k in range(0, K2, 8):
            hu_new = q.hu[8 + k:16 + k, :] - q.hbi[8 + k:16 + k, :] * (
                q.b_low[t, k:k + 8, :] - q.b_down[t, k:k + 8, :]
            )
            high = q.bih[k:k + 8, :] * q.b_up[t, k:k + 8, :]
            for n in range(2):
                r = (n + 1) * K2 + k
                lows[n] = lows[n] + q.is_low[r:r + 8, :] * hu_new
                highs[n] = highs[n] + q.is_high[r:r + 8, :] * high
        for k in range(0, KJ, 8):
            c = q.hv[k:k + 8, :] - q.hbj[k:k + 8, :] * (q.Ob[t, k:k + 8, :] - q.Hb[t, k:k + 8, :])
            for n in range(2):
                cols[n] = cols[n] + q.wo[n * KJ + k:n * KJ + k + 8, :] * c
        for n, rows in enumerate((A, W)):
            low, high, col = lows[n], highs[n], cols[n]
            for r in (4, 2):
                low, high = low + roll(low, r, 0), high + roll(high, r, 0)
            for r in (64, 32, 16, 8):
                col = col + roll(col, r, 1)
            rows[0] = rows[0] - jnp.where(sub < 2, CH * low, 0.0)
            rows[1] = rows[1] - jnp.where(sub >= 6, CH * high, 0.0)
            for m in range(2):
                rows[m] = rows[m] - jnp.where((lane >= 126) | (lane < 2), insert(col, 4 * m), 0.0)

    def send_round(t, W0, A0):
        final = t == SUBSTEPS - 1
        wa, aw, r2psi, br, brx = (q.mine[16 * n:16 * n + 16, :] for n in range(5))
        up_row, down_row = W0 + wa * A0, A0 + aw * W0
        q.fmine[t, 0], q.fmine[t, 1] = up_row, down_row
        sends = []
        wb_own = r2psi * down_row
        pa_own = br * W0 + brx * wb_own
        for o in sorted(range(nz), key=lambda o: -min(o, nz - o)):
            L = lax.rem(me + o, nz)
            if not final:
                if o:
                    row = jnp.where(L > me, up_row, down_row)
                    wc, pc = (q.ctab[L * nz + me, 16 * n:16 * n + 16, :] * row for n in range(2))
                else:
                    wc, pc = wb_own, pa_own
                q.jc[t, o] = pack_pair(wc, pc)
                q.ic_low[t, o] = jnp.where(sub < 2, wc[0:8], roll(pc[0:8], 2, 0))
                q.ic_high[t, o] = jnp.where(sub < 2, roll(wc[8:16], 2, 0), roll(pc[8:16], 4, 0))
                for n, (a, b) in enumerate((
                    (q.jc, q.jc_fl), (q.jc, q.jc_fr), (q.ic_low, q.ic_up), (q.ic_high, q.ic_down)
                )):
                    c = remote(
                        a.at[t, o], b.at[t, me], q.hc_s.at[t, n, o], q.hc_r.at[t, n, o],
                        {**sides[n], "lev": L},
                    )
                    c.start()
                    sends.append(c)
            if o:
                c = remote(
                    q.fmine.at[t, lax.div(me + o, nz)], q.fgath.at[t, me],
                    q.ls_s.at[t, o - 1], q.ls_r.at[t, o - 1], {"lev": L},
                )
                c.start()
                sends.append(c)
        return sends, wb_own, pa_own

    for t in range(SUBSTEPS):
        final = t == SUBSTEPS - 1
        if t:
            each(implicit, wb2)

            def add_columns(src, const, wp, dst):
                for k in range(0, KJ, 8):
                    dst[k:k + 8, :] = src[k:k + 8, :] - (
                        const[KJ + k:KJ + k + 8, :] * wp[0] + const[2 * KJ + k:2 * KJ + k + 8, :] * wp[1]
                    )

            def add_rows(src, const, v, dst):
                z = jnp.where(sub < 4, v, roll(v, 4, 0))
                r = roll(z, 2, 0)
                ws, ps_ = jnp.where(sub % 4 < 2, z, r), jnp.where(sub % 4 < 2, r, z)
                for k in range(0, K2, 8):
                    dst[8 + k:16 + k, :] = src[k:k + 8, :] - (
                        const[K2 + k:K2 + k + 8, :] * ws + const[2 * K2 + k:2 * K2 + k + 8, :] * ps_
                    )

            add_columns(q.Hb.at[t - 1], q.Hc, spread(halo_j), q.Hp.at[t])
            add_columns(q.Ob.at[t - 1], q.Oc, spread(pack_pair(wb, pa)), q.Op.at[t])
            low = jnp.where(sub < 2, wb[0:8], roll(pa[0:8], 2, 0))
            add_rows(q.b_up.at[t - 1], q.is_up, halo_up, q.p_up.at[t])
            add_rows(q.b_down.at[t - 1], q.is_down, halo_down, q.p_down.at[t])
            add_rows(q.b_low.at[t - 1], q.is_low, low, q.p_low.at[t])
        i_up, i_down, i_low = (
            (q.i0_up, q.i0_down, q.i0_low) if t == 0
            else (q.p_up.at[t], q.p_down.at[t], q.p_low.at[t])
        )
        own_p = q.own0 if t == 0 else q.Op.at[t]
        halo_p = q.Hp.at[t]

        for k in range(0, KJ, 8):
            q.hv[k:k + 8, :] = q.hv[k:k + 8, :] - q.hbj[k:k + 8, :] * (
                own_p[k:k + 8, :] - halo_p[k:k + 8, :]
            )

        def explicit(g, A):
            for r in range(4):
                row = g * 32 + 8 * r
                put(q.hu, 8 + row, at(q.hu, 8 + row) - at(q.hbi, 8 + row) * (
                    at(i_low, 8 + row) - at(i_down, 8 + row)
                ))
            c = at(q.hv, g * 8)
            acc = zero
            for j in reversed(range(GROUP)):
                pp, uu, vv, ww = pair(p, g, j), pair(q.us, g, j), pair(q.vs, g, j), pair(w, g, j)
                bbi, bbj, ss = pair(q.bi, g, j), pair(q.bj, g, j), pair(q.s, g, j)
                ee, dd, hh = pair(q.E, g, j), pair(q.D, g, j), pair(q.H, g, j)
                r0, r1 = roll(pp[0], 6, 0), roll(pp[1], 6, 0)
                edge = at(i_up, 8 + g * 32 + 2 * j - 6, False)
                pi = (jnp.where(sub < 6, r0, r1), jnp.where(sub < 6, r1, edge))
                un = tuple(uu[m] - bbi[m] * (pi[m] - pp[m]) for m in range(2))
                put_pair(q.us, g, j, un)
                r0, r1 = roll(un[0], 2, 0), roll(un[1], 2, 0)
                edge = at(q.hu, 8 + g * 32 + 2 * j, False)
                um = (jnp.where(sub < 2, edge, r0), jnp.where(sub < 2, r0, r1))
                newA, hs, pss, vn = [], [], [], []
                for m in range(2):
                    edge = roll(c, 126 - 4 * (2 * j + m), 1)
                    v_new = vv[m] - bbj[m] * (roll(pp[m], 126, 1) - pp[m])
                    v_new = jnp.where(lane >= 126, edge, v_new)
                    vm = jnp.where(lane < 2, edge, roll(v_new, 2, 1))
                    star = pp[m] - (CH * ss[m]) * ((un[m] - um[m]) + (v_new - vm))
                    dw = dd[m] * ww[m]
                    hs.append(dw + hh[m] * (star - A[m]))
                    newA.append(ee[m] * A[m] + ((star - ee[m] * star) - ss[m] * dw))
                    pss.append(star)
                    vn.append(v_new)
                put_pair(q.vs, g, j, vn)
                put_pair(q.ps, g, j, pss)
                put_pair(q.h, g, j, hs)
                if not final:
                    edge_rows(g, j, pss, q.iw_low.at[t], q.iw_high.at[t], 0)
                    acc = pack_columns(j, pss, acc)
                A = tuple(newA)
            if not final:
                put(q.Ow.at[t], g * 8, acc)
            return A

        A = each(explicit, (zero, zero), downward=True)

        def forward(g, x):
            acc = zero
            for j in range(GROUP):
                ee, hh = pair(q.E, g, j), pair(q.h, g, j)
                x = tuple(ee[m] * x[m] + hh[m] for m in range(2))
                put_pair(w, g, j, x)
                if not final:
                    edge_rows(g, j, x, q.iw_low.at[t], q.iw_high.at[t], K2)
                    acc = pack_columns(j, x, acc)
            if not final:
                put(q.Ow.at[t], KJ + g * 8, acc)
            return x

        x = each(forward, (zero, zero))
        if t == 0:
            for c in consts:
                c.wait()
            interface()
            A0, W0 = (jnp.concatenate(n, 0) for n in (A, x))
            sends, wb_own, pa_own = send_round(0, W0, A0)
        if not final:
            for n in range(2):
                dense(q.Ow.at[t], n * KJ, q.jw_right.at[t], q.jw_left.at[t], n * KH)
            works = four("iw", "jw", lambda n: q.hw_s.at[t, n], lambda n: q.hw_r.at[t, n], lambda r: r.at[t])
            for c in works:
                c.start()
            A1, W1 = base_rows(t)
            if t == 0:
                for c in setups:
                    c.wait()
                for n in range(3):
                    open_up(q.js_fl, q.js_fr, n * KH, q.Hc, n * KJ)
                level_sums()
            columns_without(q.Ow.at[t], q.Oc, q.Ob.at[t])
            rows_without(q.iw_low.at[t], q.is_low, q.b_low.at[t])
            for c in works:
                c.wait()
            for n in range(2):
                open_up(q.jw_fl.at[t], q.jw_fr.at[t], n * KH, q.Hw.at[t], n * KJ)
            columns_without(q.Hw.at[t], q.Hc, q.Hb.at[t])
            rows_without(q.iw_up.at[t], q.is_up, q.b_up.at[t])
            rows_without(q.iw_down.at[t], q.is_down, q.b_down.at[t])
            halo_rows(t, A1, W1)

        if final:
            def emit(g, carry):
                hvg = at(q.hv, pl.multiple_of(g * 8, 8))
                for j in range(GROUP):
                    uu, vv = pair(q.us, g, j), pair(q.vs, g, j)
                    r0, r1 = roll(uu[0], 1, 0), roll(uu[1], 1, 0)
                    edge = at(q.hu, 8 + g * 32 + 2 * j + 1, False)
                    put_pair(uo, g, j, (jnp.where(sub < 1, edge, r0), jnp.where(sub < 1, r0, r1)))
                    put_pair(vo, g, j, [
                        jnp.where(
                            lane == 0, roll(hvg, 125 - 4 * (2 * j + m), 1), roll(vv[m], 1, 1)
                        )
                        for m in range(2)
                    ])
                return carry

            each(emit, 0)
        for c in sends:
            c.wait()

        wb, pa = wb_own, pa_own
        for o in range(1, nz):
            d = lax.rem(me + o, nz)
            row = q.fgath[t, d]
            wb = wb + q.ctab[me * nz + d, 0:16, :] * row
            pa = pa + q.ctab[me * nz + d, 16:32, :] * row
        wb2, pa2 = halves(wb), halves(pa)

        if not final:
            fr, fl, halo_up, halo_down = (
                functools.reduce(lambda a, b: a + b, [ref[t, d] for d in range(nz)])
                for ref in (q.jc_fr, q.jc_fl, q.ic_up, q.ic_down)
            )
            halo_j = jnp.where(quad < 2, roll(fr, -2, 1), roll(fl, 2, 1))
            stencil = []
            for n, v in enumerate((wb2, pa2)):
                a0, a1, b0, b1 = (roll(v[m], k, 0) for k in (6, 2) for m in range(2))
                above, below = roll(halo_up, 6 - 2 * n, 0), roll(halo_down, -2 * n, 0)
                edges = [insert(halo_j, 8 * n + 4 * m) for m in range(2)]
                stencil.append((
                    v,
                    (jnp.where(sub < 6, a0, a1), jnp.where(sub < 6, a1, above)),
                    (jnp.where(sub < 2, below, b0), jnp.where(sub < 2, b0, b1)),
                    tuple(jnp.where(lane >= 126, edges[m], roll(v[m], 126, 1)) for m in range(2)),
                    tuple(jnp.where(lane < 2, edges[m], roll(v[m], 2, 1)) for m in range(2)),
                ))
            rows = []
            for f, base in enumerate((A1, W1)):
                halves_ = []
                for m in range(2):
                    terms = [base[m]]
                    for n in range(2):
                        for k in range(5):
                            c = f + n if k == 0 else 3 + 4 * (k - 1) + 2 * f + n
                            terms.append(q.coef[c, 8 * m:8 * m + 8, :] * stencil[n][k][m])
                    while len(terms) > 1:
                        terms = [
                            sum(terms[k + 1:k + 2], terms[k]) for k in range(0, len(terms), 2)
                        ]
                    halves_.append(terms[0])
                rows.append(jnp.concatenate(halves_, 0))
            sends, wb_own, pa_own = send_round(t + 1, rows[1], rows[0])

        def implicit(g, wprev, wb2=wb2, pa2=pa2):
            for j in range(GROUP):
                w0, xx, yy = pair(w, g, j), pair(q.X, g, j), pair(q.Y, g, j)
                ss, star = pair(q.s, g, j), pair(q.ps, g, j)
                wn = tuple(w0[m] + xx[m] * wb2[m] + yy[m] * pa2[m] for m in range(2))
                pn = tuple(star[m] - ss[m] * (wn[m] - wprev[m]) for m in range(2))
                put_pair(w, g, j, wn)
                put_pair(p, g, j, pn)
                wprev = wn
            return wprev

    each(implicit, wb2)


def store(u, v, w, p, u_out, v_out, w_out, p_out, sem):
    copies = [
        pltpu.make_async_copy(src, dst, sem.at[n])
        for n, (src, dst) in enumerate(((u, u_out), (v, v_out), (w, w_out), (p, p_out)))
    ]
    for c in copies:
        c.start()
    for c in copies:
        c.wait()


def solution(mesh):
    nx, ny, nz = (mesh.shape[a] for a in ("gx", "gy", "lev"))

    def shards(*fields):
        K, I, J = fields[0].shape
        assert I == 16 and J == 128 and K % (2 * GROUP) == 0
        R = K * I
        full = pltpu.VMEM((R, J), F32)
        held = scratch(K, J, nz)
        outs = pl.pallas_call(
            functools.partial(kernel, tuple(held), K, nx, ny, nz),
            out_shape=[full] * 4,
            in_specs=[pl.BlockSpec(memory_space=pl.ANY)] * 6,
            out_specs=[pl.BlockSpec(memory_space=pltpu.VMEM)] * 4,
            scratch_shapes=list(held.values()),
            compiler_params=pltpu.CompilerParams(collective_id=0, has_side_effects=True),
        )(*(f.reshape(R, J) for f in fields))
        outs = pl.pallas_call(
            store,
            out_shape=[jax.ShapeDtypeStruct((R, J), F32)] * 4,
            in_specs=[pl.BlockSpec(memory_space=pltpu.VMEM)] * 4,
            out_specs=[pl.BlockSpec(memory_space=pl.ANY)] * 4,
            scratch_shapes=[pltpu.SemaphoreType.DMA((4,))],
        )(*(pltpu.with_memory_space_constraint(o, pltpu.VMEM) for o in outs))
        return tuple(o.reshape(K, I, J) for o in outs)

    spec = P("lev", "gx", "gy")
    return jax.shard_map(
        shards, mesh=mesh, in_specs=(spec,) * 6, out_specs=(spec,) * 4, check_vma=False
    )
```

```python
import functools
from types import SimpleNamespace

import jax
import jax.numpy as jnp
from jax import lax
from jax.experimental import pallas as pl
from jax.experimental.pallas import tpu as pltpu
from jax.sharding import PartitionSpec as P

SUBSTEPS = 3
CH = 0.3
GAIN = 4096.0
MESH = pl.DeviceIdType.MESH
GROUP = 16
F32 = jnp.float32


def scratch(K, J, nz):
    R, T, KJ, K2, KH = 16 * K, SUBSTEPS, 8 * (K // GROUP), 2 * K, 4 * (K // GROUP)
    V = lambda *s: pltpu.VMEM((*s, J), F32)
    D = lambda *s: pltpu.SemaphoreType.DMA(s)
    m = max(nz - 1, 1)
    s = {n: V(R) for n in (
        "us", "vs", "s", "bi", "bj", "E", "D", "H", "X", "Y", "ps", "h",
        "dX", "dY", "P", "Q", "XG", "YG",
    )}
    s |= {n: V(3 * K2 + 16) for n in ("i0_low", "i0_high", "i0_up", "i0_down")}
    s |= {n: V(2 * KH) for n in ("j0_right", "j0_left", "j0_fl", "j0_fr")}
    s |= {n: V(3 * K2) for n in ("is_low", "is_high", "is_up", "is_down")}
    s |= {n: V(3 * KH) for n in ("js_right", "js_left", "js_fl", "js_fr")}
    s |= {n: V(T, 2 * K2) for n in ("iw_low", "iw_high", "iw_up", "iw_down")}
    s |= {n: V(T, 2 * KH) for n in ("jw_right", "jw_left", "jw_fl", "jw_fr")}
    s |= {n: V(T, nz, 8) for n in ("ic_low", "ic_high", "ic_up", "ic_down", "jc", "jc_fl", "jc_fr")}
    s |= {n: V(T, K2 + 16) for n in ("p_up", "p_down", "p_low")}
    s |= {n: V(T, K2) for n in ("b_up", "b_down", "b_low")}
    s |= {n: V(K2) for n in ("bih",)}
    s |= {n: V(2 * K2 + 16) for n in ("mi",)}
    s |= {n: V(2 * KJ) for n in ("cj", "wo")}
    s |= {"coef": V(19, 16)}
    s |= {n: V(3 * KJ) for n in ("own0",)}
    s |= {n: V(KJ) for n in ("hv", "hbj")}
    s |= {n: V(3 * KJ) for n in ("Hc", "Oc")}
    s |= {n: V(T, 2 * KJ) for n in ("Hw", "Ow")}
    s |= {n: V(T, KJ) for n in ("Hp", "Op", "Hb", "Ob")}
    s |= {n: V(K2 + 16) for n in ("hu", "hbi")}
    s |= {"cmine": V(48), "cgath": V(nz, 48), "fmine": V(T, 2, 16), "fgath": V(T, nz, 16)}
    s |= {"ctab": V(nz * nz, 32), "mine": V(80)}
    s |= {"in_sem": D(6)}
    for n in ("h0", "hs"):
        s |= {n + "_s": D(4), n + "_r": D(4)}
    s |= {"hw_s": D(T, 4), "hw_r": D(T, 4), "hc_s": D(T, 4, nz), "hc_r": D(T, 4, nz)}
    s |= {"cs_s": D(m), "cs_r": D(m), "ls_s": D(T, m), "ls_r": D(T, m)}
    return s


def kernel(names, K, nx, ny, nz, u_in, v_in, w_in, p_in, b_in, s_in, uo, vo, w, p, *refs):
    q = SimpleNamespace(**dict(zip(names, refs)))
    gx, gy, me = lax.axis_index("gx"), lax.axis_index("gy"), lax.axis_index("lev")
    up, down = lax.rem(gx + 1, nx), lax.rem(gx + nx - 1, nx)
    right, left = lax.rem(gy + 1, ny), lax.rem(gy + ny - 1, ny)
    groups = K // GROUP
    K2, KJ, KH = 2 * K, 8 * (K // GROUP), 4 * (K // GROUP)
    sides = ({"gy": right}, {"gy": left}, {"gx": down}, {"gx": up})

    loads = []
    for n, (src, dst) in enumerate(
        ((p_in, p), (b_in, q.bi), (v_in, q.vs), (s_in, q.s), (u_in, q.us), (w_in, w))
    ):
        c = pltpu.make_async_copy(src, dst, q.in_sem.at[n])
        c.start()
        loads.append(c)

    barrier = pltpu.get_barrier_semaphore()
    for dev in sides:
        pl.semaphore_signal(barrier, inc=1, device_id=dev, device_id_type=MESH)
    for o in range(1, nz):
        pl.semaphore_signal(
            barrier, inc=1, device_id={"lev": lax.rem(me + o, nz)}, device_id_type=MESH
        )

    lane = lax.broadcasted_iota(jnp.int32, (8, 128), 1)
    sub = lax.broadcasted_iota(jnp.int32, (8, 128), 0)
    quad = lane % 4
    zero = jnp.zeros((8, 128), F32)
    one = jnp.ones((8, 128), F32)

    def roll(x, shift, axis):
        shift = shift % x.shape[axis]
        return x if shift == 0 else pltpu.roll(x, shift, axis)

    def at(ref, row, aligned=True):
        return ref[pl.ds(pl.multiple_of(row, 8) if aligned else row, 8), :]

    def put(ref, row, value):
        ref[pl.ds(pl.multiple_of(row, 8), 8), :] = value

    def each(body, carry=None, downward=False):
        def step(n, c):
            g = groups - 1 - n if downward else n
            return body(g, c)
        return lax.fori_loop(0, groups, step, carry)

    def pair(ref, g, j):
        return at(ref, g * 256 + 16 * j), at(ref, g * 256 + 16 * j + 8)

    def put_pair(ref, g, j, value):
        put(ref, g * 256 + 16 * j, value[0])
        put(ref, g * 256 + 16 * j + 8, value[1])

    def edge_rows(g, j, x, low, high, base):
        row = base + g * 32 + 2 * j
        low[pl.ds(row, 2), :] = x[0][0:2]
        if high is not None:
            high[pl.ds(row, 2), :] = x[1][6:8]

    def pack_columns(j, x, acc):
        for half in range(2):
            n = 2 * j + half
            acc = jnp.where(lane // 4 == n, roll(x[half], 4 * n + 2, 1), acc)
        return acc

    def remote(src, dst, ss, rs, dev):
        return pltpu.make_async_remote_copy(
            src_ref=src, dst_ref=dst, send_sem=ss, recv_sem=rs, device_id=dev, device_id_type=MESH
        )

    def dense(own, base, to_right, to_left, row):
        for n in range(groups // 2):
            a, b = (own[base + 16 * n + 8 * m:base + 16 * n + 8 * m + 8, :] for m in range(2))
            to_right[row + 8 * n:row + 8 * n + 8, :] = jnp.where(quad < 2, a, roll(b, 2, 1))
            to_left[row + 8 * n:row + 8 * n + 8, :] = jnp.where(quad < 2, roll(a, -2, 1), b)

    def open_up(fl, fr, row, dst, base):
        for n in range(groups // 2):
            a, b = fl[row + 8 * n:row + 8 * n + 8, :], fr[row + 8 * n:row + 8 * n + 8, :]
            for m in range(2):
                k = base + 16 * n + 8 * m
                dst[k:k + 8, :] = jnp.where(
                    quad < 2, roll(b, -2 * m, 1), roll(a, 2, 1) if m == 0 else a
                )

    for c in loads[:3]:
        c.wait()

    def first_pack(g, carry):
        accp = accb = accv = zero
        for j in range(GROUP):
            accp = pack_columns(j, pair(p, g, j), accp)
            accb = pack_columns(j, pair(q.bi, g, j), accb)
            accv = pack_columns(j, pair(q.vs, g, j), accv)
        put(q.own0, g * 8, accp)
        put(q.own0, KJ + g * 8, accb)
        put(q.own0, 2 * KJ + g * 8, accv)
        return carry

    each(first_pack, 0)

    dense(q.own0, 0, q.j0_right, q.j0_left, 0)
    for n in range(groups // 2):
        rights, lefts = [], []
        for m in range(2):
            k = 16 * n + 8 * m
            ab = q.own0[KJ + k:KJ + k + 8, :]
            av = q.own0[2 * KJ + k:2 * KJ + k + 8, :]
            rights.append(jnp.where(quad == 0, roll(av, -1, 1), ab))
            lefts.append(jnp.where(quad == 0, roll(av, -2, 1), roll(ab, -1, 1)))
        k = KH + 8 * n
        for ref, (a, b) in ((q.j0_right, rights), (q.j0_left, lefts)):
            ref[k:k + 8, :] = jnp.where(quad < 2, a, roll(b, 2, 1))

    pl.semaphore_wait(barrier, 4 + nz - 1)

    def four(i, j, ss, rs, at_=lambda r: r):
        pairs = (
            (j + "_right", j + "_fl"), (j + "_left", j + "_fr"),
            (i + "_low", i + "_up"), (i + "_high", i + "_down"),
        )
        return [
            remote(at_(getattr(q, a)), at_(getattr(q, b)), ss(n), rs(n), dev)
            for n, ((a, b), dev) in enumerate(zip(pairs, sides))
        ]

    rows0 = pl.ds(8, 3 * K2)
    halos = [
        remote(
            a if n < 2 else a.at[rows0], b if n < 2 else b.at[rows0],
            q.h0_s.at[n], q.h0_r.at[n], dev,
        )
        for n, (a, b, dev) in enumerate(zip(
            (q.j0_right, q.j0_left, q.i0_low, q.i0_high),
            (q.j0_fl, q.j0_fr, q.i0_up, q.i0_down), sides,
        ))
    ]
    for c in halos[:2]:
        c.start()

    loads[4].wait()

    def first_rows(g, carry):
        for j in range(GROUP):
            for n, ref in enumerate((p, q.bi, q.us)):
                edge_rows(g, j, pair(ref, g, j), q.i0_low, q.i0_high, 8 + n * K2)
        return carry

    each(first_rows, 0)
    for c in halos[2:]:
        c.start()

    loads[3].wait()

    def factor(g, carry):
        B, Z, yend = carry
        for j in reversed(range(GROUP)):
            bb, ss = pair(q.bi, g, j), pair(q.s, g, j)
            newB, newZ, newy = [], [], []
            for m in range(2):
                row = g * 256 + 16 * j + 8 * m
                gb = GAIN * bb[m]
                o = 1.0 + gb * B[m]
                d = 1.0 / (o + gb * ss[m])
                hh = gb * d
                e = hh * ss[m]
                put(q.D, row, d)
                put(q.H, row, hh)
                od = o * d
                put(q.E, row, e)
                dz = d * Z[m]
                put(q.Y, row, dz)
                put(q.dX, row, od)
                newB.append(ss[m] * od)
                newZ.append(e * Z[m])
                newy.append(yend[m] - (gb * dz) * Z[m])
            B, Z, yend = tuple(newB), tuple(newZ), tuple(newy)
        return B, Z, yend

    B, Z, yend = each(factor, ((zero, zero), (one, one), (zero, zero)), downward=True)
    for n, val in enumerate((Z, yend, B)):
        for m in range(2):
            q.cmine[16 * n + 8 * m:16 * n + 8 * m + 8, :] = val[m]
            q.cgath[me, 16 * n + 8 * m:16 * n + 8 * m + 8, :] = val[m]
    consts = [
        remote(q.cmine, q.cgath.at[me], q.cs_s.at[o - 1], q.cs_r.at[o - 1], {"lev": lax.rem(me + o, nz)})
        for o in range(1, nz)
    ]
    for c in consts:
        c.start()

    def responses(g, carry):
        x, y = carry
        accs = [zero] * 3
        for j in range(GROUP):
            bb, ss, dd = pair(q.bi, g, j), pair(q.s, g, j), pair(q.D, g, j)
            od, dz = pair(q.dX, g, j), pair(q.Y, g, j)
            vals = []
            for m in range(2):
                sd, gb = ss[m] * dd[m], GAIN * bb[m]
                xg, yg = sd * x[m], sd * y[m] - dz[m]
                dx, dy = -(od[m] * x[m]), -(od[m] * y[m] + gb * dz[m])
                vals.append((gb * xg, gb * yg, xg, yg, dx, dy, ss[m] * dx, ss[m] * dy))
            vals = list(zip(*vals))
            x, y = vals[:2]
            for ref, val in zip((q.X, q.Y, q.XG, q.YG, q.dX, q.dY, q.P, q.Q), vals):
                put_pair(ref, g, j, val)
            for n, val in enumerate((ss, vals[6], vals[7])):
                edge_rows(g, j, val, q.is_low, q.is_high, n * K2)
                accs[n] = pack_columns(j, val, accs[n])
        for n in range(3):
            put(q.Oc, n * KJ + g * 8, accs[n])
        return x, y

    each(responses, ((one, one), (zero, zero)))
    for n in range(3):
        dense(q.Oc, n * KJ, q.js_right, q.js_left, n * KH)
    setups = four("is", "js", lambda n: q.hs_s.at[n], lambda n: q.hs_r.at[n])
    for c in setups:
        c.start()

    def crow(d, n):
        n = (0, 1, 0, 2)[n]
        return q.cgath[d, 16 * n:16 * n + 16, :]

    def stagger(g, carry):
        for j in range(GROUP):
            xb, xu, xv = pair(q.bi, g, j), pair(q.us, g, j), pair(q.vs, g, j)
            xb = tuple(CH * v for v in xb)
            for val, dst in ((xu, q.us), (xb, q.bi)):
                r0, r1 = roll(val[0], 7, 0), roll(val[1], 7, 0)
                put_pair(dst, g, j, (jnp.where(sub < 7, r0, r1), r1))
            for val, dst in ((xv, q.vs), (xb, q.bj)):
                put_pair(dst, g, j, [roll(v, 127, 1) for v in val])
        return carry

    each(stagger, 0)

    loads[5].wait()
    for c in halos:
        c.wait()

    for n in range(groups // 2):
        fr = q.j0_fr[KH + 8 * n:KH + 8 * n + 8, :]
        fl = q.j0_fl[KH + 8 * n:KH + 8 * n + 8, :]
        for m in range(2):
            k = 16 * n + 8 * m
            frg, flg = roll(fr, -2 * m, 1), roll(fl, -2 * m, 1)
            ab = q.own0[KJ + k:KJ + k + 8, :]
            av = q.own0[2 * KJ + k:2 * KJ + k + 8, :]
            vright = jnp.where(quad == 0, roll(av, -1, 1), roll(frg, 1, 1))
            bright = jnp.where(quad == 0, roll(ab, -1, 1), frg)
            vleft = jnp.where(quad == 2, roll(flg, 2, 1), roll(av, 1, 1))
            bleft = roll(jnp.where(quad == 1, flg, ab), 1, 1)
            q.hv[k:k + 8, :] = jnp.where(quad < 2, vright, vleft)
            q.hbj[k:k + 8, :] = CH * jnp.where(quad < 2, -bright, bleft)
    open_up(q.j0_fl, q.j0_fr, 0, q.Hp.at[0], 0)

    def patch(g, carry):
        for j in range(GROUP):
            row = g * 256 + 16 * j + 15
            q.us[pl.ds(row, 1), :] = q.i0_up[pl.ds(8 + 2 * K2 + g * 32 + 2 * j, 1), :]
            q.bi[pl.ds(row, 1), :] = CH * q.i0_up[pl.ds(8 + K2 + g * 32 + 2 * j, 1), :]
        for r in range(4):
            row = g * 32 + 8 * r
            for (dst, f, scale) in ((q.hu, 2, 1.0), (q.hbi, 1, CH)):
                base = 8 + f * K2 + row
                below = q.i0_down[pl.ds(base + 1, 8), :]
                own = q.i0_low[pl.ds(base - 1, 8), :]
                put(dst, 8 + row, scale * jnp.where(sub % 2 == 0, below, own))
        return carry

    each(patch, 0)

    def interface():
        beta = jnp.zeros((16, 128), F32)
        betas, rs, zbrs, lams = ([None] * nz for _ in range(4))
        for d in range(nz - 1, -1, -1):
            betas[d] = beta
            rs[d] = 1.0 / (1.0 - crow(d, 1) * beta)
            zbrs[d] = crow(d, 2) * beta * rs[d]
            lams[d] = crow(d, 2) + zbrs[d] * crow(d, 1)
            beta = crow(d, 3) + zbrs[d] * crow(d, 0)
            if d == 0:
                last = beta
        tops = [last] + betas[:-1]
        psi = jnp.zeros((16, 128), F32)
        psis, r2s, xrs, xrps = ([None] * nz for _ in range(4))
        for d in range(nz):
            xrs[d] = crow(d, 0) / (1.0 - psi * crow(d, 3))
            xrps[d] = xrs[d] * psi
            psis[d] = psi
            r2s[d] = 1.0 / (1.0 - psi * tops[d])
            psi = crow(d, 1) + xrps[d] * crow(d, 2)

        def pick(vals):
            out = vals[0]
            for d in range(1, nz):
                out = jnp.where(me == d, vals[d], out)
            return out

        br = [betas[d] * rs[d] for d in range(nz)]
        brx = [br[d] * crow(d, 0) for d in range(nz)]
        for n, vals in enumerate((xrps, zbrs, [r2s[d] * psis[d] for d in range(nz)], br, brx)):
            q.mine[16 * n:16 * n + 16, :] = pick(vals)
        for L in range(nz):
            part = r2s[L]
            for d in range(L - 1, -1, -1):
                q.ctab[L * nz + d, 0:16, :] = part
                q.ctab[L * nz + d, 16:32, :] = brx[L] * part
                part = part * xrs[d]
            part, gain = jnp.ones((16, 128), F32), 1.0 + br[L] * crow(L, 1)
            rpl = r2s[L] * psis[L] * lams[L]
            for d in range(L + 1, nz):
                cw = rpl * part
                q.ctab[L * nz + d, 0:16, :] = cw
                q.ctab[L * nz + d, 16:32, :] = part * gain + brx[L] * cw
                part = part * lams[d]

    def halves(x):
        return x[0:8], x[8:16]

    def pack_pair(wx, px):
        (w0, w1), (p0, p1) = halves(wx), halves(px)
        acc = roll(w0, 2, 1)
        for n, val in ((1, w1), (2, p0), (3, p1)):
            acc = jnp.where(lane // 4 == n, roll(val, 4 * n + 2, 1), acc)
        return acc

    def spread(t):
        z = jnp.where(lane < 16, t, 0.0)
        for n in (16, 32, 64):
            z = z + roll(z, n, 1)
        r = roll(z, 8, 1)
        return jnp.where(lane % 16 < 8, z, r), jnp.where(lane % 16 < 8, r, z)

    def insert(v, base):
        return roll(v, 126 - base, 1)

    def level_sums():
        for k in range(0, K2, 8):
            own, above = q.i0_high[pl.ds(9 + K2 + k, 8), :], q.i0_up[pl.ds(7 + K2 + k, 8), :]
            q.bih[k:k + 8, :] = CH * jnp.where(sub % 2 == 0, own, above)
            for n in range(2):
                q.mi[n * K2 + k:n * K2 + k + 8, :] = (
                    q.hbi[8 + k:16 + k, :] * q.is_down[(n + 1) * K2 + k:(n + 1) * K2 + k + 8, :]
                )
        for k in range(0, KJ, 8):
            hb = q.hbj[k:k + 8, :]
            for n in range(2):
                h, o = (r[(n + 1) * KJ + k:(n + 1) * KJ + k + 8, :] for r in (q.Hc, q.Oc))
                q.cj[n * KJ + k:n * KJ + k + 8, :] = jnp.where(quad < 2, -hb, hb) * h
                q.wo[n * KJ + k:n * KJ + k + 8, :] = CH * jnp.where(quad < 2, -o, o)

        def add(acc, n, m, value):
            acc[n][m] = acc[n][m] + value

        def along_i(g, carry):
            acc = [list(c) for c in carry]
            for j in range(GROUP):
                pq = (pair(q.P, g, j), pair(q.Q, g, j))
                bb = pair(q.bi, g, j)
                ahead, behind = [], []
                for n, (g0, g1) in enumerate(pq):
                    r0, r1 = roll(g0, 6, 0), roll(g1, 6, 0)
                    edge = q.is_up[pl.ds((n + 1) * K2 + g * 32 + 2 * j - 6, 8), :]
                    ahead.append((
                        bb[0] * jnp.where(sub < 6, r0, r1), bb[1] * jnp.where(sub < 6, r1, edge)
                    ))
                    r0, r1 = roll(bb[0] * g0, 2, 0), roll(bb[1] * g1, 2, 0)
                    edge = q.mi[pl.ds(n * K2 + g * 32 + 2 * j, 8), :]
                    behind.append((jnp.where(sub < 2, edge, r0), jnp.where(sub < 2, r0, r1)))
                for f in range(2):
                    for m in range(2):
                        cf = CH * pq[f][m]
                        for n in range(2):
                            add(acc, 2 * f + n, m, cf * ahead[n][m])
                            add(acc, 4 + 2 * f + n, m, cf * behind[n][m])
            return tuple(tuple(c) for c in acc)

        def along_j(g, carry):
            acc = [list(c) for c in carry]
            cs = [at(q.cj, n * KJ + g * 8) for n in range(2)]
            for j in range(GROUP):
                pq = (pair(q.P, g, j), pair(q.Q, g, j))
                bb = pair(q.bj, g, j)
                for m in range(2):
                    ahead, behind = [], []
                    for n in range(2):
                        edge = insert(cs[n], 4 * (2 * j + m))
                        ahead.append(jnp.where(lane >= 126, edge, bb[m] * roll(pq[n][m], 126, 1)))
                        behind.append(jnp.where(lane < 2, edge, roll(bb[m] * pq[n][m], 2, 1)))
                    for f in range(2):
                        cf = CH * pq[f][m]
                        for n in range(2):
                            add(acc, 2 * f + n, m, cf * ahead[n])
                            add(acc, 4 + 2 * f + n, m, cf * behind[n])
            return tuple(tuple(c) for c in acc)

        def centre(g, carry):
            acc = [list(c) for c in carry]
            hb = at(q.hbj, g * 8)
            hb = jnp.where(quad < 2, -hb, hb)
            for j in range(GROUP):
                bbi, bbj = pair(q.bi, g, j), pair(q.bj, g, j)
                pp, qq, dx, dy = (pair(r, g, j) for r in (q.P, q.Q, q.dX, q.dY))
                xx, yy, xg, yg = (pair(r, g, j) for r in (q.X, q.Y, q.XG, q.YG))
                r0, r1 = roll(bbi[0], 2, 0), roll(bbi[1], 2, 0)
                edge = at(q.hbi, 8 + g * 32 + 2 * j, False)
                bim = (jnp.where(sub < 2, edge, r0), jnp.where(sub < 2, r0, r1))
                for m in range(2):
                    edge = insert(hb, 4 * (2 * j + m))
                    bjm = jnp.where(lane < 2, edge, roll(bbj[m], 2, 1))
                    sb = CH * ((bbi[m] + bim[m]) + (jnp.where(lane >= 126, edge, bbj[m]) + bjm))
                    fx, fy = dx[m] - sb * pp[m], dy[m] - sb * qq[m]
                    add(acc, 0, m, pp[m] * fx - xg[m] * xx[m])
                    add(acc, 1, m, qq[m] * fx - xg[m] * yy[m])
                    add(acc, 2, m, qq[m] * fy - yg[m] * yy[m])
            return tuple(tuple(c) for c in acc)

        first = 0
        for body, count in ((centre, 3), (along_i, 8), (along_j, 8)):
            for n, val in enumerate(each(body, ((zero, zero),) * count)):
                q.coef[first + n, 0:8, :], q.coef[first + n, 8:16, :] = val
            first += count

    def base_rows(t):
        def body(g, carry):
            A, W, before = carry
            for j in range(GROUP):
                star, w0, ss, uu, vv, bbi, bbj, dx, dy, pp, qq, xg, yg = (
                    pair(r, g, j) for r in (
                        q.ps, w, q.s, q.us, q.vs, q.bi, q.bj, q.dX, q.dY, q.P, q.Q, q.XG, q.YG
                    )
                )
                pt = tuple(star[m] - ss[m] * (w0[m] - before[m]) for m in range(2))
                r0, r1 = roll(pt[0], 6, 0), roll(pt[1], 6, 0)
                pi = (jnp.where(sub < 6, r0, r1), jnp.where(sub < 6, r1, 0.0))
                un = tuple(uu[m] - bbi[m] * (pi[m] - pt[m]) for m in range(2))
                r0, r1 = roll(un[0], 2, 0), roll(un[1], 2, 0)
                um = (jnp.where(sub < 2, 0.0, r0), jnp.where(sub < 2, r0, r1))
                newA, newW = [], []
                for m in range(2):
                    vn = vv[m] - bbj[m] * (roll(pt[m], 126, 1) - pt[m])
                    vn = jnp.where(lane >= 126, 0.0, vn)
                    vm = jnp.where(lane < 2, 0.0, roll(vn, 2, 1))
                    div = CH * ((un[m] - um[m]) + (vn - vm))
                    newA.append(A[m] + (pp[m] * div - (dx[m] * pt[m] + xg[m] * w0[m])))
                    newW.append(W[m] + (qq[m] * div - (dy[m] * pt[m] + yg[m] * w0[m])))
                A, W, before = tuple(newA), tuple(newW), w0
            return A, W, before

        A, W, _ = each(body, ((zero, zero),) * 3)
        return list(A), list(W)

    def rows_without(src, const, dst):
        before = zero
        for k in range(0, K2, 8):
            star, w0, cs = src[k:k + 8, :], src[K2 + k:K2 + k + 8, :], const[k:k + 8, :]
            now = roll(w0, 2, 0)
            dst[k:k + 8, :] = star - cs * (w0 - jnp.where(sub < 2, before, now))
            before = now

    def columns_without(src, const, dst):
        before = zero
        for k in range(0, KJ, 8):
            star, w0, cs = src[k:k + 8, :], src[KJ + k:KJ + k + 8, :], const[k:k + 8, :]
            now = roll(w0, 8, 1)
            dst[k:k + 8, :] = star - cs * (w0 - jnp.where(lane < 8, before, now))
            before = now

    def halo_rows(t, A, W):
        lows, highs, cols = [zero, zero], [zero, zero], [zero, zero]
        for k in range(0, K2, 8):
            hu_new = q.hu[8 + k:16 + k, :] - q.hbi[8 + k:16 + k, :] * (
                q.b_low[t, k:k + 8, :] - q.b_down[t, k:k + 8, :]
            )
            high = q.bih[k:k + 8, :] * q.b_up[t, k:k + 8, :]
            for n in range(2):
                r = (n + 1) * K2 + k
                lows[n] = lows[n] + q.is_low[r:r + 8, :] * hu_new
                highs[n] = highs[n] + q.is_high[r:r + 8, :] * high
        for k in range(0, KJ, 8):
            c = q.hv[k:k + 8, :] - q.hbj[k:k + 8, :] * (q.Ob[t, k:k + 8, :] - q.Hb[t, k:k + 8, :])
            for n in range(2):
                cols[n] = cols[n] + q.wo[n * KJ + k:n * KJ + k + 8, :] * c
        for n, rows in enumerate((A, W)):
            low, high, col = lows[n], highs[n], cols[n]
            for r in (4, 2):
                low, high = low + roll(low, r, 0), high + roll(high, r, 0)
            for r in (32, 8):
                col = (col + roll(col, r, 1)) + (roll(col, 2 * r, 1) + roll(col, 3 * r, 1))
            rows[0] = rows[0] - jnp.where(sub < 2, CH * low, 0.0)
            rows[1] = rows[1] - jnp.where(sub >= 6, CH * high, 0.0)
            for m in range(2):
                rows[m] = rows[m] - jnp.where((lane >= 126) | (lane < 2), insert(col, 4 * m), 0.0)

    def send_round(t, W0, A0):
        final = t == SUBSTEPS - 1
        wa, aw, r2psi, br, brx = (q.mine[16 * n:16 * n + 16, :] for n in range(5))
        up_row, down_row = W0 + wa * A0, A0 + aw * W0
        q.fmine[t, 0], q.fmine[t, 1] = up_row, down_row
        sends = []
        wb_own = r2psi * down_row
        pa_own = br * W0 + brx * wb_own
        for o in sorted(range(nz), key=lambda o: -min(o, nz - o)):
            L = lax.rem(me + o, nz)
            if not final:
                if o:
                    row = jnp.where(L > me, up_row, down_row)
                    wc, pc = (q.ctab[L * nz + me, 16 * n:16 * n + 16, :] * row for n in range(2))
                else:
                    wc, pc = wb_own, pa_own
                q.jc[t, o] = pack_pair(wc, pc)
                q.ic_low[t, o] = jnp.where(sub < 2, wc[0:8], roll(pc[0:8], 2, 0))
                q.ic_high[t, o] = jnp.where(sub < 2, roll(wc[8:16], 2, 0), roll(pc[8:16], 4, 0))
                for n, (a, b) in enumerate((
                    (q.jc, q.jc_fl), (q.jc, q.jc_fr), (q.ic_low, q.ic_up), (q.ic_high, q.ic_down)
                )):
                    c = remote(
                        a.at[t, o], b.at[t, me], q.hc_s.at[t, n, o], q.hc_r.at[t, n, o],
                        {**sides[n], "lev": L},
                    )
                    c.start()
                    sends.append(c)
            if o:
                c = remote(
                    q.fmine.at[t, lax.div(me + o, nz)], q.fgath.at[t, me],
                    q.ls_s.at[t, o - 1], q.ls_r.at[t, o - 1], {"lev": L},
                )
                c.start()
                sends.append(c)
        return sends, wb_own, pa_own

    for t in range(SUBSTEPS):
        final = t == SUBSTEPS - 1
        if t:
            each(implicit, wb2)

            def add_columns(src, const, wp, dst):
                for k in range(0, KJ, 8):
                    dst[k:k + 8, :] = src[k:k + 8, :] - (
                        const[KJ + k:KJ + k + 8, :] * wp[0] + const[2 * KJ + k:2 * KJ + k + 8, :] * wp[1]
                    )

            def add_rows(src, const, v, dst):
                z = jnp.where(sub < 4, v, roll(v, 4, 0))
                r = roll(z, 2, 0)
                ws, ps_ = jnp.where(sub % 4 < 2, z, r), jnp.where(sub % 4 < 2, r, z)
                for k in range(0, K2, 8):
                    dst[8 + k:16 + k, :] = src[k:k + 8, :] - (
                        const[K2 + k:K2 + k + 8, :] * ws + const[2 * K2 + k:2 * K2 + k + 8, :] * ps_
                    )

            add_columns(q.Hb.at[t - 1], q.Hc, spread(halo_j), q.Hp.at[t])
            add_columns(q.Ob.at[t - 1], q.Oc, spread(pack_pair(wb, pa)), q.Op.at[t])
            low = jnp.where(sub < 2, wb[0:8], roll(pa[0:8], 2, 0))
            add_rows(q.b_up.at[t - 1], q.is_up, halo_up, q.p_up.at[t])
            add_rows(q.b_down.at[t - 1], q.is_down, halo_down, q.p_down.at[t])
            add_rows(q.b_low.at[t - 1], q.is_low, low, q.p_low.at[t])
        i_up, i_down, i_low = (
            (q.i0_up, q.i0_down, q.i0_low) if t == 0
            else (q.p_up.at[t], q.p_down.at[t], q.p_low.at[t])
        )
        own_p = q.own0 if t == 0 else q.Op.at[t]
        halo_p = q.Hp.at[t]

        for k in range(0, KJ, 8):
            q.hv[k:k + 8, :] = q.hv[k:k + 8, :] - q.hbj[k:k + 8, :] * (
                own_p[k:k + 8, :] - halo_p[k:k + 8, :]
            )

        def explicit(g, A):
            for r in range(4):
                row = g * 32 + 8 * r
                put(q.hu, 8 + row, at(q.hu, 8 + row) - at(q.hbi, 8 + row) * (
                    at(i_low, 8 + row) - at(i_down, 8 + row)
                ))
            c = at(q.hv, g * 8)
            acc = zero
            for j in reversed(range(GROUP)):
                pp, uu, vv, ww = pair(p, g, j), pair(q.us, g, j), pair(q.vs, g, j), pair(w, g, j)
                bbi, bbj, ss = pair(q.bi, g, j), pair(q.bj, g, j), pair(q.s, g, j)
                ee, dd, hh = pair(q.E, g, j), pair(q.D, g, j), pair(q.H, g, j)
                r0, r1 = roll(pp[0], 6, 0), roll(pp[1], 6, 0)
                edge = at(i_up, 8 + g * 32 + 2 * j - 6, False)
                pi = (jnp.where(sub < 6, r0, r1), jnp.where(sub < 6, r1, edge))
                un = tuple(uu[m] - bbi[m] * (pi[m] - pp[m]) for m in range(2))
                put_pair(q.us, g, j, un)
                r0, r1 = roll(un[0], 2, 0), roll(un[1], 2, 0)
                edge = at(q.hu, 8 + g * 32 + 2 * j, False)
                um = (jnp.where(sub < 2, edge, r0), jnp.where(sub < 2, r0, r1))
                newA, hs, pss, vn = [], [], [], []
                for m in range(2):
                    edge = roll(c, 126 - 4 * (2 * j + m), 1)
                    v_new = vv[m] - bbj[m] * (roll(pp[m], 126, 1) - pp[m])
                    v_new = jnp.where(lane >= 126, edge, v_new)
                    vm = jnp.where(lane < 2, edge, roll(v_new, 2, 1))
                    star = pp[m] - (CH * ss[m]) * ((un[m] - um[m]) + (v_new - vm))
                    dw = dd[m] * ww[m]
                    hs.append(dw + hh[m] * (star - A[m]))
                    newA.append(ee[m] * A[m] + ((star - ee[m] * star) - ss[m] * dw))
                    pss.append(star)
                    vn.append(v_new)
                put_pair(q.vs, g, j, vn)
                put_pair(q.ps, g, j, pss)
                put_pair(q.h, g, j, hs)
                if not final:
                    edge_rows(g, j, pss, q.iw_low.at[t], q.iw_high.at[t], 0)
                    acc = pack_columns(j, pss, acc)
                A = tuple(newA)
            if not final:
                put(q.Ow.at[t], g * 8, acc)
            return A

        A = each(explicit, (zero, zero), downward=True)

        def forward(g, x):
            acc = zero
            for j in range(GROUP):
                ee, hh = pair(q.E, g, j), pair(q.h, g, j)
                x = tuple(ee[m] * x[m] + hh[m] for m in range(2))
                put_pair(w, g, j, x)
                if not final:
                    edge_rows(g, j, x, q.iw_low.at[t], q.iw_high.at[t], K2)
                    acc = pack_columns(j, x, acc)
            if not final:
                put(q.Ow.at[t], KJ + g * 8, acc)
            return x

        x = each(forward, (zero, zero))
        if t == 0:
            for c in consts:
                c.wait()
            interface()
            A0, W0 = (jnp.concatenate(n, 0) for n in (A, x))
            sends, wb_own, pa_own = send_round(0, W0, A0)
        if not final:
            for n in range(2):
                dense(q.Ow.at[t], n * KJ, q.jw_right.at[t], q.jw_left.at[t], n * KH)
            works = four("iw", "jw", lambda n: q.hw_s.at[t, n], lambda n: q.hw_r.at[t, n], lambda r: r.at[t])
            for c in works:
                c.start()
            A1, W1 = base_rows(t)
            if t == 0:
                for c in setups:
                    c.wait()
                for n in range(3):
                    open_up(q.js_fl, q.js_fr, n * KH, q.Hc, n * KJ)
                level_sums()
            columns_without(q.Ow.at[t], q.Oc, q.Ob.at[t])
            rows_without(q.iw_low.at[t], q.is_low, q.b_low.at[t])

            def finish(A, W):
                for c in works:
                    c.wait()
                for n in range(2):
                    open_up(q.jw_fl.at[t], q.jw_fr.at[t], n * KH, q.Hw.at[t], n * KJ)
                columns_without(q.Hw.at[t], q.Hc, q.Hb.at[t])
                rows_without(q.iw_up.at[t], q.is_up, q.b_up.at[t])
                rows_without(q.iw_down.at[t], q.is_down, q.b_down.at[t])
                halo_rows(t, A, W)

            if t == 0:
                finish(A1, W1)

        if final:
            def emit(g, carry):
                hvg = at(q.hv, pl.multiple_of(g * 8, 8))
                for j in range(GROUP):
                    uu, vv = pair(q.us, g, j), pair(q.vs, g, j)
                    r0, r1 = roll(uu[0], 1, 0), roll(uu[1], 1, 0)
                    edge = at(q.hu, 8 + g * 32 + 2 * j + 1, False)
                    put_pair(uo, g, j, (jnp.where(sub < 1, edge, r0), jnp.where(sub < 1, r0, r1)))
                    put_pair(vo, g, j, [
                        jnp.where(
                            lane == 0, roll(hvg, 125 - 4 * (2 * j + m), 1), roll(vv[m], 1, 1)
                        )
                        for m in range(2)
                    ])
                return carry

            each(emit, 0)
        for c in sends:
            c.wait()

        wb, pa = wb_own, pa_own
        for o in range(1, nz):
            d = lax.rem(me + o, nz)
            row = q.fgath[t, d]
            wb = wb + q.ctab[me * nz + d, 0:16, :] * row
            pa = pa + q.ctab[me * nz + d, 16:32, :] * row
        wb2, pa2 = halves(wb), halves(pa)

        if not final:
            fr, fl, halo_up, halo_down = (
                functools.reduce(lambda a, b: a + b, [ref[t, d] for d in range(nz)])
                for ref in (q.jc_fr, q.jc_fl, q.ic_up, q.ic_down)
            )
            halo_j = jnp.where(quad < 2, roll(fr, -2, 1), roll(fl, 2, 1))
            stencil = []
            for n, v in enumerate((wb2, pa2)):
                a0, a1, b0, b1 = (roll(v[m], k, 0) for k in (6, 2) for m in range(2))
                above, below = roll(halo_up, 6 - 2 * n, 0), roll(halo_down, -2 * n, 0)
                edges = [
                    jnp.where(
                        lane >= 126, roll(fr, 124 - 8 * n - 4 * m, 1), roll(fl, -8 * n - 4 * m, 1)
                    )
                    for m in range(2)
                ]
                stencil.append((
                    v,
                    (jnp.where(sub < 6, a0, a1), jnp.where(sub < 6, a1, above)),
                    (jnp.where(sub < 2, below, b0), jnp.where(sub < 2, b0, b1)),
                    tuple(jnp.where(lane >= 126, edges[m], roll(v[m], 126, 1)) for m in range(2)),
                    tuple(jnp.where(lane < 2, edges[m], roll(v[m], 2, 1)) for m in range(2)),
                ))
            rows = []
            for f, base in enumerate((A1, W1)):
                halves_ = []
                for m in range(2):
                    terms = [base[m]]
                    for n in range(2):
                        for k in range(5):
                            c = f + n if k == 0 else 3 + 4 * (k - 1) + 2 * f + n
                            terms.append(q.coef[c, 8 * m:8 * m + 8, :] * stencil[n][k][m])
                    while len(terms) > 1:
                        terms = [
                            sum(terms[k + 1:k + 2], terms[k]) for k in range(0, len(terms), 2)
                        ]
                    halves_.append(terms[0])
                rows.append(halves_)
            if t:
                finish(*rows)
            rows = [jnp.concatenate(r, 0) for r in rows]
            sends, wb_own, pa_own = send_round(t + 1, rows[1], rows[0])

        def implicit(g, wprev, wb2=wb2, pa2=pa2):
            for j in range(GROUP):
                w0, xx, yy = pair(w, g, j), pair(q.X, g, j), pair(q.Y, g, j)
                ss, star = pair(q.s, g, j), pair(q.ps, g, j)
                wn = tuple(w0[m] + xx[m] * wb2[m] + yy[m] * pa2[m] for m in range(2))
                pn = tuple(star[m] - ss[m] * (wn[m] - wprev[m]) for m in range(2))
                put_pair(w, g, j, wn)
                put_pair(p, g, j, pn)
                wprev = wn
            return wprev

    each(implicit, wb2)


def store(u, v, w, p, u_out, v_out, w_out, p_out, sem):
    copies = [
        pltpu.make_async_copy(src, dst, sem.at[n])
        for n, (src, dst) in enumerate(((u, u_out), (v, v_out), (w, w_out), (p, p_out)))
    ]
    for c in copies:
        c.start()
    for c in copies:
        c.wait()


def solution(mesh):
    nx, ny, nz = (mesh.shape[a] for a in ("gx", "gy", "lev"))

    def shards(*fields):
        K, I, J = fields[0].shape
        assert I == 16 and J == 128 and K % (2 * GROUP) == 0
        R = K * I
        full = pltpu.VMEM((R, J), F32)
        held = scratch(K, J, nz)
        outs = pl.pallas_call(
            functools.partial(kernel, tuple(held), K, nx, ny, nz),
            out_shape=[full] * 4,
            in_specs=[pl.BlockSpec(memory_space=pl.ANY)] * 6,
            out_specs=[pl.BlockSpec(memory_space=pltpu.VMEM)] * 4,
            scratch_shapes=list(held.values()),
            compiler_params=pltpu.CompilerParams(collective_id=0, has_side_effects=True),
        )(*(f.reshape(R, J) for f in fields))
        outs = pl.pallas_call(
            store,
            out_shape=[jax.ShapeDtypeStruct((R, J), F32)] * 4,
            in_specs=[pl.BlockSpec(memory_space=pltpu.VMEM)] * 4,
            out_specs=[pl.BlockSpec(memory_space=pl.ANY)] * 4,
            scratch_shapes=[pltpu.SemaphoreType.DMA((4,))],
        )(*(pltpu.with_memory_space_constraint(o, pltpu.VMEM) for o in outs))
        return tuple(o.reshape(K, I, J) for o in outs)

    spec = P("lev", "gx", "gy")
    return jax.shard_map(
        shards, mesh=mesh, in_specs=(spec,) * 6, out_specs=(spec,) * 4, check_vma=False
    )
```

```python
import functools
from types import SimpleNamespace

import jax
import jax.numpy as jnp
from jax import lax
from jax.experimental import pallas as pl
from jax.experimental.pallas import tpu as pltpu
from jax.sharding import PartitionSpec as P

SUBSTEPS = 3
CH = 0.3
GAIN = 4096.0
MESH = pl.DeviceIdType.MESH
GROUP = 16
CHUNKS = 2
F32 = jnp.float32


def scratch(K, J, nz):
    R, T, KJ, K2, KH = 16 * K, SUBSTEPS, 8 * (K // GROUP), 2 * K, 4 * (K // GROUP)
    V = lambda *s: pltpu.VMEM((*s, J), F32)
    D = lambda *s: pltpu.SemaphoreType.DMA(s)
    m = max(nz - 1, 1)
    s = {n: V(R) for n in (
        "us", "vs", "p", "bi", "bj", "E", "D", "H", "h",
        "dX", "dY", "P", "Q", "XG", "YG",
    )}
    s |= {n: V(3 * K2 + 16) for n in ("i0_low", "i0_high", "i0_up", "i0_down")}
    s |= {n: V(2 * KH) for n in ("j0_right", "j0_left", "j0_fl", "j0_fr")}
    s |= {n: V(3 * K2) for n in ("is_low", "is_high", "is_up", "is_down")}
    s |= {n: V(3 * KH) for n in ("js_right", "js_left", "js_fl", "js_fr")}
    s |= {n: V(T, 2 * K2) for n in ("iw_low", "iw_high", "iw_up", "iw_down")}
    s |= {n: V(T, 2 * KH) for n in ("jw_right", "jw_left", "jw_fl", "jw_fr")}
    s |= {n: V(T, nz, 8) for n in ("ic_low", "ic_high", "ic_up", "ic_down", "jc", "jc_fl", "jc_fr")}
    s |= {n: V(T, K2 + 16) for n in ("p_up", "p_down", "p_low")}
    s |= {n: V(T, K2) for n in ("b_up", "b_down", "b_low")}
    s |= {n: V(K2) for n in ("bih",)}
    s |= {n: V(2 * K2 + 16) for n in ("mi",)}
    s |= {n: V(2 * KJ) for n in ("cj", "wo")}
    s |= {"coef": V(19, 16)}
    s |= {n: V(3 * KJ) for n in ("own0",)}
    s |= {n: V(KJ) for n in ("hv", "hbj")}
    s |= {n: V(3 * KJ) for n in ("Hc", "Oc")}
    s |= {n: V(T, 2 * KJ) for n in ("Hw", "Ow")}
    s |= {n: V(T, KJ) for n in ("Hp", "Op", "Hb", "Ob")}
    s |= {n: V(K2 + 16) for n in ("hu", "hbi")}
    s |= {"cmine": V(48), "cgath": V(nz, 48), "fmine": V(T, 2, 16), "fgath": V(T, nz, 16)}
    s |= {"ctab": V(nz * nz, 32), "mine": V(80)}
    s |= {"in_sem": D(6)}
    for n in ("h0", "hs"):
        s |= {n + "_s": D(4), n + "_r": D(4)}
    s |= {"hw_s": D(T, 4), "hw_r": D(T, 4), "hc_s": D(T, 4, nz), "hc_r": D(T, 4, nz)}
    s |= {"cs_s": D(m), "cs_r": D(m), "ls_s": D(T, m), "ls_r": D(T, m)}
    return s


def kernel(names, K, nx, ny, nz, u_in, v_in, w_in, p_in, b_in, s_in, uo, vo, w, ps, s, X, Y, wend, *refs):
    q = SimpleNamespace(**dict(zip(names, refs)), ps=ps, s=s, X=X, Y=Y)
    p = q.p
    gx, gy, me = lax.axis_index("gx"), lax.axis_index("gy"), lax.axis_index("lev")
    up, down = lax.rem(gx + 1, nx), lax.rem(gx + nx - 1, nx)
    right, left = lax.rem(gy + 1, ny), lax.rem(gy + ny - 1, ny)
    groups = K // GROUP
    K2, KJ, KH = 2 * K, 8 * (K // GROUP), 4 * (K // GROUP)
    sides = ({"gy": right}, {"gy": left}, {"gx": down}, {"gx": up})

    loads = []
    for n, (src, dst) in enumerate(
        ((p_in, p), (b_in, q.bi), (v_in, q.vs), (s_in, q.s), (u_in, q.us), (w_in, w))
    ):
        c = pltpu.make_async_copy(src, dst, q.in_sem.at[n])
        c.start()
        loads.append(c)

    barrier = pltpu.get_barrier_semaphore()
    for dev in sides:
        pl.semaphore_signal(barrier, inc=1, device_id=dev, device_id_type=MESH)
    for o in range(1, nz):
        pl.semaphore_signal(
            barrier, inc=1, device_id={"lev": lax.rem(me + o, nz)}, device_id_type=MESH
        )

    lane = lax.broadcasted_iota(jnp.int32, (8, 128), 1)
    sub = lax.broadcasted_iota(jnp.int32, (8, 128), 0)
    quad = lane % 4
    zero = jnp.zeros((8, 128), F32)
    one = jnp.ones((8, 128), F32)

    def roll(x, shift, axis):
        shift = shift % x.shape[axis]
        return x if shift == 0 else pltpu.roll(x, shift, axis)

    def at(ref, row, aligned=True):
        return ref[pl.ds(pl.multiple_of(row, 8) if aligned else row, 8), :]

    def put(ref, row, value):
        ref[pl.ds(pl.multiple_of(row, 8), 8), :] = value

    def each(body, carry=None, downward=False):
        def step(n, c):
            g = groups - 1 - n if downward else n
            return body(g, c)
        return lax.fori_loop(0, groups, step, carry)

    def pair(ref, g, j):
        return at(ref, g * 256 + 16 * j), at(ref, g * 256 + 16 * j + 8)

    def put_pair(ref, g, j, value):
        put(ref, g * 256 + 16 * j, value[0])
        put(ref, g * 256 + 16 * j + 8, value[1])

    def edge_rows(g, j, x, low, high, base):
        row = base + g * 32 + 2 * j
        low[pl.ds(row, 2), :] = x[0][0:2]
        if high is not None:
            high[pl.ds(row, 2), :] = x[1][6:8]

    def pack_columns(j, x, acc):
        for half in range(2):
            n = 2 * j + half
            acc = jnp.where(lane // 4 == n, roll(x[half], 4 * n + 2, 1), acc)
        return acc

    def remote(src, dst, ss, rs, dev):
        return pltpu.make_async_remote_copy(
            src_ref=src, dst_ref=dst, send_sem=ss, recv_sem=rs, device_id=dev, device_id_type=MESH
        )

    def dense(own, base, to_right, to_left, row):
        for n in range(groups // 2):
            a, b = (own[base + 16 * n + 8 * m:base + 16 * n + 8 * m + 8, :] for m in range(2))
            to_right[row + 8 * n:row + 8 * n + 8, :] = jnp.where(quad < 2, a, roll(b, 2, 1))
            to_left[row + 8 * n:row + 8 * n + 8, :] = jnp.where(quad < 2, roll(a, -2, 1), b)

    def open_up(fl, fr, row, dst, base):
        for n in range(groups // 2):
            a, b = fl[row + 8 * n:row + 8 * n + 8, :], fr[row + 8 * n:row + 8 * n + 8, :]
            for m in range(2):
                k = base + 16 * n + 8 * m
                dst[k:k + 8, :] = jnp.where(
                    quad < 2, roll(b, -2 * m, 1), roll(a, 2, 1) if m == 0 else a
                )

    for c in loads[:3]:
        c.wait()

    def first_pack(g, carry):
        accp = accb = accv = zero
        for j in range(GROUP):
            accp = pack_columns(j, pair(p, g, j), accp)
            accb = pack_columns(j, pair(q.bi, g, j), accb)
            accv = pack_columns(j, pair(q.vs, g, j), accv)
        put(q.own0, g * 8, accp)
        put(q.own0, KJ + g * 8, accb)
        put(q.own0, 2 * KJ + g * 8, accv)
        return carry

    each(first_pack, 0)

    dense(q.own0, 0, q.j0_right, q.j0_left, 0)
    for n in range(groups // 2):
        rights, lefts = [], []
        for m in range(2):
            k = 16 * n + 8 * m
            ab = q.own0[KJ + k:KJ + k + 8, :]
            av = q.own0[2 * KJ + k:2 * KJ + k + 8, :]
            rights.append(jnp.where(quad == 0, roll(av, -1, 1), ab))
            lefts.append(jnp.where(quad == 0, roll(av, -2, 1), roll(ab, -1, 1)))
        k = KH + 8 * n
        for ref, (a, b) in ((q.j0_right, rights), (q.j0_left, lefts)):
            ref[k:k + 8, :] = jnp.where(quad < 2, a, roll(b, 2, 1))

    pl.semaphore_wait(barrier, 4 + nz - 1)

    def four(i, j, ss, rs, at_=lambda r: r):
        pairs = (
            (j + "_right", j + "_fl"), (j + "_left", j + "_fr"),
            (i + "_low", i + "_up"), (i + "_high", i + "_down"),
        )
        return [
            remote(at_(getattr(q, a)), at_(getattr(q, b)), ss(n), rs(n), dev)
            for n, ((a, b), dev) in enumerate(zip(pairs, sides))
        ]

    rows0 = pl.ds(8, 3 * K2)
    halos = [
        remote(
            a if n < 2 else a.at[rows0], b if n < 2 else b.at[rows0],
            q.h0_s.at[n], q.h0_r.at[n], dev,
        )
        for n, (a, b, dev) in enumerate(zip(
            (q.j0_right, q.j0_left, q.i0_low, q.i0_high),
            (q.j0_fl, q.j0_fr, q.i0_up, q.i0_down), sides,
        ))
    ]
    for c in halos[:2]:
        c.start()

    loads[4].wait()

    def first_rows(g, carry):
        for j in range(GROUP):
            for n, ref in enumerate((p, q.bi, q.us)):
                edge_rows(g, j, pair(ref, g, j), q.i0_low, q.i0_high, 8 + n * K2)
        return carry

    each(first_rows, 0)
    for c in halos[2:]:
        c.start()

    loads[3].wait()

    def factor(g, carry):
        B, Z, yend = carry
        for j in reversed(range(GROUP)):
            bb, ss = pair(q.bi, g, j), pair(q.s, g, j)
            newB, newZ, newy = [], [], []
            for m in range(2):
                row = g * 256 + 16 * j + 8 * m
                gb = GAIN * bb[m]
                o = 1.0 + gb * B[m]
                d = 1.0 / (o + gb * ss[m])
                hh = gb * d
                e = hh * ss[m]
                put(q.D, row, d)
                put(q.H, row, hh)
                od = o * d
                put(q.E, row, e)
                dz = d * Z[m]
                put(q.Y, row, dz)
                put(q.dX, row, od)
                newB.append(ss[m] * od)
                newZ.append(e * Z[m])
                newy.append(yend[m] - (gb * dz) * Z[m])
            B, Z, yend = tuple(newB), tuple(newZ), tuple(newy)
        return B, Z, yend

    B, Z, yend = each(factor, ((zero, zero), (one, one), (zero, zero)), downward=True)
    for n, val in enumerate((Z, yend, B)):
        for m in range(2):
            q.cmine[16 * n + 8 * m:16 * n + 8 * m + 8, :] = val[m]
            q.cgath[me, 16 * n + 8 * m:16 * n + 8 * m + 8, :] = val[m]
    consts = [
        remote(q.cmine, q.cgath.at[me], q.cs_s.at[o - 1], q.cs_r.at[o - 1], {"lev": lax.rem(me + o, nz)})
        for o in range(1, nz)
    ]
    for c in consts:
        c.start()

    def responses(g, carry):
        x, y = carry
        accs = [zero] * 3
        for j in range(GROUP):
            bb, ss, dd = pair(q.bi, g, j), pair(q.s, g, j), pair(q.D, g, j)
            od, dz = pair(q.dX, g, j), pair(q.Y, g, j)
            vals = []
            for m in range(2):
                sd, gb = ss[m] * dd[m], GAIN * bb[m]
                xg, yg = sd * x[m], sd * y[m] - dz[m]
                dx, dy = -(od[m] * x[m]), -(od[m] * y[m] + gb * dz[m])
                vals.append((gb * xg, gb * yg, xg, yg, dx, dy, ss[m] * dx, ss[m] * dy))
            vals = list(zip(*vals))
            x, y = vals[:2]
            for ref, val in zip((q.X, q.Y, q.XG, q.YG, q.dX, q.dY, q.P, q.Q), vals):
                put_pair(ref, g, j, val)
            for n, val in enumerate((ss, vals[6], vals[7])):
                edge_rows(g, j, val, q.is_low, q.is_high, n * K2)
                accs[n] = pack_columns(j, val, accs[n])
        for n in range(3):
            put(q.Oc, n * KJ + g * 8, accs[n])
        return x, y

    each(responses, ((one, one), (zero, zero)))
    for n in range(3):
        dense(q.Oc, n * KJ, q.js_right, q.js_left, n * KH)
    setups = four("is", "js", lambda n: q.hs_s.at[n], lambda n: q.hs_r.at[n])
    for c in setups:
        c.start()

    def crow(d, n):
        n = (0, 1, 0, 2)[n]
        return q.cgath[d, 16 * n:16 * n + 16, :]

    def stagger(g, carry):
        for j in range(GROUP):
            xb, xu, xv = pair(q.bi, g, j), pair(q.us, g, j), pair(q.vs, g, j)
            xb = tuple(CH * v for v in xb)
            for val, dst in ((xu, q.us), (xb, q.bi)):
                r0, r1 = roll(val[0], 7, 0), roll(val[1], 7, 0)
                put_pair(dst, g, j, (jnp.where(sub < 7, r0, r1), r1))
            for val, dst in ((xv, q.vs), (xb, q.bj)):
                put_pair(dst, g, j, [roll(v, 127, 1) for v in val])
        return carry

    each(stagger, 0)

    loads[5].wait()
    for c in halos:
        c.wait()

    for n in range(groups // 2):
        fr = q.j0_fr[KH + 8 * n:KH + 8 * n + 8, :]
        fl = q.j0_fl[KH + 8 * n:KH + 8 * n + 8, :]
        for m in range(2):
            k = 16 * n + 8 * m
            frg, flg = roll(fr, -2 * m, 1), roll(fl, -2 * m, 1)
            ab = q.own0[KJ + k:KJ + k + 8, :]
            av = q.own0[2 * KJ + k:2 * KJ + k + 8, :]
            vright = jnp.where(quad == 0, roll(av, -1, 1), roll(frg, 1, 1))
            bright = jnp.where(quad == 0, roll(ab, -1, 1), frg)
            vleft = jnp.where(quad == 2, roll(flg, 2, 1), roll(av, 1, 1))
            bleft = roll(jnp.where(quad == 1, flg, ab), 1, 1)
            q.hv[k:k + 8, :] = jnp.where(quad < 2, vright, vleft)
            q.hbj[k:k + 8, :] = CH * jnp.where(quad < 2, -bright, bleft)
    open_up(q.j0_fl, q.j0_fr, 0, q.Hp.at[0], 0)

    def patch(g, carry):
        for j in range(GROUP):
            row = g * 256 + 16 * j + 15
            q.us[pl.ds(row, 1), :] = q.i0_up[pl.ds(8 + 2 * K2 + g * 32 + 2 * j, 1), :]
            q.bi[pl.ds(row, 1), :] = CH * q.i0_up[pl.ds(8 + K2 + g * 32 + 2 * j, 1), :]
        for r in range(4):
            row = g * 32 + 8 * r
            for (dst, f, scale) in ((q.hu, 2, 1.0), (q.hbi, 1, CH)):
                base = 8 + f * K2 + row
                below = q.i0_down[pl.ds(base + 1, 8), :]
                own = q.i0_low[pl.ds(base - 1, 8), :]
                put(dst, 8 + row, scale * jnp.where(sub % 2 == 0, below, own))
        return carry

    each(patch, 0)

    def interface():
        beta = jnp.zeros((16, 128), F32)
        betas, rs, zbrs, lams = ([None] * nz for _ in range(4))
        for d in range(nz - 1, -1, -1):
            betas[d] = beta
            rs[d] = 1.0 / (1.0 - crow(d, 1) * beta)
            zbrs[d] = crow(d, 2) * beta * rs[d]
            lams[d] = crow(d, 2) + zbrs[d] * crow(d, 1)
            beta = crow(d, 3) + zbrs[d] * crow(d, 0)
            if d == 0:
                last = beta
        tops = [last] + betas[:-1]
        psi = jnp.zeros((16, 128), F32)
        psis, r2s, xrs, xrps = ([None] * nz for _ in range(4))
        for d in range(nz):
            xrs[d] = crow(d, 0) / (1.0 - psi * crow(d, 3))
            xrps[d] = xrs[d] * psi
            psis[d] = psi
            r2s[d] = 1.0 / (1.0 - psi * tops[d])
            psi = crow(d, 1) + xrps[d] * crow(d, 2)

        def pick(vals):
            out = vals[0]
            for d in range(1, nz):
                out = jnp.where(me == d, vals[d], out)
            return out

        br = [betas[d] * rs[d] for d in range(nz)]
        brx = [br[d] * crow(d, 0) for d in range(nz)]
        for n, vals in enumerate((xrps, zbrs, [r2s[d] * psis[d] for d in range(nz)], br, brx)):
            q.mine[16 * n:16 * n + 16, :] = pick(vals)
        for L in range(nz):
            part = r2s[L]
            for d in range(L - 1, -1, -1):
                q.ctab[L * nz + d, 0:16, :] = part
                q.ctab[L * nz + d, 16:32, :] = brx[L] * part
                part = part * xrs[d]
            part, gain = jnp.ones((16, 128), F32), 1.0 + br[L] * crow(L, 1)
            rpl = r2s[L] * psis[L] * lams[L]
            for d in range(L + 1, nz):
                cw = rpl * part
                q.ctab[L * nz + d, 0:16, :] = cw
                q.ctab[L * nz + d, 16:32, :] = part * gain + brx[L] * cw
                part = part * lams[d]

    def halves(x):
        return x[0:8], x[8:16]

    def pack_pair(wx, px):
        (w0, w1), (p0, p1) = halves(wx), halves(px)
        acc = roll(w0, 2, 1)
        for n, val in ((1, w1), (2, p0), (3, p1)):
            acc = jnp.where(lane // 4 == n, roll(val, 4 * n + 2, 1), acc)
        return acc

    def spread(t):
        z = jnp.where(lane < 16, t, 0.0)
        for n in (16, 32, 64):
            z = z + roll(z, n, 1)
        r = roll(z, 8, 1)
        return jnp.where(lane % 16 < 8, z, r), jnp.where(lane % 16 < 8, r, z)

    def insert(v, base):
        return roll(v, 126 - base, 1)

    def level_sums():
        for k in range(0, K2, 8):
            own, above = q.i0_high[pl.ds(9 + K2 + k, 8), :], q.i0_up[pl.ds(7 + K2 + k, 8), :]
            q.bih[k:k + 8, :] = CH * jnp.where(sub % 2 == 0, own, above)
            for n in range(2):
                q.mi[n * K2 + k:n * K2 + k + 8, :] = (
                    q.hbi[8 + k:16 + k, :] * q.is_down[(n + 1) * K2 + k:(n + 1) * K2 + k + 8, :]
                )
        for k in range(0, KJ, 8):
            hb = q.hbj[k:k + 8, :]
            for n in range(2):
                h, o = (r[(n + 1) * KJ + k:(n + 1) * KJ + k + 8, :] for r in (q.Hc, q.Oc))
                q.cj[n * KJ + k:n * KJ + k + 8, :] = jnp.where(quad < 2, -hb, hb) * h
                q.wo[n * KJ + k:n * KJ + k + 8, :] = CH * jnp.where(quad < 2, -o, o)

        def add(acc, n, m, value):
            acc[n][m] = acc[n][m] + value

        def along_i(g, carry):
            acc = [list(c) for c in carry]
            for j in range(GROUP):
                pq = (pair(q.P, g, j), pair(q.Q, g, j))
                bb = pair(q.bi, g, j)
                ahead, behind = [], []
                for n, (g0, g1) in enumerate(pq):
                    r0, r1 = roll(g0, 6, 0), roll(g1, 6, 0)
                    edge = q.is_up[pl.ds((n + 1) * K2 + g * 32 + 2 * j - 6, 8), :]
                    ahead.append((
                        bb[0] * jnp.where(sub < 6, r0, r1), bb[1] * jnp.where(sub < 6, r1, edge)
                    ))
                    r0, r1 = roll(bb[0] * g0, 2, 0), roll(bb[1] * g1, 2, 0)
                    edge = q.mi[pl.ds(n * K2 + g * 32 + 2 * j, 8), :]
                    behind.append((jnp.where(sub < 2, edge, r0), jnp.where(sub < 2, r0, r1)))
                for f in range(2):
                    for m in range(2):
                        cf = CH * pq[f][m]
                        for n in range(2):
                            add(acc, 2 * f + n, m, cf * ahead[n][m])
                            add(acc, 4 + 2 * f + n, m, cf * behind[n][m])
            return tuple(tuple(c) for c in acc)

        def along_j(g, carry):
            acc = [list(c) for c in carry]
            cs = [at(q.cj, n * KJ + g * 8) for n in range(2)]
            for j in range(GROUP):
                pq = (pair(q.P, g, j), pair(q.Q, g, j))
                bb = pair(q.bj, g, j)
                for m in range(2):
                    ahead, behind = [], []
                    for n in range(2):
                        edge = insert(cs[n], 4 * (2 * j + m))
                        ahead.append(jnp.where(lane >= 126, edge, bb[m] * roll(pq[n][m], 126, 1)))
                        behind.append(jnp.where(lane < 2, edge, roll(bb[m] * pq[n][m], 2, 1)))
                    for f in range(2):
                        cf = CH * pq[f][m]
                        for n in range(2):
                            add(acc, 2 * f + n, m, cf * ahead[n])
                            add(acc, 4 + 2 * f + n, m, cf * behind[n])
            return tuple(tuple(c) for c in acc)

        def centre(g, carry):
            acc = [list(c) for c in carry]
            hb = at(q.hbj, g * 8)
            hb = jnp.where(quad < 2, -hb, hb)
            for j in range(GROUP):
                bbi, bbj = pair(q.bi, g, j), pair(q.bj, g, j)
                pp, qq, dx, dy = (pair(r, g, j) for r in (q.P, q.Q, q.dX, q.dY))
                xx, yy, xg, yg = (pair(r, g, j) for r in (q.X, q.Y, q.XG, q.YG))
                r0, r1 = roll(bbi[0], 2, 0), roll(bbi[1], 2, 0)
                edge = at(q.hbi, 8 + g * 32 + 2 * j, False)
                bim = (jnp.where(sub < 2, edge, r0), jnp.where(sub < 2, r0, r1))
                for m in range(2):
                    edge = insert(hb, 4 * (2 * j + m))
                    bjm = jnp.where(lane < 2, edge, roll(bbj[m], 2, 1))
                    sb = CH * ((bbi[m] + bim[m]) + (jnp.where(lane >= 126, edge, bbj[m]) + bjm))
                    fx, fy = dx[m] - sb * pp[m], dy[m] - sb * qq[m]
                    add(acc, 0, m, pp[m] * fx - xg[m] * xx[m])
                    add(acc, 1, m, qq[m] * fx - xg[m] * yy[m])
                    add(acc, 2, m, qq[m] * fy - yg[m] * yy[m])
            return tuple(tuple(c) for c in acc)

        first = 0
        for body, count in ((centre, 3), (along_i, 8), (along_j, 8)):
            for n, val in enumerate(each(body, ((zero, zero),) * count)):
                q.coef[first + n, 0:8, :], q.coef[first + n, 8:16, :] = val
            first += count

    def base_rows(t):
        def body(g, carry):
            A, W, before = carry
            for j in range(GROUP):
                star, w0, ss, uu, vv, bbi, bbj, dx, dy, pp, qq, xg, yg = (
                    pair(r, g, j) for r in (
                        q.ps, w, q.s, q.us, q.vs, q.bi, q.bj, q.dX, q.dY, q.P, q.Q, q.XG, q.YG
                    )
                )
                pt = tuple(star[m] - ss[m] * (w0[m] - before[m]) for m in range(2))
                r0, r1 = roll(pt[0], 6, 0), roll(pt[1], 6, 0)
                pi = (jnp.where(sub < 6, r0, r1), jnp.where(sub < 6, r1, 0.0))
                un = tuple(uu[m] - bbi[m] * (pi[m] - pt[m]) for m in range(2))
                r0, r1 = roll(un[0], 2, 0), roll(un[1], 2, 0)
                um = (jnp.where(sub < 2, 0.0, r0), jnp.where(sub < 2, r0, r1))
                newA, newW = [], []
                for m in range(2):
                    vn = vv[m] - bbj[m] * (roll(pt[m], 126, 1) - pt[m])
                    vn = jnp.where(lane >= 126, 0.0, vn)
                    vm = jnp.where(lane < 2, 0.0, roll(vn, 2, 1))
                    div = CH * ((un[m] - um[m]) + (vn - vm))
                    newA.append(A[m] + (pp[m] * div - (dx[m] * pt[m] + xg[m] * w0[m])))
                    newW.append(W[m] + (qq[m] * div - (dy[m] * pt[m] + yg[m] * w0[m])))
                A, W, before = tuple(newA), tuple(newW), w0
            return A, W, before

        A, W, _ = each(body, ((zero, zero),) * 3)
        return list(A), list(W)

    def rows_without(src, const, dst):
        before = zero
        for k in range(0, K2, 8):
            star, w0, cs = src[k:k + 8, :], src[K2 + k:K2 + k + 8, :], const[k:k + 8, :]
            now = roll(w0, 2, 0)
            dst[k:k + 8, :] = star - cs * (w0 - jnp.where(sub < 2, before, now))
            before = now

    def columns_without(src, const, dst):
        before = zero
        for k in range(0, KJ, 8):
            star, w0, cs = src[k:k + 8, :], src[KJ + k:KJ + k + 8, :], const[k:k + 8, :]
            now = roll(w0, 8, 1)
            dst[k:k + 8, :] = star - cs * (w0 - jnp.where(lane < 8, before, now))
            before = now

    def halo_rows(t, A, W):
        lows, highs, cols = [zero, zero], [zero, zero], [zero, zero]
        for k in range(0, K2, 8):
            hu_new = q.hu[8 + k:16 + k, :] - q.hbi[8 + k:16 + k, :] * (
                q.b_low[t, k:k + 8, :] - q.b_down[t, k:k + 8, :]
            )
            high = q.bih[k:k + 8, :] * q.b_up[t, k:k + 8, :]
            for n in range(2):
                r = (n + 1) * K2 + k
                lows[n] = lows[n] + q.is_low[r:r + 8, :] * hu_new
                highs[n] = highs[n] + q.is_high[r:r + 8, :] * high
        for k in range(0, KJ, 8):
            c = q.hv[k:k + 8, :] - q.hbj[k:k + 8, :] * (q.Ob[t, k:k + 8, :] - q.Hb[t, k:k + 8, :])
            for n in range(2):
                cols[n] = cols[n] + q.wo[n * KJ + k:n * KJ + k + 8, :] * c
        for n, rows in enumerate((A, W)):
            low, high, col = lows[n], highs[n], cols[n]
            for r in (4, 2):
                low, high = low + roll(low, r, 0), high + roll(high, r, 0)
            for r in (32, 8):
                col = (col + roll(col, r, 1)) + (roll(col, 2 * r, 1) + roll(col, 3 * r, 1))
            rows[0] = rows[0] - jnp.where(sub < 2, CH * low, 0.0)
            rows[1] = rows[1] - jnp.where(sub >= 6, CH * high, 0.0)
            for m in range(2):
                rows[m] = rows[m] - jnp.where((lane >= 126) | (lane < 2), insert(col, 4 * m), 0.0)

    def send_round(t, W0, A0):
        final = t == SUBSTEPS - 1
        wa, aw, r2psi, br, brx = (q.mine[16 * n:16 * n + 16, :] for n in range(5))
        up_row, down_row = W0 + wa * A0, A0 + aw * W0
        q.fmine[t, 0], q.fmine[t, 1] = up_row, down_row
        sends = []
        wb_own = r2psi * down_row
        pa_own = br * W0 + brx * wb_own
        for o in sorted(range(nz), key=lambda o: -min(o, nz - o)):
            L = lax.rem(me + o, nz)
            if not final:
                if o:
                    row = jnp.where(L > me, up_row, down_row)
                    wc, pc = (q.ctab[L * nz + me, 16 * n:16 * n + 16, :] * row for n in range(2))
                else:
                    wc, pc = wb_own, pa_own
                q.jc[t, o] = pack_pair(wc, pc)
                q.ic_low[t, o] = jnp.where(sub < 2, wc[0:8], roll(pc[0:8], 2, 0))
                q.ic_high[t, o] = jnp.where(sub < 2, roll(wc[8:16], 2, 0), roll(pc[8:16], 4, 0))
                for n, (a, b) in enumerate((
                    (q.jc, q.jc_fl), (q.jc, q.jc_fr), (q.ic_low, q.ic_up), (q.ic_high, q.ic_down)
                )):
                    c = remote(
                        a.at[t, o], b.at[t, me], q.hc_s.at[t, n, o], q.hc_r.at[t, n, o],
                        {**sides[n], "lev": L},
                    )
                    c.start()
                    sends.append(c)
            if o:
                c = remote(
                    q.fmine.at[t, lax.div(me + o, nz)], q.fgath.at[t, me],
                    q.ls_s.at[t, o - 1], q.ls_r.at[t, o - 1], {"lev": L},
                )
                c.start()
                sends.append(c)
        return sends, wb_own, pa_own

    for t in range(SUBSTEPS):
        final = t == SUBSTEPS - 1
        if t:
            each(implicit, wb2)

            def add_columns(src, const, wp, dst):
                for k in range(0, KJ, 8):
                    dst[k:k + 8, :] = src[k:k + 8, :] - (
                        const[KJ + k:KJ + k + 8, :] * wp[0] + const[2 * KJ + k:2 * KJ + k + 8, :] * wp[1]
                    )

            def add_rows(src, const, v, dst):
                z = jnp.where(sub < 4, v, roll(v, 4, 0))
                r = roll(z, 2, 0)
                ws, ps_ = jnp.where(sub % 4 < 2, z, r), jnp.where(sub % 4 < 2, r, z)
                for k in range(0, K2, 8):
                    dst[8 + k:16 + k, :] = src[k:k + 8, :] - (
                        const[K2 + k:K2 + k + 8, :] * ws + const[2 * K2 + k:2 * K2 + k + 8, :] * ps_
                    )

            add_columns(q.Hb.at[t - 1], q.Hc, spread(halo_j), q.Hp.at[t])
            add_columns(q.Ob.at[t - 1], q.Oc, spread(pack_pair(wb, pa)), q.Op.at[t])
            low = jnp.where(sub < 2, wb[0:8], roll(pa[0:8], 2, 0))
            add_rows(q.b_up.at[t - 1], q.is_up, halo_up, q.p_up.at[t])
            add_rows(q.b_down.at[t - 1], q.is_down, halo_down, q.p_down.at[t])
            add_rows(q.b_low.at[t - 1], q.is_low, low, q.p_low.at[t])
        i_up, i_down, i_low = (
            (q.i0_up, q.i0_down, q.i0_low) if t == 0
            else (q.p_up.at[t], q.p_down.at[t], q.p_low.at[t])
        )
        own_p = q.own0 if t == 0 else q.Op.at[t]
        halo_p = q.Hp.at[t]

        for k in range(0, KJ, 8):
            q.hv[k:k + 8, :] = q.hv[k:k + 8, :] - q.hbj[k:k + 8, :] * (
                own_p[k:k + 8, :] - halo_p[k:k + 8, :]
            )

        def explicit(g, A):
            for r in range(4):
                row = g * 32 + 8 * r
                put(q.hu, 8 + row, at(q.hu, 8 + row) - at(q.hbi, 8 + row) * (
                    at(i_low, 8 + row) - at(i_down, 8 + row)
                ))
            c = at(q.hv, g * 8)
            acc = zero
            for j in reversed(range(GROUP)):
                pp, uu, vv, ww = pair(p, g, j), pair(q.us, g, j), pair(q.vs, g, j), pair(w, g, j)
                bbi, bbj, ss = pair(q.bi, g, j), pair(q.bj, g, j), pair(q.s, g, j)
                ee, dd, hh = pair(q.E, g, j), pair(q.D, g, j), pair(q.H, g, j)
                r0, r1 = roll(pp[0], 6, 0), roll(pp[1], 6, 0)
                edge = at(i_up, 8 + g * 32 + 2 * j - 6, False)
                pi = (jnp.where(sub < 6, r0, r1), jnp.where(sub < 6, r1, edge))
                un = tuple(uu[m] - bbi[m] * (pi[m] - pp[m]) for m in range(2))
                put_pair(q.us, g, j, un)
                r0, r1 = roll(un[0], 2, 0), roll(un[1], 2, 0)
                edge = at(q.hu, 8 + g * 32 + 2 * j, False)
                um = (jnp.where(sub < 2, edge, r0), jnp.where(sub < 2, r0, r1))
                newA, hs, pss, vn = [], [], [], []
                for m in range(2):
                    edge = roll(c, 126 - 4 * (2 * j + m), 1)
                    v_new = vv[m] - bbj[m] * (roll(pp[m], 126, 1) - pp[m])
                    v_new = jnp.where(lane >= 126, edge, v_new)
                    vm = jnp.where(lane < 2, edge, roll(v_new, 2, 1))
                    star = pp[m] - (CH * ss[m]) * ((un[m] - um[m]) + (v_new - vm))
                    dw = dd[m] * ww[m]
                    hs.append(dw + hh[m] * (star - A[m]))
                    newA.append(ee[m] * A[m] + ((star - ee[m] * star) - ss[m] * dw))
                    pss.append(star)
                    vn.append(v_new)
                put_pair(q.vs, g, j, vn)
                put_pair(q.ps, g, j, pss)
                put_pair(q.h, g, j, hs)
                if not final:
                    edge_rows(g, j, pss, q.iw_low.at[t], q.iw_high.at[t], 0)
                    acc = pack_columns(j, pss, acc)
                A = tuple(newA)
            if not final:
                put(q.Ow.at[t], g * 8, acc)
            return A

        A = each(explicit, (zero, zero), downward=True)

        def forward(g, x):
            acc = zero
            for j in range(GROUP):
                ee, hh = pair(q.E, g, j), pair(q.h, g, j)
                x = tuple(ee[m] * x[m] + hh[m] for m in range(2))
                put_pair(w, g, j, x)
                if not final:
                    edge_rows(g, j, x, q.iw_low.at[t], q.iw_high.at[t], K2)
                    acc = pack_columns(j, x, acc)
            if not final:
                put(q.Ow.at[t], KJ + g * 8, acc)
            return x

        x = each(forward, (zero, zero))
        if t == 0:
            for c in consts:
                c.wait()
            interface()
            A0, W0 = (jnp.concatenate(n, 0) for n in (A, x))
            sends, wb_own, pa_own = send_round(0, W0, A0)
        if not final:
            for n in range(2):
                dense(q.Ow.at[t], n * KJ, q.jw_right.at[t], q.jw_left.at[t], n * KH)
            works = four("iw", "jw", lambda n: q.hw_s.at[t, n], lambda n: q.hw_r.at[t, n], lambda r: r.at[t])
            for c in works:
                c.start()
            A1, W1 = base_rows(t)
            if t == 0:
                for c in setups:
                    c.wait()
                for n in range(3):
                    open_up(q.js_fl, q.js_fr, n * KH, q.Hc, n * KJ)
                level_sums()
            columns_without(q.Ow.at[t], q.Oc, q.Ob.at[t])
            rows_without(q.iw_low.at[t], q.is_low, q.b_low.at[t])

            def finish(A, W):
                for c in works:
                    c.wait()
                for n in range(2):
                    open_up(q.jw_fl.at[t], q.jw_fr.at[t], n * KH, q.Hw.at[t], n * KJ)
                columns_without(q.Hw.at[t], q.Hc, q.Hb.at[t])
                rows_without(q.iw_up.at[t], q.is_up, q.b_up.at[t])
                rows_without(q.iw_down.at[t], q.is_down, q.b_down.at[t])
                halo_rows(t, A, W)

            if t == 0:
                finish(A1, W1)

        if final:
            def emit(g, carry):
                hvg = at(q.hv, pl.multiple_of(g * 8, 8))
                for j in range(GROUP):
                    uu, vv = pair(q.us, g, j), pair(q.vs, g, j)
                    r0, r1 = roll(uu[0], 1, 0), roll(uu[1], 1, 0)
                    edge = at(q.hu, 8 + g * 32 + 2 * j + 1, False)
                    put_pair(uo, g, j, (jnp.where(sub < 1, edge, r0), jnp.where(sub < 1, r0, r1)))
                    put_pair(vo, g, j, [
                        jnp.where(
                            lane == 0, roll(hvg, 125 - 4 * (2 * j + m), 1), roll(vv[m], 1, 1)
                        )
                        for m in range(2)
                    ])
                return carry

            each(emit, 0)
        for c in sends:
            c.wait()

        wb, pa = wb_own, pa_own
        for o in range(1, nz):
            d = lax.rem(me + o, nz)
            row = q.fgath[t, d]
            wb = wb + q.ctab[me * nz + d, 0:16, :] * row
            pa = pa + q.ctab[me * nz + d, 16:32, :] * row
        wb2, pa2 = halves(wb), halves(pa)

        if not final:
            fr, fl, halo_up, halo_down = (
                functools.reduce(lambda a, b: a + b, [ref[t, d] for d in range(nz)])
                for ref in (q.jc_fr, q.jc_fl, q.ic_up, q.ic_down)
            )
            halo_j = jnp.where(quad < 2, roll(fr, -2, 1), roll(fl, 2, 1))
            stencil = []
            for n, v in enumerate((wb2, pa2)):
                a0, a1, b0, b1 = (roll(v[m], k, 0) for k in (6, 2) for m in range(2))
                above, below = roll(halo_up, 6 - 2 * n, 0), roll(halo_down, -2 * n, 0)
                edges = [
                    jnp.where(
                        lane >= 126, roll(fr, 124 - 8 * n - 4 * m, 1), roll(fl, -8 * n - 4 * m, 1)
                    )
                    for m in range(2)
                ]
                stencil.append((
                    v,
                    (jnp.where(sub < 6, a0, a1), jnp.where(sub < 6, a1, above)),
                    (jnp.where(sub < 2, below, b0), jnp.where(sub < 2, b0, b1)),
                    tuple(jnp.where(lane >= 126, edges[m], roll(v[m], 126, 1)) for m in range(2)),
                    tuple(jnp.where(lane < 2, edges[m], roll(v[m], 2, 1)) for m in range(2)),
                ))
            rows = []
            for f, base in enumerate((A1, W1)):
                halves_ = []
                for m in range(2):
                    terms = [base[m]]
                    for n in range(2):
                        for k in range(5):
                            c = f + n if k == 0 else 3 + 4 * (k - 1) + 2 * f + n
                            terms.append(q.coef[c, 8 * m:8 * m + 8, :] * stencil[n][k][m])
                    while len(terms) > 1:
                        terms = [
                            sum(terms[k + 1:k + 2], terms[k]) for k in range(0, len(terms), 2)
                        ]
                    halves_.append(terms[0])
                rows.append(halves_)
            if t:
                finish(*rows)
            rows = [jnp.concatenate(r, 0) for r in rows]
            sends, wb_own, pa_own = send_round(t + 1, rows[1], rows[0])

        def implicit(g, wprev, wb2=wb2, pa2=pa2):
            for j in range(GROUP):
                w0, xx, yy = pair(w, g, j), pair(q.X, g, j), pair(q.Y, g, j)
                ss, star = pair(q.s, g, j), pair(q.ps, g, j)
                wn = tuple(w0[m] + xx[m] * wb2[m] + yy[m] * pa2[m] for m in range(2))
                pn = tuple(star[m] - ss[m] * (wn[m] - wprev[m]) for m in range(2))
                put_pair(w, g, j, wn)
                put_pair(p, g, j, pn)
                wprev = wn
            return wprev

    wend[0:16, :], wend[16:32, :] = wb, pa


def store(K, u, v, w, ps, s, X, Y, wend, u_out, v_out, w_out, p_out, wf, pf, sem):
    copies = []

    def begin(src, dst, n):
        c = pltpu.make_async_copy(src, dst, sem.at[n])
        c.start()
        copies.append(c)

    begin(u, u_out, 0)
    begin(v, v_out, 1)
    wb, pa = ((wend[16 * n:16 * n + 8, :], wend[16 * n + 8:16 * n + 16, :]) for n in range(2))
    before, size = wb, 16 * K // CHUNKS

    def step(k, before):
        after = []
        for m in range(2):
            rows = pl.ds(pl.multiple_of(k * 16 + 8 * m, 8), 8)
            wn = w[rows, :] + X[rows, :] * wb[m] + Y[rows, :] * pa[m]
            wf[rows, :] = wn
            pf[rows, :] = ps[rows, :] - s[rows, :] * (wn - before[m])
            after.append(wn)
        return tuple(after)

    for n in range(CHUNKS):
        part = K // CHUNKS
        before = lax.fori_loop(n * part, (n + 1) * part, step, before, unroll=8)
        rows = pl.ds(n * size, size)
        begin(wf.at[rows], w_out.at[rows], 2 + 2 * n)
        begin(pf.at[rows], p_out.at[rows], 3 + 2 * n)
    for c in copies:
        c.wait()


def solution(mesh):
    nx, ny, nz = (mesh.shape[a] for a in ("gx", "gy", "lev"))

    def shards(*fields):
        K, I, J = fields[0].shape
        assert I == 16 and J == 128 and K % (2 * GROUP) == 0
        R = K * I
        full = pltpu.VMEM((R, J), F32)
        held = scratch(K, J, nz)
        outs = pl.pallas_call(
            functools.partial(kernel, tuple(held), K, nx, ny, nz),
            out_shape=[full] * 7 + [pltpu.VMEM((32, J), F32)],
            in_specs=[pl.BlockSpec(memory_space=pl.ANY)] * 6,
            out_specs=[pl.BlockSpec(memory_space=pltpu.VMEM)] * 8,
            scratch_shapes=list(held.values()),
            compiler_params=pltpu.CompilerParams(
                collective_id=0, has_side_effects=True, vmem_limit_bytes=60 * 2**20
            ),
        )(*(f.reshape(R, J) for f in fields))
        outs = pl.pallas_call(
            functools.partial(store, K),
            out_shape=[jax.ShapeDtypeStruct((R, J), F32)] * 4,
            in_specs=[pl.BlockSpec(memory_space=pltpu.VMEM)] * 8,
            out_specs=[pl.BlockSpec(memory_space=pl.ANY)] * 4,
            scratch_shapes=[full, full, pltpu.SemaphoreType.DMA((2 + 2 * CHUNKS,))],
            compiler_params=pltpu.CompilerParams(vmem_limit_bytes=16 * 2**20),
        )(*(pltpu.with_memory_space_constraint(o, pltpu.VMEM) for o in outs))
        return tuple(o.reshape(K, I, J) for o in outs)

    spec = P("lev", "gx", "gy")
    return jax.shard_map(
        shards, mesh=mesh, in_specs=(spec,) * 6, out_specs=(spec,) * 4, check_vma=False
    )
```
